32 devices in a mesh: groups: 2 (over y), seq: 4 (over z), head: 4 (over x, core).
Axes of the slice: x: 2, y: 2, z: 4, core: 2. Of those that a mesh axis runs over, the one named last changes fastest.
Arguments:
- residual: bfloat16 [4096, 2560], P(('groups', 'seq'), 'head'), parts along dimension 0, may hold values from -6 to 6
- x_in: bfloat16 [4096, 5120], P(('groups', 'seq'), 'head'), parts along dimension 0, may hold values from -6 to 6
- bc_in: bfloat16 [4096, 256], P(('groups', 'seq')), parts along dimension 0, may hold values from -1.5 to 1.5
- z_in: bfloat16 [4096, 5120], P(('groups', 'seq'), 'head'), parts along dimension 0, may hold values from -6 to 6
- dt_raw: float32 [80, 4096], P('head', ('groups', 'seq')), parts along dimension 1, may hold values from -5 to 5
- dt_bias: float32 [80], P('head'), may hold values from -3 to 0
- decay_rate: float32 [80], P('head'), may hold values from 0.0003 to 0.15
- d_skip: float32 [80], P('head'), may hold values from 1 to 4
- conv_x_weight: bfloat16 [4, 5120], P(None, 'head'), may hold values from -3 to 3
- conv_x_bias: bfloat16 [5120], P('head'), may hold values from -3 to 3
- conv_bc_weight: bfloat16 [4, 256], replicated, may hold values from -3 to 3
- conv_bc_bias: bfloat16 [256], replicated, may hold values from -3 to 3
- norm_gain: bfloat16 [5120], P('head'), may hold values from 0.5 to 1.5
- out_weight: bfloat16 [5120, 2560], P('head'), may hold values from -0.078125 to 0.078125
- final_gain: bfloat16 [2560], replicated, may hold values from 0.5 to 1.5
- lm_weight: bfloat16 [2560, 25600], P('seq', 'head'), may hold values from -15.811388 to 15.811388
- targets: int32 [4096], P(('groups', 'seq')), parts along dimension 0, may hold values from 0 to 25599
- doc_lengths: int32 [8], P('groups'), parts along dimension 0, may hold values from 1 to 1536, as said below
Outputs:
- block_out: bfloat16 [4096, 2560], P(('groups', 'seq'), 'head'), parts along dimension 0
- doc_loss: float32 [8], P('groups'), parts along dimension 0
The draws below stay inside these ranges and needn't reach their ends.
There are 2 independent parts, one for each index of `groups`. The reference program is written for one: setup_inputs(seed, part) draws one part's arguments, and reference() takes and returns one part's arrays. A program takes and returns all parts, laid end to end along the dimension named above; an argument that names none is the same for every part. Nothing has to cross between parts.
Inputs may be any that keep to these rules, and one draw needn't show every extreme that they name: `doc_lengths`: the lengths of a group's 4 documents, in the order in which they are packed into its 2048 tokens; they sum to 2048.
All inputs are finite; a program needn't handle non-finite values.
Results may differ from the reference program's by a relative error of at most 0.00145.
The reference program's roundings to bfloat16 on the way count: a program that leaves them out, or rounds other values in their place, can miss the bound.
Values may be sent and summed in bfloat16 or wider, within the bound.
A program may use at most 128 MiB of HBM per device.

```python
import math
import jax
import jax.numpy as jnp
import numpy as np
from jax import lax

D = 2560
HEADS = 80
HEAD_SIZE = 64
STATE = 128
KERNEL = 4
VOCAB = 25600
SPAN = 256
TOK_DEV = 512
INNER = 5120
TOKENS = 2048
DOCS = 4
N_SEQ = 4


def draw_lm_weight(key, part):
    entries = jax.random.truncated_normal(jax.random.fold_in(key, 11), -5.0, 5.0, (D, VOCAB), jnp.float32) * (3.0 / math.sqrt(D))
    return entries.astype(jnp.bfloat16)


def draw_doc_lengths(key, part):
    longest = 3 * TOK_DEV
    rest = TOKENS - longest
    others = DOCS - 1
    spacing = rest // others
    jitter = jax.random.randint(jax.random.fold_in(key, 21), (others - 1,), 0, spacing, jnp.int32)
    cuts = (jnp.arange(1, others, dtype=jnp.int32) * spacing + jitter).astype(jnp.int32)
    edges = jnp.concatenate([jnp.zeros((1,), jnp.int32), cuts, jnp.full((1,), rest, jnp.int32)])
    pieces = (edges[1:] - edges[:-1]).astype(jnp.int32)
    joined = jnp.concatenate([pieces, jnp.full((1,), longest, jnp.int32)])
    place = jax.random.randint(jax.random.fold_in(key, 22), (), 0, DOCS, jnp.int32)
    order = jnp.arange(DOCS, dtype=jnp.int32)
    index = jnp.where(order < place, order, jnp.where(order == place, others, order - 1)).astype(jnp.int32)
    return joined[index]


def plant(array, own_key, least, largest):
    longest = array.shape.index(max(array.shape))
    spots = []
    for shift in (0, 1):
        where = [jax.random.randint(jax.random.fold_in(own_key, axis), (), 0, length) for axis, length in enumerate(array.shape)]
        where[longest] = (where[longest] + shift) % array.shape[longest]
        spots.append(tuple(where))
    return array.at[spots[0]].set(least).at[spots[1]].set(largest)


def steps_of(own_key, shape, split, low, high):
    gain = 1.0
    for axis_at, blocks in split:
        draws = jax.random.uniform(jax.random.fold_in(jax.random.fold_in(own_key, 6), axis_at), (blocks,), jnp.float32, low / len(split), high / len(split))
        gain = gain * jnp.repeat(jnp.exp(draws), shape[axis_at] // blocks).reshape((-1,) + (1,) * (len(shape) - 1 - axis_at))
    return gain


def rank_bounds(amount, lean):
    portions = [(1 << 20) // math.isqrt(standing ** lean) + 1 for standing in range(1, amount + 1)]
    width = 1 + sum(portions) // (1 << 30)
    return np.cumsum(np.array([max(1, weight // width) for weight in portions]))


def skewed_ids(rng, shape, number_of, slope):
    listing = rank_bounds(number_of, slope)
    lot = jax.random.randint(jax.random.fold_in(rng, 1), shape, 0, int(listing[number_of - 1]))
    rank = jnp.searchsorted(jnp.asarray(listing, jnp.int32), lot, side="right")
    return jax.random.permutation(jax.random.fold_in(rng, 2), number_of)[rank].astype(jnp.int32)


def gaussian(rng, dims, width, limit, shards=(), kind=jnp.bfloat16):
    result = jax.random.normal(rng, dims, jnp.float32) * width
    if len(shards) > 0:
        result = steps_of(rng, dims, shards, -0.22, 0.18) * result
    return jnp.clip(result, min=-limit, max=limit).astype(kind)


def setup_inputs(seed: int = 0, part: int = 0) -> dict:
    arg_keys = jax.random.split(jax.random.key(seed), 19)
    part_splits = jax.random.split(jax.random.fold_in(arg_keys[18], part), 19)
    return {
        "residual": gaussian(part_splits[0], (TOKENS, D), 1.0, 6.0, ((0, 4), (1, 4))),
        "x_in": gaussian(part_splits[1], (TOKENS, INNER), 1.0, 6.0, ((0, 4), (1, 4))),
        "bc_in": gaussian(part_splits[2], (TOKENS, 2 * STATE), 0.25, 1.5, ((0, 4),)),
        "z_in": gaussian(part_splits[3], (TOKENS, INNER), 1.0, 6.0, ((0, 4), (1, 4))),
        "dt_raw": gaussian(part_splits[4], (HEADS, TOKENS), 1.0, 5.0, ((0, 4), (1, 4)), jnp.float32),
        "dt_bias": jnp.clip(-3.0 + 3.0 * jax.random.uniform(arg_keys[5], (HEADS,), jnp.float32) ** steps_of(arg_keys[5], (HEADS,), ((0, 4),), -0.2, 0.2), -3.0, 0.0),
        "decay_rate": jnp.clip(jnp.exp(math.log(0.15) - 6.214608 * jax.random.uniform(arg_keys[6], (HEADS,), jnp.float32) ** steps_of(arg_keys[6], (HEADS,), ((0, 4),), -0.2, 0.2)), 0.0003, 0.15),
        "d_skip": jnp.clip(1.0 + 3.0 * jax.random.uniform(arg_keys[7], (HEADS,), jnp.float32) ** steps_of(arg_keys[7], (HEADS,), ((0, 4),), -0.2, 0.2), 1.0, 4.0),
        "conv_x_weight": gaussian(arg_keys[8], (KERNEL, INNER), KERNEL ** -0.5, 3.0, ((1, 4),)),
        "conv_x_bias": gaussian(arg_keys[9], (INNER,), 0.5, 3.0, ((0, 4),)),
        "conv_bc_weight": gaussian(arg_keys[10], (KERNEL, 2 * STATE), KERNEL ** -0.5, 3.0),
        "conv_bc_bias": gaussian(arg_keys[11], (2 * STATE,), 0.5, 3.0),
        "norm_gain": jnp.clip(1.0 + 0.1 * jax.random.normal(arg_keys[12], (INNER,), jnp.float32), 0.5, 1.5).astype(jnp.bfloat16),
        "out_weight": gaussian(arg_keys[13], (INNER, D), INNER ** -0.5, 0.078125, ((0, 4),)),
        "final_gain": jnp.clip(1.0 + 0.1 * jax.random.normal(arg_keys[14], (D,), jnp.float32), 0.5, 1.5).astype(jnp.bfloat16),
        "lm_weight": draw_lm_weight(jax.random.fold_in(arg_keys[18], 71), part),
        "targets": plant(skewed_ids(part_splits[16], (TOKENS,), VOCAB, 2), jax.random.fold_in(part_splits[16], 3), 0, VOCAB - 1).astype(jnp.int32),
        "doc_lengths": draw_doc_lengths(jax.random.fold_in(jax.random.fold_in(arg_keys[18], part), 71), part),
    }


EPSILON = 1e-05
HIGH = lax.Precision.HIGHEST

def document_of(positions, doc_lengths):
    starts = jnp.cumsum(doc_lengths) - doc_lengths
    return lax.optimization_barrier(jnp.sum((positions[:, None] >= starts[None, :]).astype(jnp.int32), axis=1)) - 1

def causal_conv(signal, rim_rows, weight, bias, positions, doc_ids, doc_lengths):
    length = signal.shape[0]
    taps = weight.shape[0]
    joined = jnp.concatenate([rim_rows, signal], axis=0).astype(jnp.float32)
    total = jnp.zeros(signal.shape, jnp.float32) + bias.astype(jnp.float32)[None, :]
    for offset in range(taps):
        lag = taps - 1 - offset
        source = document_of(positions - lag, doc_lengths)
        same = (source == doc_ids).astype(jnp.float32)
        total = total + weight[offset].astype(jnp.float32)[None, :] * joined[offset:offset + length] * same[:, None]
    return jax.nn.silu(total).astype(jnp.bfloat16)

def span_step(state, pieces, rates):
    signal, bmat, cmat, steps, doc_ids, doc_prev = pieces
    signal = signal.astype(jnp.float32)
    bmat = bmat.astype(jnp.float32)
    cmat = cmat.astype(jnp.float32)
    climb = jnp.cumsum(steps * rates[:, None], axis=1)
    extent = doc_ids.shape[0]
    order = jnp.arange(extent, dtype=jnp.int32)
    inside = (doc_ids[:, None] == doc_ids[None, :]) & (order[:, None] >= order[None, :])
    gap = climb[:, :, None] - climb[:, None, :]
    decay = jnp.where(inside[None], jnp.exp(-jnp.where(inside[None], gap, 0.0)), 0.0)
    scores = jnp.dot(cmat, bmat.T, precision=HIGH)
    weights = decay * scores[None] * steps[:, None, :]
    output = jnp.einsum('hts,shp->thp', weights, signal, precision=HIGH)
    carried = (doc_ids == doc_prev).astype(jnp.float32)
    entry = jnp.exp(-climb) * carried[None, :]
    output = output + jnp.einsum('tn,hpn->thp', cmat, state, precision=HIGH) * entry.T[:, :, None]
    last = doc_ids[extent - 1]
    tail = jnp.exp(climb - climb[:, extent - 1:]) * (doc_ids == last).astype(jnp.float32)[None, :] * steps
    kept = jnp.exp(-climb[:, extent - 1]) * (last == doc_prev).astype(jnp.float32)
    fresh = jnp.einsum('hs,shp,sn->hpn', tail, signal, bmat, precision=HIGH)
    return (kept[:, None, None] * state + fresh, output)

def reference(residual, x_in, bc_in, z_in, dt_raw, dt_bias, decay_rate, d_skip, conv_x_weight, conv_x_bias, conv_bc_weight, conv_bc_bias, norm_gain, out_weight, final_gain, lm_weight, targets, doc_lengths):
    positions = jnp.arange(TOKENS, dtype=jnp.int32)
    doc_ids = document_of(positions, doc_lengths)
    margin = KERNEL - 1
    signal = causal_conv(x_in, jnp.zeros((margin, INNER), jnp.bfloat16), conv_x_weight, conv_x_bias, positions, doc_ids, doc_lengths)
    keys_queries = causal_conv(bc_in, jnp.zeros((margin, 2 * STATE), jnp.bfloat16), conv_bc_weight, conv_bc_bias, positions, doc_ids, doc_lengths)
    steps = jax.nn.softplus(dt_raw + dt_bias[:, None])
    blocks = TOKENS // SPAN
    block_starts = jnp.arange(blocks, dtype=jnp.int32) * SPAN
    pieces = (signal.reshape(blocks, SPAN, HEADS, HEAD_SIZE), keys_queries[:, :STATE].reshape(blocks, SPAN, STATE), keys_queries[:, STATE:].reshape(blocks, SPAN, STATE), steps.reshape(HEADS, blocks, SPAN).transpose(1, 0, 2), doc_ids.reshape(blocks, SPAN), document_of(block_starts - 1, doc_lengths))

    def advance(state, piece):
        return span_step(state, piece, decay_rate)
    ignored, outputs = lax.scan(advance, jnp.zeros((HEADS, HEAD_SIZE, STATE), jnp.float32), pieces)
    mixed = outputs.reshape(TOKENS, HEADS, HEAD_SIZE) + d_skip[None, :, None] * signal.reshape(TOKENS, HEADS, HEAD_SIZE).astype(jnp.float32)
    gated = mixed.reshape(TOKENS, INNER) * jax.nn.silu(z_in.astype(jnp.float32))
    scale = lax.rsqrt(lax.optimization_barrier(jnp.sum(gated * gated, axis=1)) / INNER + EPSILON)
    normed = (gated * scale[:, None] * norm_gain.astype(jnp.float32)[None, :]).astype(jnp.bfloat16)
    projected = jnp.dot(normed, out_weight, preferred_element_type=jnp.float32)
    block_out = (residual.astype(jnp.float32) + projected).astype(jnp.bfloat16)
    widened = block_out.astype(jnp.float32)
    final_scale = lax.rsqrt(lax.optimization_barrier(jnp.sum(widened * widened, axis=1)) / D + EPSILON)
    hidden = (widened * final_scale[:, None] * final_gain.astype(jnp.float32)[None, :]).astype(jnp.bfloat16)

    def token_loss(piece):
        hidden_rows, target_rows = piece
        logits = jnp.dot(hidden_rows, lm_weight, preferred_element_type=jnp.float32)
        peak = lax.optimization_barrier(jnp.max(logits, axis=1))
        total = lax.optimization_barrier(jnp.sum(jnp.exp(logits - peak[:, None]), axis=1))
        column = jnp.arange(VOCAB, dtype=jnp.int32)
        picked = lax.optimization_barrier(jnp.sum(jnp.where(column[None, :] == target_rows[:, None], logits, 0.0), axis=1))
        return peak + jnp.log(total) - picked
    losses = lax.map(token_loss, (hidden.reshape(N_SEQ, TOK_DEV, D), targets.reshape(N_SEQ, TOK_DEV))).reshape(TOKENS)
    member = (doc_ids[:, None] == jnp.arange(DOCS, dtype=jnp.int32)[None, :]).astype(jnp.float32)
    sums = jnp.dot(losses, member, precision=HIGH)
    return (block_out, sums / doc_lengths.astype(jnp.float32))
```

```python
import functools

import jax
import jax.numpy as jnp
from jax import lax
from jax.experimental import pallas as pl
from jax.experimental.pallas import tpu as pltpu
from jax.sharding import PartitionSpec as P

D = 2560
HEAD_SIZE = 64
STATE = 128
KERNEL = 4
SPAN = 256
INNER = 5120


EPSILON = 1e-05
HIGH = lax.Precision.HIGHEST
HALF = lax.Precision.HIGH
LOW = -1e30
MESH = pl.DeviceIdType.MESH


def shifted(array, axis, by):
    length = lax.axis_size(axis)
    pairs = [(i, i + by) for i in range(length) if 0 <= i + by < length]
    return lax.ppermute(array, axis, pairs)


def rotated(array, axis, by):
    length = lax.axis_size(axis)
    return lax.ppermute(array, axis, [(i, (i + by) % length) for i in range(length)])


def sibling(array, axis):
    length = lax.axis_size(axis)
    return lax.ppermute(array, axis, [(i, i ^ 1) for i in range(length)])


def scattered_product(normed, weight, axis):
    length = lax.axis_size(axis)
    rank = lax.axis_index(axis)
    chips = length // 2
    share = weight.shape[1] // length

    def columns(core):
        return jnp.concatenate(
            [
                lax.dynamic_slice_in_dim(
                    weight, ((rank // 2 + by) % chips * 2 + core) * share, share, 1
                )
                for by in range(chips)
            ],
            axis=1,
        )

    theirs = columns(1 - rank % 2)
    ours = columns(rank % 2)
    other = jnp.dot(normed, theirs, preferred_element_type=jnp.float32)
    arrived = sibling(other, axis)
    pair = jnp.dot(normed, ours, preferred_element_type=jnp.float32) + arrived
    total = pair[:, :share]
    for by in range(1, chips):
        total = total + rotated(pair[:, by * share : (by + 1) * share], axis, 2 * by)
    return total


def gathered_features(part, axis):
    length = lax.axis_size(axis)
    rank = lax.axis_index(axis)
    chips = length // 2
    rows, share = part.shape
    column = [part] + [rotated(part, axis, 2 * by) for by in range(1, chips)]
    joined = jnp.concatenate(column, axis=1)
    twin = sibling(joined, axis)
    full = jnp.zeros((rows, share * length), part.dtype)
    for by in range(chips):
        source = (rank + 2 * (chips - by)) % length
        piece = slice(by * share, (by + 1) * share)
        full = lax.dynamic_update_slice_in_dim(full, joined[:, piece], source * share, 1)
        full = lax.dynamic_update_slice_in_dim(full, twin[:, piece], (source ^ 1) * share, 1)
    return full


def entering(through, state, axis):
    length = lax.axis_size(axis)
    tag = jnp.broadcast_to(through[:, None, None], (through.shape[0], 8, state.shape[2]))
    packed = shifted(jnp.concatenate([state, tag], axis=1), axis, 1)
    extent = state.shape[1]
    reach = 1
    while reach < length:
        earlier = shifted(packed, axis, reach)
        decay = packed[:, extent : extent + 1, :]
        packed = jnp.concatenate(
            [packed[:, :extent] + decay * earlier[:, :extent], decay * earlier[:, extent:]], axis=1
        )
        reach *= 2
    return packed[:, :extent]


def share_of(array):
    return array.shape[1] % TILE == 0


def document_of(positions, doc_lengths):
    starts = jnp.cumsum(doc_lengths) - doc_lengths
    return jnp.sum((positions[:, None] >= starts[None, :]).astype(jnp.int32), axis=1) - 1


def causal_conv(signal, rim_rows, weight, bias, positions, doc_ids, doc_lengths):
    length = signal.shape[0]
    taps = weight.shape[0]
    joined = jnp.concatenate([rim_rows, signal], axis=0).astype(jnp.float32)
    total = jnp.zeros(signal.shape, jnp.float32) + bias.astype(jnp.float32)[None, :]
    for offset in range(taps):
        lag = taps - 1 - offset
        source = document_of(positions - lag, doc_lengths)
        same = (source == doc_ids).astype(jnp.float32)
        total = (
            total
            + weight[offset].astype(jnp.float32)[None, :]
            * joined[offset : offset + length]
            * same[:, None]
        )
    return jax.nn.silu(total).astype(jnp.bfloat16)


def conv_state_kernel(x_ref, rim_ref, taps_ref, bias_ref, same_ref, cols_ref, bmat_ref, values_ref, state_ref, held):
    length, lanes = x_ref.shape
    taps = taps_ref.shape[0]
    held[0:8, :] = rim_ref[...].astype(jnp.float32)
    held[8:, :] = x_ref[...].astype(jnp.float32)
    total = jnp.zeros((length, lanes), jnp.float32) + bias_ref[...]
    for offset in range(taps):
        lag = taps - 1 - offset
        rows = held[8 - lag : 8 - lag + length, :]
        total = total + taps_ref[offset : offset + 1, :] * rows * same_ref[:, lag : lag + 1]
    values = jax.nn.silu(total).astype(jnp.bfloat16)
    values_ref[...] = values
    first = lax.broadcasted_iota(jnp.int32, (length, lanes), 1) < HEAD_SIZE
    tail = jnp.where(first, cols_ref[0, :, 2:3], cols_ref[0, :, 3:4])
    scaled = values.astype(jnp.float32) * tail
    high = scaled.astype(jnp.bfloat16)
    low = (scaled - high.astype(jnp.float32)).astype(jnp.bfloat16)
    bmat = bmat_ref[...]
    dims = (((0,), (0,)), ((), ()))
    state_ref[...] = lax.dot_general(
        high, bmat, dims, preferred_element_type=jnp.float32
    ) + lax.dot_general(low, bmat, dims, preferred_element_type=jnp.float32)


def within_kernel(values_ref, scores_ref, cols_ref, rows_ref, skip_ref, out_ref):
    length, lanes = values_ref.shape
    for cut in range(0, length, SPAN):
        upto = cut + SPAN
        values = values_ref[0:upto, :]
        scores = scores_ref[cut:upto, 0:upto]
        parts = []
        for which in range(2):
            gap = rows_ref[0, which : which + 1, 0:upto] - cols_ref[0, cut:upto, which : which + 1]
            weights = (
                jnp.exp(jnp.minimum(gap, 0.0)) * scores * rows_ref[0, 2 + which : 3 + which, 0:upto]
            )
            high = weights.astype(jnp.bfloat16)
            low = (weights - high.astype(jnp.float32)).astype(jnp.bfloat16)
            parts.append(
                jnp.dot(high, values, preferred_element_type=jnp.float32)
                + jnp.dot(low, values, preferred_element_type=jnp.float32)
            )
        first = lax.broadcasted_iota(jnp.int32, (SPAN, lanes), 1) < HEAD_SIZE
        own = values_ref[cut:upto, :].astype(jnp.float32)
        out_ref[cut:upto, :] = jnp.where(first, parts[0], parts[1]) + skip_ref[...] * own


def conv_state(x_in, rim, taps, bias, same, cols, bmat):
    length, inner_here = x_in.shape
    lanes = 2 * HEAD_SIZE
    return pl.pallas_call(
        conv_state_kernel,
        grid=(inner_here // lanes,),
        in_specs=[
            pl.BlockSpec((length, lanes), lambda i: (0, i)),
            pl.BlockSpec((8, lanes), lambda i: (0, i)),
            pl.BlockSpec((taps.shape[0], lanes), lambda i: (0, i)),
            pl.BlockSpec((1, lanes), lambda i: (0, i)),
            pl.BlockSpec(same.shape, lambda i: (0, 0)),
            pl.BlockSpec((1, length, 4), lambda i: (i, 0, 0)),
            pl.BlockSpec(bmat.shape, lambda i: (0, 0)),
        ],
        out_specs=[
            pl.BlockSpec((length, lanes), lambda i: (0, i)),
            pl.BlockSpec((lanes, STATE), lambda i: (i, 0)),
        ],
        out_shape=[
            jax.ShapeDtypeStruct((length, inner_here), jnp.bfloat16),
            jax.ShapeDtypeStruct((inner_here, STATE), jnp.float32),
        ],
        scratch_shapes=[pltpu.VMEM((length + 8, lanes), jnp.float32)],
        cost_estimate=pl.CostEstimate(flops=10**9, bytes_accessed=6 * 10**6, transcendentals=10**6),
    )(x_in, rim, taps, bias, same, cols, bmat)


def within(values, scores, cols, rows, skip):
    length, inner_here = values.shape
    lanes = 2 * HEAD_SIZE
    return pl.pallas_call(
        within_kernel,
        grid=(inner_here // lanes,),
        in_specs=[
            pl.BlockSpec((length, lanes), lambda i: (0, i)),
            pl.BlockSpec(scores.shape, lambda i: (0, 0)),
            pl.BlockSpec((1, length, 4), lambda i: (i, 0, 0)),
            pl.BlockSpec((1, 4, length), lambda i: (i, 0, 0)),
            pl.BlockSpec((1, lanes), lambda i: (0, i)),
        ],
        out_specs=pl.BlockSpec((length, lanes), lambda i: (0, i)),
        out_shape=jax.ShapeDtypeStruct((length, inner_here), jnp.float32),
        cost_estimate=pl.CostEstimate(flops=8 * 10**9, bytes_accessed=20 * 10**6, transcendentals=10**7),
    )(values, scores, cols, rows, skip)


TAIL_ROWS = 256
TILE = 128


def tail_kernel(
    n, heads, first_of, hid_ref, tgt_ref, member_ref, w_ref, out_ref,
    full, w_buf, tgts, marks, parts, sums,
    w_sem, along_send, side_send, arrive, tgt_send, tgt_recv, mark_send, mark_recv, sum_send, sum_recv,
):
    z = lax.axis_index("seq")
    h = lax.axis_index("head")
    rows, share = hid_ref.shape
    width = w_ref.shape[1]
    total_peers = n * heads
    me = z * heads + h
    twin = h + 1 - 2 * lax.rem(h, 2)
    side = lax.rem(h + 2, heads)

    load = pltpu.make_async_copy(w_ref, w_buf, w_sem)
    load.start()
    barrier = pltpu.get_barrier_semaphore()

    def peer(k):
        flat = lax.rem(me + k, total_peers)
        return flat // heads, lax.rem(flat, heads)

    @pl.loop(1, total_peers)
    def _(k):
        there, where_head = peer(k)
        pl.semaphore_signal(
            barrier, inc=1, device_id={"seq": there, "head": where_head}, device_id_type=MESH
        )

    pl.semaphore_wait(barrier, total_peers - 1)

    def slot(block, head):
        return full.at[block, :, pl.ds(pl.multiple_of(head * share, TILE), share)]

    def ship(kind, block, head, target, source=None):
        sem = along_send if kind < 2 else side_send
        return pltpu.make_async_remote_copy(
            src_ref=slot(block, head) if source is None else source,
            dst_ref=slot(block, head),
            send_sem=sem.at[kind % 2, block, head] if kind < 2 else sem.at[kind - 2, block, head],
            recv_sem=arrive.at[block, head],
            device_id=target,
            device_id_type=MESH,
        )

    def right(block, source=None):
        return ship(0, block, h, {"seq": z + 1}, source)

    def left(block, source=None):
        return ship(1, block, h, {"seq": z - 1}, source)

    def across(block, source=None):
        return ship(2, block, h, {"head": side}, source)

    def twinned(block, head, source=None):
        return ship(3, block, head, {"head": twin}, source)

    def arrived(block, head):
        ship(0, block, head, {"head": twin}).wait_recv()

    def tell(k):
        return pltpu.make_async_remote_copy(
            src_ref=tgt_ref,
            dst_ref=tgts.at[z],
            send_sem=tgt_send.at[k],
            recv_sem=tgt_recv.at[z],
            device_id={"seq": lax.rem(z + k, n)},
            device_id_type=MESH,
        )

    across(z, hid_ref).start()

    @pl.when(z < n - 1)
    def _():
        right(z, hid_ref).start()

    @pl.when(z > 0)
    def _():
        left(z, hid_ref).start()

    twinned(z, h, hid_ref).start()
    for k in range(1, n):
        tell(k).start()
    tgts[z] = tgt_ref[...]
    full[z, :, pl.ds(pl.multiple_of(h * share, TILE), share)] = hid_ref[...]
    load.wait()

    def mark_copy(block, head):
        return pltpu.make_async_remote_copy(
            src_ref=marks.at[block, :, pl.ds(pl.multiple_of(head * TILE, TILE), TILE)],
            dst_ref=parts.at[me],
            send_sem=mark_send.at[block, head],
            recv_sem=mark_recv.at[me],
            device_id={"seq": block, "head": head},
            device_id_type=MESH,
        )

    def compute(block):
        dead, first = first_of(z, h, width)

        @pl.loop(0, rows // TAIL_ROWS)
        def _(step):
            at = pl.multiple_of(step * TAIL_ROWS, TAIL_ROWS)
            logits = jnp.dot(
                full[block, pl.ds(at, TAIL_ROWS), :], w_buf[...], preferred_element_type=jnp.float32
            )
            wanted = tgts[block, 0:1, pl.ds(at, TAIL_ROWS)]
            wanted = jnp.transpose(jnp.broadcast_to(wanted, (TILE, TAIL_ROWS))) - first
            lane = lax.broadcasted_iota(jnp.int32, (TAIL_ROWS, TILE), 1)
            pieces = []
            for cut in range(0, width, TILE):
                piece = logits[:, cut : cut + TILE]
                pieces.append(jnp.where(lane + cut >= dead, piece, LOW))
            peak = pieces[0]
            for piece in pieces[1:]:
                peak = jnp.maximum(peak, piece)
            peak = jnp.max(peak, axis=1, keepdims=True)
            total = jnp.zeros((TAIL_ROWS, TILE), jnp.float32)
            picked = jnp.zeros((TAIL_ROWS, TILE), jnp.float32)
            for index, piece in enumerate(pieces):
                total = total + jnp.exp(piece - peak)
                here = (lane + index * TILE == wanted) & (lane + index * TILE >= dead)
                picked = picked + jnp.where(here, piece, 0.0)
            total = jnp.sum(total, axis=1, keepdims=True)
            picked = jnp.sum(picked, axis=1, keepdims=True)
            tile = jnp.where(lane == 0, peak, jnp.where(lane == 1, total, picked))
            marks[block, :, pl.ds(at, TAIL_ROWS)] = jnp.transpose(tile)[0:8, :]

        @pl.loop(0, heads)
        def _(head):
            @pl.when((block != z) | (head != h))
            def _():
                mark_copy(block, head).start()

    def finish(block):
        arrived(block, side)
        twinned(block, side).start()
        arrived(block, twin)
        arrived(block, lax.rem(twin + 2, heads))
        compute(block)

    for step in range(1, n):
        @pl.when(z >= step)
        def _():
            block = z - step
            arrived(block, h)

            @pl.when(z < n - 1)
            def _():
                right(block).start()

            across(block).start()
            twinned(block, h).start()

        @pl.when(z + step < n)
        def _():
            block = z + step
            arrived(block, h)

            @pl.when(z > 0)
            def _():
                left(block).start()

            across(block).start()
            twinned(block, h).start()

        if step == 1:
            for k in range(1, n):
                source = lax.rem(z + n - k, n)
                pltpu.make_async_remote_copy(
                    src_ref=tgt_ref,
                    dst_ref=tgts.at[source],
                    send_sem=tgt_send.at[k],
                    recv_sem=tgt_recv.at[source],
                    device_id={"seq": lax.rem(z + k, n)},
                    device_id_type=MESH,
                ).wait()
            finish(z)
        else:
            @pl.when(z >= step - 1)
            def _():
                finish(z - step + 1)

            @pl.when(z + step - 1 < n)
            def _():
                finish(z + step - 1)

    if n > 1:
        @pl.when(z >= n - 1)
        def _():
            finish(z - n + 1)

        @pl.when(z + n - 1 < n)
        def _():
            finish(z + n - 1)

    parts[me] = marks[z, :, pl.ds(pl.multiple_of(h * TILE, TILE), TILE)]

    def mark_arrival(k):
        there, where_head = peer(k)
        flat = there * heads + where_head
        pltpu.make_async_remote_copy(
            src_ref=parts.at[flat],
            dst_ref=parts.at[flat],
            send_sem=mark_send.at[there, where_head],
            recv_sem=mark_recv.at[flat],
            device_id={"seq": there, "head": where_head},
            device_id_type=MESH,
        ).wait()

    @pl.loop(1, total_peers)
    def _(k):
        mark_arrival(k)

    peak = parts[0, 0:1, :]
    for flat in range(1, total_peers):
        peak = jnp.maximum(peak, parts[flat, 0:1, :])
    total = jnp.zeros((1, TILE), jnp.float32)
    picked = jnp.zeros((1, TILE), jnp.float32)
    for flat in range(total_peers):
        total = total + parts[flat, 1:2, :] * jnp.exp(parts[flat, 0:1, :] - peak)
        picked = picked + parts[flat, 2:3, :]
    losses = peak + jnp.log(total) - picked
    mine = jnp.sum(member_ref[...] * losses, axis=1, keepdims=True)
    sums[me] = jnp.broadcast_to(mine, sums.shape[1:])

    def sum_copy(k, slot_of):
        there, where_head = peer(k)
        return pltpu.make_async_remote_copy(
            src_ref=sums.at[slot_of],
            dst_ref=sums.at[slot_of],
            send_sem=sum_send.at[k],
            recv_sem=sum_recv.at[slot_of],
            device_id={"seq": there, "head": where_head},
            device_id_type=MESH,
        )

    @pl.loop(1, total_peers)
    def _(k):
        sum_copy(k, me).start()

    for block in range(n):
        @pl.when((z < n - 1) & (z >= block))
        def _():
            right(block).wait_send()

        @pl.when((z > 0) & (z <= block))
        def _():
            left(block).wait_send()

        across(block).wait_send()
        twinned(block, h).wait_send()
        twinned(block, side).wait_send()

    @pl.loop(1, total_peers)
    def _(k):
        sum_copy(k, lax.rem(me + k, total_peers)).wait()

    grand = sums[0]
    for flat in range(1, total_peers):
        grand = grand + sums[flat]
    out_ref[...] = grand


def loss_stage(hidden_part, targets_row, member, weight, n, heads, first_of):
    rows, _ = hidden_part.shape
    deep, width = weight.shape
    peers = n * heads
    dma = pltpu.SemaphoreType.DMA
    flops = 2 * n * rows * deep * width
    return pl.pallas_call(
        functools.partial(tail_kernel, n, heads, first_of),
        out_shape=jax.ShapeDtypeStruct(member.shape, jnp.float32),
        in_specs=[pl.BlockSpec(memory_space=pltpu.VMEM)] * 3 + [pl.BlockSpec(memory_space=pl.ANY)],
        out_specs=pl.BlockSpec(memory_space=pltpu.VMEM),
        scratch_shapes=[
            pltpu.VMEM((n, rows, deep), jnp.bfloat16),
            pltpu.VMEM((deep, width), jnp.bfloat16),
            pltpu.VMEM((n, 8, rows), jnp.int32),
            pltpu.VMEM((n, 8, rows), jnp.float32),
            pltpu.VMEM((peers, 8, TILE), jnp.float32),
            pltpu.VMEM((peers,) + member.shape, jnp.float32),
            dma,
            dma((2, n, heads)),
            dma((2, n, heads)),
            dma((n, heads)),
            dma((n,)),
            dma((n,)),
            dma((n, heads)),
            dma((peers,)),
            dma((peers,)),
            dma((peers,)),
        ],
        compiler_params=pltpu.CompilerParams(
            collective_id=0, has_side_effects=True, vmem_limit_bytes=60 * 2**20
        ),
        cost_estimate=pl.CostEstimate(
            flops=flops, bytes_accessed=deep * width * 2, transcendentals=n * rows * width
        ),
    )(hidden_part, targets_row, member, weight)


def local(
    residual,
    x_in,
    bc_in,
    z_in,
    dt_raw,
    dt_bias,
    decay_rate,
    d_skip,
    conv_x_weight,
    conv_x_bias,
    conv_bc_weight,
    conv_bc_bias,
    norm_gain,
    out_weight,
    final_gain,
    lm_weight,
    targets,
    doc_lengths,
):
    length = x_in.shape[0]
    inner_here = x_in.shape[1]
    heads_here = dt_raw.shape[0]
    seq_rank = lax.axis_index("seq")
    head_rank = lax.axis_index("head")
    offset_here = seq_rank * length
    positions = offset_here + jnp.arange(length, dtype=jnp.int32)
    doc_ids = document_of(positions, doc_lengths)
    columns_here = lm_weight.shape[1]
    devices = lax.axis_size("seq")
    width = -(-columns_here // (devices * 128)) * 128

    def window(rank):
        return jnp.minimum(rank * width, columns_here - width)

    depth = lm_weight.shape[0]
    vocab_weight = jnp.zeros((depth * devices, width), lm_weight.dtype)
    group = lax.axis_index("groups")
    groups = lax.axis_size("groups")
    band = depth // groups
    pieces = [
        lax.dynamic_slice(
            lm_weight, (group * band, window((seq_rank + by) % devices)), (band, width)
        )
        for by in range(1, devices)
    ]
    heads = lax.axis_size("head")
    room = 2 * (devices * length * D + D * width) < 40 * 2**20
    fused = room and heads == 4 and length == heads * TILE and share_of(residual) and devices > 1
    aims = [targets]
    for by in range(1, 1 if fused else devices):
        aims.append(rotated(targets, "seq", by))
    margin = KERNEL - 1
    rims = shifted(
        jnp.concatenate([x_in[length - margin :], bc_in[length - margin :]], axis=1), "seq", 1
    )
    x_rim, bc_rim = rims[:, :inner_here], rims[:, inner_here:]
    keys_queries = causal_conv(
        bc_in, bc_rim, conv_bc_weight, conv_bc_bias, positions, doc_ids, doc_lengths
    )
    bmat, cmat = keys_queries[:, :STATE], keys_queries[:, STATE:]
    steps = jax.nn.softplus(dt_raw + dt_bias[:, None])
    climb = jnp.cumsum(steps * decay_rate[:, None], axis=1)
    before = document_of(jnp.reshape(offset_here - 1, (1,)), doc_lengths)[0]
    carried = (doc_ids == before).astype(jnp.float32)
    through = jnp.exp(-climb[:, length - 1]) * carried[length - 1]
    same = jnp.stack(
        [
            (document_of(positions - lag, doc_lengths) == doc_ids).astype(jnp.float32)
            for lag in range(KERNEL)
        ],
        axis=1,
    )
    last = (doc_ids == doc_ids[length - 1]).astype(jnp.float32)
    tail = jnp.exp(climb - climb[:, length - 1 :]) * last[None, :] * steps
    couples = heads_here // 2
    rows = jnp.concatenate(
        [climb.reshape(couples, 2, length), steps.reshape(couples, 2, length)], axis=1
    )
    cols = jnp.concatenate(
        [climb.reshape(couples, 2, length), tail.reshape(couples, 2, length)], axis=1
    ).transpose(0, 2, 1)
    rim = jnp.concatenate([jnp.zeros((8 - margin, inner_here), x_rim.dtype), x_rim], axis=0)
    values, own_end = conv_state(
        x_in,
        rim,
        conv_x_weight.astype(jnp.float32),
        conv_x_bias.astype(jnp.float32)[None, :],
        same,
        cols,
        bmat,
    )
    of_head = jnp.arange(inner_here, dtype=jnp.int32)[None, :] // HEAD_SIZE
    spread = (of_head == jnp.arange(heads_here, dtype=jnp.int32)[:, None]).astype(jnp.float32)
    incoming = entering(
        through, own_end.reshape(heads_here, HEAD_SIZE, STATE), "seq"
    ).reshape(inner_here, STATE)
    held_back = lax.optimization_barrier(tuple(pieces[1:]) + (incoming,))
    pieces, incoming = pieces[:1] + list(held_back[:-1]), held_back[-1]
    arrivals = []
    for by in range(1, devices):
        arrivals.append(rotated(pieces[by - 1], "seq", by))
    bands = []
    for by in range(1, devices):
        bands.append(
            [arrivals[by - 1]]
            + [rotated(arrivals[by - 1], "groups", hop) for hop in range(1, groups)]
        )
    order = jnp.arange(length, dtype=jnp.int32)
    inside = (doc_ids[:, None] == doc_ids[None, :]) & (order[:, None] >= order[None, :])
    scores = jnp.where(
        inside,
        lax.dot_general(
            cmat, bmat, (((1,), (1,)), ((), ())), preferred_element_type=jnp.float32
        ),
        0.0,
    )
    skip = jnp.dot(d_skip[None, :], spread, precision=HIGH)
    output = within(values, scores, cols, rows, skip)
    entry = jnp.dot((jnp.exp(-climb) * carried[None, :]).T, spread, precision=HIGH)
    arriving = lax.dot_general(
        cmat.astype(jnp.float32), incoming, (((1,), (1,)), ((), ())), precision=HALF
    )
    gated = (output + arriving * entry) * jax.nn.silu(z_in.astype(jnp.float32))
    square_sum = lax.psum(jnp.sum(gated * gated, axis=1), "head")
    scale = lax.rsqrt(square_sum / INNER + EPSILON)
    normed = (gated * scale[:, None] * norm_gain.astype(jnp.float32)[None, :]).astype(jnp.bfloat16)
    share = residual.shape[1]
    projected = scattered_product(normed, out_weight, "head")
    block_out = (residual.astype(jnp.float32) + projected).astype(jnp.bfloat16)
    widened = block_out.astype(jnp.float32)
    square_total = lax.psum(jnp.sum(widened * widened, axis=1), "head")
    gain_part = lax.dynamic_slice_in_dim(final_gain, head_rank * share, share, 0)
    final_scale = lax.rsqrt(square_total / D + EPSILON)
    hidden_part = (widened * final_scale[:, None] * gain_part.astype(jnp.float32)[None, :]).astype(
        jnp.bfloat16
    )
    own = lax.dynamic_slice_in_dim(lm_weight, window(seq_rank), width, 1)
    vocab_weight = lax.dynamic_update_slice_in_dim(vocab_weight, own, seq_rank * depth, 0)
    for by in range(1, devices):
        source = (seq_rank + devices - by) % devices
        for hop in range(groups):
            start = source * depth + (group + groups - hop) % groups * band
            vocab_weight = lax.dynamic_update_slice_in_dim(
                vocab_weight, bands[by - 1][hop], start, 0
            )
    if fused:
        documents = -(-doc_lengths.shape[0] // 8) * 8
        own_ids = lax.dynamic_slice_in_dim(doc_ids, head_rank * TILE, TILE, 0)
        member = (own_ids[None, :] == jnp.arange(documents, dtype=jnp.int32)[:, None]).astype(
            jnp.float32
        )

        def first_of(z, h, wide):
            start = jnp.minimum(z * wide, columns_here - wide)
            return z * wide - start, h * columns_here + start

        row = jnp.broadcast_to(targets[None, :], (8, length))
        sums = loss_stage(hidden_part, row, member, vocab_weight, devices, heads, first_of)
        sums = sums[: doc_lengths.shape[0], 0]
        return (block_out, sums / doc_lengths.astype(jnp.float32))
    column = jnp.arange(width, dtype=jnp.int32)
    first = head_rank * columns_here + window(seq_rank)
    live = column + window(seq_rank) >= seq_rank * width
    marks = jnp.zeros((3, length * devices), jnp.float32)
    for by in range(devices):
        source = (seq_rank + devices - by) % devices
        if by and by % 4 == 0:
            hidden_part, marks = lax.optimization_barrier((hidden_part, marks))
        rows = rotated(hidden_part, "seq", by) if by else hidden_part
        hidden = gathered_features(rows, "head")
        logits = jnp.dot(hidden, vocab_weight, preferred_element_type=jnp.float32)
        logits = jnp.where(live[None, :], logits, LOW)
        peak = jnp.max(logits, axis=1)
        wanted = aims[by] - first
        total = jnp.sum(jnp.exp(logits - peak[:, None]), axis=1)
        picked = jnp.sum(
            jnp.where((column[None, :] == wanted[:, None]) & live[None, :], logits, 0.0), axis=1
        )
        marks = lax.dynamic_update_slice_in_dim(
            marks, jnp.stack([peak, total, picked]), source * length, 1
        )
    for axis in ("head", "seq"):
        every_mark = lax.all_gather(marks, axis)
        peak = jnp.max(every_mark[:, 0], axis=0)
        total = jnp.sum(every_mark[:, 1] * jnp.exp(every_mark[:, 0] - peak[None]), axis=0)
        marks = jnp.stack([peak, total, jnp.sum(every_mark[:, 2], axis=0)])
    losses = marks[0] + jnp.log(marks[1]) - marks[2]
    every = document_of(jnp.arange(length * devices, dtype=jnp.int32), doc_lengths)
    documents = jnp.arange(doc_lengths.shape[0], dtype=jnp.int32)
    member = every[None, :] == documents[:, None]
    sums = jnp.sum(jnp.where(member, losses[None, :], 0.0), axis=1)
    return (block_out, sums / doc_lengths.astype(jnp.float32))


def solution(mesh):
    in_specs = (
        P(("groups", "seq"), "head"),
        P(("groups", "seq"), "head"),
        P(("groups", "seq"), None),
        P(("groups", "seq"), "head"),
        P("head", ("groups", "seq")),
        P("head"),
        P("head"),
        P("head"),
        P(None, "head"),
        P("head"),
        P(),
        P(),
        P("head"),
        P("head", None),
        P(),
        P("seq", "head"),
        P(("groups", "seq")),
        P("groups"),
    )
    out_specs = (P(("groups", "seq"), "head"), P("groups"))


    return jax.shard_map(local, mesh=mesh, in_specs=in_specs, out_specs=out_specs, check_vma=False)
```

```python
import functools

import jax
import jax.numpy as jnp
from jax import lax
from jax.experimental import pallas as pl
from jax.experimental.pallas import tpu as pltpu
from jax.sharding import PartitionSpec as P

D = 2560
HEAD_SIZE = 64
STATE = 128
KERNEL = 4
SPAN = 256
INNER = 5120


EPSILON = 1e-05
HIGH = lax.Precision.HIGHEST
HALF = lax.Precision.HIGH
LOW = -1e30
MESH = pl.DeviceIdType.MESH


def shifted(array, axis, by):
    length = lax.axis_size(axis)
    pairs = [(i, i + by) for i in range(length) if 0 <= i + by < length]
    return lax.ppermute(array, axis, pairs)


def rotated(array, axis, by):
    length = lax.axis_size(axis)
    return lax.ppermute(array, axis, [(i, (i + by) % length) for i in range(length)])


def sibling(array, axis):
    length = lax.axis_size(axis)
    return lax.ppermute(array, axis, [(i, i ^ 1) for i in range(length)])


def scattered_product(normed, weight, axis):
    length = lax.axis_size(axis)
    rank = lax.axis_index(axis)
    chips = length // 2
    share = weight.shape[1] // length

    def columns(core):
        return jnp.concatenate(
            [
                lax.dynamic_slice_in_dim(
                    weight, ((rank // 2 + by) % chips * 2 + core) * share, share, 1
                )
                for by in range(chips)
            ],
            axis=1,
        )

    theirs = columns(1 - rank % 2)
    ours = columns(rank % 2)
    other = jnp.dot(normed, theirs, preferred_element_type=jnp.float32)
    arrived = sibling(other, axis)
    pair = jnp.dot(normed, ours, preferred_element_type=jnp.float32) + arrived
    total = pair[:, :share]
    for by in range(1, chips):
        total = total + rotated(pair[:, by * share : (by + 1) * share], axis, 2 * by)
    return total


def gathered_features(part, axis):
    length = lax.axis_size(axis)
    rank = lax.axis_index(axis)
    chips = length // 2
    rows, share = part.shape
    column = [part] + [rotated(part, axis, 2 * by) for by in range(1, chips)]
    joined = jnp.concatenate(column, axis=1)
    twin = sibling(joined, axis)
    full = jnp.zeros((rows, share * length), part.dtype)
    for by in range(chips):
        source = (rank + 2 * (chips - by)) % length
        piece = slice(by * share, (by + 1) * share)
        full = lax.dynamic_update_slice_in_dim(full, joined[:, piece], source * share, 1)
        full = lax.dynamic_update_slice_in_dim(full, twin[:, piece], (source ^ 1) * share, 1)
    return full


def entering(through, state, axis):
    length = lax.axis_size(axis)
    tag = jnp.broadcast_to(through[:, None, None], (through.shape[0], 8, state.shape[2]))
    packed = shifted(jnp.concatenate([state, tag], axis=1), axis, 1)
    extent = state.shape[1]
    reach = 1
    while reach < length:
        earlier = shifted(packed, axis, reach)
        decay = packed[:, extent : extent + 1, :]
        packed = jnp.concatenate(
            [packed[:, :extent] + decay * earlier[:, :extent], decay * earlier[:, extent:]], axis=1
        )
        reach *= 2
    return packed[:, :extent]


def document_of(positions, doc_lengths):
    starts = jnp.cumsum(doc_lengths) - doc_lengths
    return jnp.sum((positions[:, None] >= starts[None, :]).astype(jnp.int32), axis=1) - 1


def causal_conv(signal, rim_rows, weight, bias, positions, doc_ids, doc_lengths):
    length = signal.shape[0]
    taps = weight.shape[0]
    joined = jnp.concatenate([rim_rows, signal], axis=0).astype(jnp.float32)
    total = jnp.zeros(signal.shape, jnp.float32) + bias.astype(jnp.float32)[None, :]
    for offset in range(taps):
        lag = taps - 1 - offset
        source = document_of(positions - lag, doc_lengths)
        same = (source == doc_ids).astype(jnp.float32)
        total = (
            total
            + weight[offset].astype(jnp.float32)[None, :]
            * joined[offset : offset + length]
            * same[:, None]
        )
    return jax.nn.silu(total).astype(jnp.bfloat16)


def conv_state_kernel(x_ref, rim_ref, taps_ref, bias_ref, same_ref, cols_ref, bmat_ref, values_ref, state_ref, held):
    length, lanes = x_ref.shape
    taps = taps_ref.shape[0]
    held[0:8, :] = rim_ref[...].astype(jnp.float32)
    held[8:, :] = x_ref[...].astype(jnp.float32)
    total = jnp.zeros((length, lanes), jnp.float32) + bias_ref[...]
    for offset in range(taps):
        lag = taps - 1 - offset
        rows = held[8 - lag : 8 - lag + length, :]
        total = total + taps_ref[offset : offset + 1, :] * rows * same_ref[:, lag : lag + 1]
    values = jax.nn.silu(total).astype(jnp.bfloat16)
    values_ref[...] = values
    first = lax.broadcasted_iota(jnp.int32, (length, lanes), 1) < HEAD_SIZE
    tail = jnp.where(first, cols_ref[0, :, 2:3], cols_ref[0, :, 3:4])
    scaled = values.astype(jnp.float32) * tail
    high = scaled.astype(jnp.bfloat16)
    low = (scaled - high.astype(jnp.float32)).astype(jnp.bfloat16)
    bmat = bmat_ref[...]
    dims = (((0,), (0,)), ((), ()))
    state_ref[...] = lax.dot_general(
        high, bmat, dims, preferred_element_type=jnp.float32
    ) + lax.dot_general(low, bmat, dims, preferred_element_type=jnp.float32)


def within_kernel(values_ref, scores_ref, cols_ref, rows_ref, skip_ref, out_ref):
    length, lanes = values_ref.shape
    for cut in range(0, length, SPAN):
        upto = cut + SPAN
        values = values_ref[0:upto, :]
        scores = scores_ref[cut:upto, 0:upto]
        parts = []
        for which in range(2):
            gap = rows_ref[0, which : which + 1, 0:upto] - cols_ref[0, cut:upto, which : which + 1]
            weights = (
                jnp.exp(jnp.minimum(gap, 0.0)) * scores * rows_ref[0, 2 + which : 3 + which, 0:upto]
            )
            high = weights.astype(jnp.bfloat16)
            low = (weights - high.astype(jnp.float32)).astype(jnp.bfloat16)
            parts.append(
                jnp.dot(high, values, preferred_element_type=jnp.float32)
                + jnp.dot(low, values, preferred_element_type=jnp.float32)
            )
        first = lax.broadcasted_iota(jnp.int32, (SPAN, lanes), 1) < HEAD_SIZE
        own = values_ref[cut:upto, :].astype(jnp.float32)
        out_ref[cut:upto, :] = jnp.where(first, parts[0], parts[1]) + skip_ref[...] * own


def conv_state(x_in, rim, taps, bias, same, cols, bmat):
    length, inner_here = x_in.shape
    lanes = 2 * HEAD_SIZE
    return pl.pallas_call(
        conv_state_kernel,
        grid=(inner_here // lanes,),
        in_specs=[
            pl.BlockSpec((length, lanes), lambda i: (0, i)),
            pl.BlockSpec((8, lanes), lambda i: (0, i)),
            pl.BlockSpec((taps.shape[0], lanes), lambda i: (0, i)),
            pl.BlockSpec((1, lanes), lambda i: (0, i)),
            pl.BlockSpec(same.shape, lambda i: (0, 0)),
            pl.BlockSpec((1, length, 4), lambda i: (i, 0, 0)),
            pl.BlockSpec(bmat.shape, lambda i: (0, 0)),
        ],
        out_specs=[
            pl.BlockSpec((length, lanes), lambda i: (0, i)),
            pl.BlockSpec((lanes, STATE), lambda i: (i, 0)),
        ],
        out_shape=[
            jax.ShapeDtypeStruct((length, inner_here), jnp.bfloat16),
            jax.ShapeDtypeStruct((inner_here, STATE), jnp.float32),
        ],
        scratch_shapes=[pltpu.VMEM((length + 8, lanes), jnp.float32)],
        cost_estimate=pl.CostEstimate(flops=10**9, bytes_accessed=6 * 10**6, transcendentals=10**6),
    )(x_in, rim, taps, bias, same, cols, bmat)


def within(values, scores, cols, rows, skip):
    length, inner_here = values.shape
    lanes = 2 * HEAD_SIZE
    return pl.pallas_call(
        within_kernel,
        grid=(inner_here // lanes,),
        in_specs=[
            pl.BlockSpec((length, lanes), lambda i: (0, i)),
            pl.BlockSpec(scores.shape, lambda i: (0, 0)),
            pl.BlockSpec((1, length, 4), lambda i: (i, 0, 0)),
            pl.BlockSpec((1, 4, length), lambda i: (i, 0, 0)),
            pl.BlockSpec((1, lanes), lambda i: (0, i)),
        ],
        out_specs=pl.BlockSpec((length, lanes), lambda i: (0, i)),
        out_shape=jax.ShapeDtypeStruct((length, inner_here), jnp.float32),
        cost_estimate=pl.CostEstimate(flops=8 * 10**9, bytes_accessed=20 * 10**6, transcendentals=10**7),
    )(values, scores, cols, rows, skip)


TILE = 128
LOSS_ROWS = 256
HALO = 16
PARTS = 2


def block_kernel(
    n, heads, groups, inner, features,
    x_ref, z_ref, bc_ref, taps_ref, bias_ref, bc_taps_ref, bc_bias_ref, cols_ref, rows_ref,
    same_ref, doc_ref, skip_ref, gain_ref, res_ref, final_ref, tgt_ref, member_ref, ow_ref, lm_ref,
    block_ref, out_ref,
    ow_buf, w_buf, full, tgts, marks, parts, sums, halo_x, halo_bc, held, masks, values, keys,
    scores, state_out, state_in, gated, squares, tiles, normed, share_out, share_in, hid,
    load_sem, halo_send, halo_recv, w_send, w_recv, y_send, y_recv, state_send, state_recv,
    tile_send, tile_recv, share_send, share_recv,
    along_send, side_send, arrive, tgt_send, tgt_recv, mark_send, mark_recv, sum_send, sum_recv,
):
    g = lax.axis_index("groups")
    z = lax.axis_index("seq")
    h = lax.axis_index("head")
    length, inner_here = x_ref.shape
    share = res_ref.shape[1]
    depth, columns = lm_ref.shape
    width = w_buf.shape[1]
    band = depth // groups
    sub = band // PARTS
    total_peers = n * heads
    me = z * heads + h
    twin = h + 1 - 2 * lax.rem(h, 2)
    side = lax.rem(h + 2, heads)
    chunks = inner_here // TILE

    def remote(src, dst, send, recv, target):
        return pltpu.make_async_remote_copy(
            src_ref=src, dst_ref=dst, send_sem=send, recv_sem=recv,
            device_id=target, device_id_type=MESH,
        )

    def window(rank):
        return pl.multiple_of(rank * width - rank // (n - 1) * (n * width - columns), TILE)

    def peer(k):
        flat = lax.rem(me + k, total_peers)
        return flat // heads, lax.rem(flat, heads)

    load_out = pltpu.make_async_copy(ow_ref, ow_buf, load_sem.at[0])
    load_own = pltpu.make_async_copy(
        lm_ref.at[:, pl.ds(window(z), width)],
        w_buf.at[pl.ds(pl.multiple_of(z * depth, 16), depth), :],
        load_sem.at[1],
    )
    load_out.start()
    load_own.start()

    barrier = pltpu.get_barrier_semaphore()

    @pl.loop(1, total_peers)
    def _(k):
        there, where_head = peer(k)
        pl.semaphore_signal(
            barrier, inc=1, device_id={"seq": there, "head": where_head}, device_id_type=MESH
        )

    for hop in range(1, groups):
        pl.semaphore_signal(
            barrier, inc=1, device_id={"groups": lax.rem(g + hop, groups)}, device_id_type=MESH
        )
    pl.semaphore_wait(barrier, total_peers - 1 + groups - 1)

    def halo_copies():
        tail_rows = pl.ds(length - HALO, HALO)
        return [
            remote(x_ref.at[tail_rows, :], halo_x, halo_send.at[0], halo_recv.at[0], {"seq": z + 1}),
            remote(bc_ref.at[tail_rows, :], halo_bc, halo_send.at[1], halo_recv.at[1], {"seq": z + 1}),
        ]

    @pl.when(z < n - 1)
    def _():
        for copy in halo_copies():
            copy.start()

    def w_rows(source, group, part):
        return pl.ds(pl.multiple_of(source * depth + group * band + part * sub, 16), sub)

    def w_copy(k, part):
        there = lax.rem(z + k, n)
        return remote(
            lm_ref.at[pl.ds(pl.multiple_of(g * band + part * sub, 16), sub), pl.ds(window(there), width)],
            w_buf.at[w_rows(z, g, part), :],
            w_send.at[k, part],
            w_recv.at[z, part],
            {"seq": there},
        )

    def w_forward(source, part, hop):
        place = w_buf.at[w_rows(source, g, part), :]
        return remote(
            place, place, y_send.at[source, part, hop], y_recv.at[g, source, part],
            {"groups": lax.rem(g + hop, groups)},
        )

    def w_pass_on(k, part):
        source = lax.rem(z + n - k, n)
        place = w_buf.at[w_rows(source, g, part), :]
        remote(place, place, w_send.at[k, part], w_recv.at[source, part], {"seq": source}).wait_recv()
        for hop in range(1, groups):
            w_forward(source, part, hop).start()

    def w_start(k):
        for part in range(PARTS):
            w_copy(k, part).start()

    w_start(1)
    for k in range(2, n):
        @pl.when(z + k >= n)
        def _():
            w_start(k)

    def tell(k, source):
        return remote(
            tgt_ref, tgts.at[source], tgt_send.at[k], tgt_recv.at[source],
            {"seq": lax.rem(z + k, n)},
        )

    for k in range(1, n):
        tell(k, z).start()
    tgts[z] = tgt_ref[...]

    for lag in range(1, KERNEL):
        masks[lag - 1] = jnp.broadcast_to(same_ref[:, lag : lag + 1], (length, TILE))

    @pl.when(z == 0)
    def _():
        halo_x[...] = jnp.zeros_like(halo_x)
        halo_bc[...] = jnp.zeros_like(halo_bc)
        state_in[...] = jnp.zeros_like(state_in)

    @pl.when(z > 0)
    def _():
        for copy in halo_copies():
            copy.wait_recv()

    def convolved(signal, halo, weight, bias, lanes):
        held[0:HALO, :] = halo[:, lanes].astype(jnp.float32)
        held[HALO:, :] = signal[:, lanes].astype(jnp.float32)
        total = jnp.zeros((length, TILE), jnp.float32) + bias[:, lanes]
        for offset in range(KERNEL):
            lag = KERNEL - 1 - offset
            term = weight[offset : offset + 1, lanes] * held[HALO - lag : HALO - lag + length, :]
            total = total + (term * masks[lag - 1] if lag else term)
        return jax.nn.silu(total).astype(jnp.bfloat16)

    for half in range(2):
        lanes = pl.ds(half * STATE, STATE)
        keys[:, lanes] = convolved(bc_ref, halo_bc, bc_taps_ref, bc_bias_ref, lanes)
    nt = (((1,), (1,)), ((), ()))
    for cut in range(0, length, SPAN):
        near = pl.ds(cut, SPAN)
        inside = (same_ref[near, 5:6] == doc_ref[0:1, :]) & (
            lax.broadcasted_iota(jnp.int32, (SPAN, length), 0) + cut
            >= lax.broadcasted_iota(jnp.int32, (SPAN, length), 1)
        )
        product = lax.dot_general(
            keys[near, STATE:], keys[:, :STATE], nt, preferred_element_type=jnp.float32
        )
        scores[near, :] = jnp.where(inside, product, 0.0)

    def state_copy(c):
        return remote(
            state_out.at[c], state_in.at[c], state_send.at[c], state_recv.at[c], {"seq": z + 1}
        )

    first = lax.broadcasted_iota(jnp.int32, (SPAN, TILE), 1) < HEAD_SIZE

    @pl.loop(0, chunks)
    def _(c):
        lanes = pl.ds(pl.multiple_of(c * TILE, TILE), TILE)
        own = convolved(x_ref, halo_x, taps_ref, bias_ref, lanes)
        values[:, lanes] = own
        early = lax.broadcasted_iota(jnp.int32, (length, TILE), 1) < HEAD_SIZE
        decay = jnp.where(early, cols_ref[c, :, 2:3], cols_ref[c, :, 3:4])
        scaled = own.astype(jnp.float32) * decay
        high = scaled.astype(jnp.bfloat16)
        low = (scaled - high.astype(jnp.float32)).astype(jnp.bfloat16)
        bmat = keys[:, :STATE]
        tn = (((0,), (0,)), ((), ()))
        state_out[c] = lax.dot_general(
            high, bmat, tn, preferred_element_type=jnp.float32
        ) + lax.dot_general(low, bmat, tn, preferred_element_type=jnp.float32)

        @pl.when(z == 0)
        def _():
            state_copy(c).start()

    squares[...] = jnp.zeros_like(squares)

    @pl.loop(0, chunks)
    def _(c):
        lanes = pl.ds(pl.multiple_of(c * TILE, TILE), TILE)

        @pl.when(z > 0)
        def _():
            state_copy(c).wait_recv()

        @pl.when((z > 0) & (z < n - 1))
        def _():
            top = lax.broadcasted_iota(jnp.int32, (TILE, STATE), 0) < HEAD_SIZE
            final = cols_ref[c, length - 1 : length, 0:2]
            through = jnp.where(top, jnp.exp(-final[:, 0:1]), jnp.exp(-final[:, 1:2]))
            through = through * same_ref[length - 1 : length, 4:5]
            state_out[c] = through * state_in[c] + state_out[c]
            state_copy(c).start()

        incoming = state_in[c]
        in_high = incoming.astype(jnp.bfloat16)
        in_low = (incoming - in_high.astype(jnp.float32)).astype(jnp.bfloat16)
        for cut in range(0, length, SPAN):
            upto = cut + SPAN
            near = pl.ds(cut, SPAN)
            signal = values[0:upto, lanes]
            sums_of = []
            entries = []
            for which in range(2):
                climb = cols_ref[c, near, which : which + 1]
                gap = rows_ref[c, which : which + 1, 0:upto] - climb
                weights = (
                    jnp.exp(jnp.minimum(gap, 0.0))
                    * scores[near, 0:upto]
                    * rows_ref[c, 2 + which : 3 + which, 0:upto]
                )
                high = weights.astype(jnp.bfloat16)
                low = (weights - high.astype(jnp.float32)).astype(jnp.bfloat16)
                sums_of.append(
                    jnp.dot(high, signal, preferred_element_type=jnp.float32)
                    + jnp.dot(low, signal, preferred_element_type=jnp.float32)
                )
                entries.append(jnp.exp(-climb) * same_ref[near, 4:5])
            cmat = keys[near, STATE:]
            arriving = lax.dot_general(
                cmat, in_high, nt, preferred_element_type=jnp.float32
            ) + lax.dot_general(cmat, in_low, nt, preferred_element_type=jnp.float32)
            mixed = (
                jnp.where(first, sums_of[0], sums_of[1])
                + skip_ref[:, lanes] * values[near, lanes].astype(jnp.float32)
                + arriving * jnp.where(first, entries[0], entries[1])
            )
            result = mixed * jax.nn.silu(z_ref[near, lanes].astype(jnp.float32))
            gated[near, lanes] = result
            squares[near, :] += result * result

    for k in range(2, n):
        @pl.when(z + k < n)
        def _():
            w_start(k)

    def tile_copy(which, k, slot_of):
        return remote(
            tiles.at[which, slot_of], tiles.at[which, slot_of], tile_send.at[which, k],
            tile_recv.at[which, slot_of], {"head": lax.rem(h + k, heads)},
        )

    def scale_of(which, partial, count):
        column = jnp.broadcast_to(jnp.sum(partial, axis=1, keepdims=True), (length, TILE))
        tiles[which, h] = jnp.transpose(column)[0:8, :]
        for k in range(1, heads):
            tile_copy(which, k, h).start()
        for k in range(1, heads):
            tile_copy(which, k, lax.rem(h + k, heads)).wait()
        total = tiles[which, 0]
        for head in range(1, heads):
            total = total + tiles[which, head]
        scale = lax.rsqrt(total / count + EPSILON)
        return jnp.transpose(jnp.broadcast_to(scale[0:1, :], (TILE, length)))

    squares[...] = scale_of(0, squares[...], inner)

    @pl.loop(0, chunks)
    def _(c):
        lanes = pl.ds(pl.multiple_of(c * TILE, TILE), TILE)
        normed[:, lanes] = (gated[:, lanes] * squares[...] * gain_ref[:, lanes]).astype(jnp.bfloat16)

    load_out.wait()

    def project(head, slot_of):
        @pl.loop(0, length // LOSS_ROWS)
        def _(step):
            near = pl.ds(pl.multiple_of(step * LOSS_ROWS, LOSS_ROWS), LOSS_ROWS)
            share_out[slot_of, near, :] = jnp.dot(
                normed[near, :],
                ow_buf[:, pl.ds(pl.multiple_of(head * share, TILE), share)],
                preferred_element_type=jnp.float32,
            )

    def share_copy(slot_of, target):
        return remote(
            share_out.at[slot_of], share_in.at[slot_of], share_send.at[slot_of],
            share_recv.at[slot_of], {"head": target},
        )

    project(lax.rem(twin + 2, heads), 0)
    share_copy(0, twin).start()
    project(side, 1)
    share_copy(0, twin).wait_recv()
    share_out[1] = share_out[1] + share_in[0]
    share_copy(1, side).start()
    project(twin, 2)
    share_copy(2, twin).start()
    for part in range(PARTS):
        w_pass_on(1, part)
    project(h, 3)
    share_copy(2, twin).wait_recv()
    share_copy(1, side).wait_recv()

    @pl.loop(0, length // LOSS_ROWS)
    def _(step):
        near = pl.ds(pl.multiple_of(step * LOSS_ROWS, LOSS_ROWS), LOSS_ROWS)
        total = share_out[3, near, :] + share_in[2, near, :] + share_in[1, near, :]
        block_ref[near, :] = (res_ref[near, :].astype(jnp.float32) + total).astype(jnp.bfloat16)

    square = jnp.zeros((length, TILE), jnp.float32)
    for cut in range(0, share, TILE):
        piece = block_ref[:, cut : cut + TILE].astype(jnp.float32)
        square = square + piece * piece
    squares[...] = scale_of(1, square, features)
    for cut in range(0, share, TILE):
        piece = block_ref[:, cut : cut + TILE].astype(jnp.float32)
        hid[:, cut : cut + TILE] = (
            piece * squares[...] * final_ref[:, cut : cut + TILE]
        ).astype(jnp.bfloat16)

    full[z, :, pl.ds(pl.multiple_of(h * share, TILE), share)] = hid[...]

    def slot(block, head):
        return full.at[block, :, pl.ds(pl.multiple_of(head * share, TILE), share)]

    def ship(sem, block, head, target, source=None):
        return remote(
            slot(block, head) if source is None else source, slot(block, head),
            sem, arrive.at[block, head], target,
        )

    def right(block, source=None):
        return ship(along_send.at[0, block], block, h, {"seq": z + 1}, source)

    def left(block, source=None):
        return ship(along_send.at[1, block], block, h, {"seq": z - 1}, source)

    def across(block, source=None):
        return ship(side_send.at[block], block, h, {"head": side}, source)

    def twinned(kind, block, head, source=None):
        return ship(along_send.at[2 + kind, block], block, head, {"head": twin}, source)

    def arrived(block, head):
        twinned(0, block, head).wait_recv()

    across(z, hid).start()

    @pl.when(z < n - 1)
    def _():
        right(z, hid).start()

    @pl.when(z > 0)
    def _():
        left(z, hid).start()

    twinned(0, z, h, hid).start()

    def mark_copy(block, head):
        return remote(
            marks.at[block, :, pl.ds(pl.multiple_of(head * TILE, TILE), TILE)], parts.at[me],
            mark_send.at[block, head], mark_recv.at[me], {"seq": block, "head": head},
        )

    dead = z * width - window(z)
    start_column = h * columns + window(z)

    def compute(block):
        @pl.loop(0, length // LOSS_ROWS)
        def _(step):
            at = pl.multiple_of(step * LOSS_ROWS, LOSS_ROWS)
            logits = jnp.dot(
                full[block, pl.ds(at, LOSS_ROWS), :], w_buf[...], preferred_element_type=jnp.float32
            )
            wanted = tgts[block, 0:1, pl.ds(at, LOSS_ROWS)]
            wanted = jnp.transpose(jnp.broadcast_to(wanted, (TILE, LOSS_ROWS))) - start_column
            lane = lax.broadcasted_iota(jnp.int32, (LOSS_ROWS, TILE), 1)
            pieces = []
            for cut in range(0, width, TILE):
                piece = logits[:, cut : cut + TILE]
                pieces.append(jnp.where(lane + cut >= dead, piece, LOW))
            peak = pieces[0]
            for piece in pieces[1:]:
                peak = jnp.maximum(peak, piece)
            peak = jnp.max(peak, axis=1, keepdims=True)
            total = jnp.zeros((LOSS_ROWS, TILE), jnp.float32)
            picked = jnp.zeros((LOSS_ROWS, TILE), jnp.float32)
            for index, piece in enumerate(pieces):
                total = total + jnp.exp(piece - peak)
                here = (lane + index * TILE == wanted) & (lane + index * TILE >= dead)
                picked = picked + jnp.where(here, piece, 0.0)
            total = jnp.sum(total, axis=1, keepdims=True)
            picked = jnp.sum(picked, axis=1, keepdims=True)
            tile = jnp.where(lane == 0, peak, jnp.where(lane == 1, total, picked))
            marks[block, :, pl.ds(at, LOSS_ROWS)] = jnp.transpose(tile)[0:8, :]

        @pl.loop(0, heads)
        def _(head):
            @pl.when((block != z) | (head != h))
            def _():
                mark_copy(block, head).start()

    def finish(block):
        arrived(block, side)
        twinned(1, block, side).start()
        arrived(block, twin)
        arrived(block, lax.rem(twin + 2, heads))
        compute(block)

    for k in range(2, n):
        for part in range(PARTS):
            w_pass_on(k, part)

    for step in range(1, n):
        @pl.when(z >= step)
        def _():
            block = z - step
            arrived(block, h)

            @pl.when(z < n - 1)
            def _():
                right(block).start()

            across(block).start()
            twinned(0, block, h).start()

        @pl.when(z + step < n)
        def _():
            block = z + step
            arrived(block, h)

            @pl.when(z > 0)
            def _():
                left(block).start()

            across(block).start()
            twinned(0, block, h).start()

        if step == 1:
            load_own.wait()
            for k in range(1, n):
                source = lax.rem(z + n - k, n)
                tell(k, source).wait()
                for hop in range(1, groups):
                    other = lax.rem(g + groups - hop, groups)
                    for part in range(PARTS):
                        place = w_buf.at[w_rows(source, other, part), :]
                        remote(
                            place, place, y_send.at[source, part, hop],
                            y_recv.at[other, source, part], {"groups": other},
                        ).wait_recv()
            finish(z)
        else:
            @pl.when(z >= step - 1)
            def _():
                finish(z - step + 1)

            @pl.when(z + step - 1 < n)
            def _():
                finish(z + step - 1)

    @pl.when(z >= n - 1)
    def _():
        finish(z - n + 1)

    @pl.when(z + n - 1 < n)
    def _():
        finish(z + n - 1)

    @pl.when(z < n - 1)
    def _():
        for copy in halo_copies():
            copy.wait_send()

        @pl.loop(0, chunks)
        def _(c):
            state_copy(c).wait_send()

    for slot_of, target in ((0, twin), (1, side), (2, twin)):
        share_copy(slot_of, target).wait_send()
    for k in range(1, n):
        source = lax.rem(z + n - k, n)
        for part in range(PARTS):
            w_copy(k, part).wait_send()
            for hop in range(1, groups):
                w_forward(source, part, hop).wait_send()
    for block in range(n):
        @pl.when((z < n - 1) & (z >= block))
        def _():
            right(block).wait_send()

        @pl.when((z > 0) & (z <= block))
        def _():
            left(block).wait_send()

        across(block).wait_send()
        twinned(0, block, h).wait_send()
        twinned(1, block, side).wait_send()

    parts[me] = marks[z, :, pl.ds(pl.multiple_of(h * TILE, TILE), TILE)]

    @pl.loop(1, total_peers)
    def _(k):
        there, where_head = peer(k)
        flat = there * heads + where_head
        remote(
            parts.at[flat], parts.at[flat], mark_send.at[there, where_head], mark_recv.at[flat],
            {"seq": there, "head": where_head},
        ).wait()

    peak = parts[0, 0:1, :]
    for flat in range(1, total_peers):
        peak = jnp.maximum(peak, parts[flat, 0:1, :])
    total = jnp.zeros((1, TILE), jnp.float32)
    picked = jnp.zeros((1, TILE), jnp.float32)
    for flat in range(total_peers):
        total = total + parts[flat, 1:2, :] * jnp.exp(parts[flat, 0:1, :] - peak)
        picked = picked + parts[flat, 2:3, :]
    losses = peak + jnp.log(total) - picked
    mine = jnp.sum(member_ref[...] * losses, axis=1, keepdims=True)
    sums[me] = jnp.broadcast_to(mine, sums.shape[1:])

    def sum_copy(k, slot_of):
        there, where_head = peer(k)
        return remote(
            sums.at[slot_of], sums.at[slot_of], sum_send.at[k], sum_recv.at[slot_of],
            {"seq": there, "head": where_head},
        )

    @pl.loop(1, total_peers)
    def _(k):
        sum_copy(k, me).start()

    @pl.loop(1, total_peers)
    def _(k):
        sum_copy(k, lax.rem(me + k, total_peers)).wait()

    grand = sums[0]
    for flat in range(1, total_peers):
        grand = grand + sums[flat]
    out_ref[...] = grand


def fits(length, inner_here, share, depth, columns, width, n, heads, groups):
    room = 2 * (n * length * n * depth + n * depth * width + inner_here * n * depth)
    room += 4 * (length * inner_here * 4 + 6 * length * share + length * length)
    even = [inner_here % TILE, share % TILE, columns % TILE, depth % (groups * PARTS * 16)]
    even += [length % SPAN, length % LOSS_ROWS, length - heads * TILE, heads - 4]
    even += [share * heads - depth * n]
    return not any(even) and n > 1 and (n - 1) * width <= columns and room < 56 * 2**20


def block_stage(operands, whole, member, width, n, heads, groups):
    x_in, res = operands[0], operands[13]
    out_weight, _ = whole
    length, inner_here = x_in.shape
    share = res.shape[1]
    features = out_weight.shape[1]
    peers = n * heads
    chunks = inner_here // TILE
    dma = pltpu.SemaphoreType.DMA
    vmem = pltpu.VMEM
    f32, bf16 = jnp.float32, jnp.bfloat16
    return pl.pallas_call(
        functools.partial(block_kernel, n, heads, groups, inner_here * heads, features),
        out_shape=[
            jax.ShapeDtypeStruct((length, share), bf16),
            jax.ShapeDtypeStruct(member.shape, f32),
        ],
        in_specs=[pl.BlockSpec(memory_space=pltpu.VMEM)] * (len(operands) + 1)
        + [pl.BlockSpec(memory_space=pl.ANY)] * 2,
        out_specs=[pl.BlockSpec(memory_space=pltpu.VMEM)] * 2,
        scratch_shapes=[
            vmem((inner_here, features), bf16),
            vmem((features, width), bf16),
            vmem((n, length, features), bf16),
            vmem((n, 8, length), jnp.int32),
            vmem((n, 8, length), f32),
            vmem((peers, 8, TILE), f32),
            vmem((peers,) + member.shape, f32),
            vmem((HALO, inner_here), bf16),
            vmem((HALO, 2 * STATE), bf16),
            vmem((length + HALO, TILE), f32),
            vmem((KERNEL - 1, length, TILE), f32),
            vmem((length, inner_here), bf16),
            vmem((length, 2 * STATE), bf16),
            vmem((length, length), f32),
            vmem((chunks, TILE, STATE), f32),
            vmem((chunks, TILE, STATE), f32),
            vmem((length, inner_here), f32),
            vmem((length, TILE), f32),
            vmem((2, heads, 8, length), f32),
            vmem((length, inner_here), bf16),
            vmem((4, length, share), f32),
            vmem((3, length, share), f32),
            vmem((length, share), bf16),
            dma((2,)),
            dma((2,)),
            dma((2,)),
            dma((n, PARTS)),
            dma((n, PARTS)),
            dma((n, PARTS, groups)),
            dma((groups, n, PARTS)),
            dma((chunks,)),
            dma((chunks,)),
            dma((2, heads)),
            dma((2, heads)),
            dma((3,)),
            dma((3,)),
            dma((4, n)),
            dma((n,)),
            dma((n, heads)),
            dma((n,)),
            dma((n,)),
            dma((n, heads)),
            dma((peers,)),
            dma((peers,)),
            dma((peers,)),
        ],
        compiler_params=pltpu.CompilerParams(
            collective_id=0, has_side_effects=True, vmem_limit_bytes=63 * 2**20
        ),
        cost_estimate=pl.CostEstimate(
            flops=2 * n * length * features * width, bytes_accessed=4 * 10**7, transcendentals=10**7
        ),
    )(*operands, member, *whole)


def width_of(columns):
    devices = lax.axis_size("seq")
    return -(-columns // (devices * TILE)) * TILE


def fused_fits(residual, x_in, lm_weight):
    length, inner_here = x_in.shape
    depth, columns = lm_weight.shape
    sizes = [lax.axis_size(axis) for axis in ("seq", "head", "groups")]
    return fits(
        length, inner_here, residual.shape[1], depth, columns, width_of(columns), *sizes
    )


def fused(
    residual,
    x_in,
    bc_in,
    z_in,
    dt_raw,
    dt_bias,
    decay_rate,
    d_skip,
    conv_x_weight,
    conv_x_bias,
    conv_bc_weight,
    conv_bc_bias,
    norm_gain,
    out_weight,
    final_gain,
    lm_weight,
    targets,
    doc_lengths,
):
    length, _ = x_in.shape
    heads_here = dt_raw.shape[0]
    share = residual.shape[1]
    head_rank = lax.axis_index("head")
    offset_here = lax.axis_index("seq") * length
    positions = offset_here + jnp.arange(length, dtype=jnp.int32)
    doc_ids = document_of(positions, doc_lengths)
    before = document_of(jnp.reshape(offset_here - 1, (1,)), doc_lengths)[0]
    steps = jax.nn.softplus(dt_raw + dt_bias[:, None])
    climb = jnp.cumsum(steps * decay_rate[:, None], axis=1)
    last = (doc_ids == doc_ids[length - 1]).astype(jnp.float32)
    tail = jnp.exp(climb - climb[:, length - 1 :]) * last[None, :] * steps
    couples = heads_here // 2
    rows = jnp.concatenate(
        [climb.reshape(couples, 2, length), steps.reshape(couples, 2, length)], axis=1
    )
    cols = jnp.concatenate(
        [climb.reshape(couples, 2, length), tail.reshape(couples, 2, length)], axis=1
    ).transpose(0, 2, 1)
    flags = [document_of(positions - lag, doc_lengths) == doc_ids for lag in range(KERNEL)]
    flags += [doc_ids == before, doc_ids, doc_ids, doc_ids]
    same = jnp.stack([flag.astype(jnp.float32) for flag in flags], axis=1)
    doc_row = jnp.broadcast_to(doc_ids.astype(jnp.float32)[None, :], (8, length))
    documents = -(-doc_lengths.shape[0] // 8) * 8
    own_ids = lax.dynamic_slice_in_dim(doc_ids, head_rank * TILE, TILE, 0)
    member = (own_ids[None, :] == jnp.arange(documents, dtype=jnp.int32)[:, None]).astype(
        jnp.float32
    )
    final = lax.dynamic_slice_in_dim(final_gain, head_rank * share, share, 0)
    operands = [
        x_in,
        z_in,
        bc_in,
        conv_x_weight.astype(jnp.float32),
        conv_x_bias.astype(jnp.float32)[None, :],
        conv_bc_weight.astype(jnp.float32),
        conv_bc_bias.astype(jnp.float32)[None, :],
        cols,
        rows,
        same,
        doc_row,
        jnp.repeat(d_skip, HEAD_SIZE)[None, :],
        norm_gain.astype(jnp.float32)[None, :],
        residual,
        final.astype(jnp.float32)[None, :],
        jnp.broadcast_to(targets[None, :], (8, length)),
    ]
    sizes = [lax.axis_size(axis) for axis in ("seq", "head", "groups")]
    block_out, sums = block_stage(
        operands, (out_weight, lm_weight), member, width_of(lm_weight.shape[1]), *sizes
    )
    sums = sums[: doc_lengths.shape[0], 0]
    return (block_out, sums / doc_lengths.astype(jnp.float32))


def local(
    residual,
    x_in,
    bc_in,
    z_in,
    dt_raw,
    dt_bias,
    decay_rate,
    d_skip,
    conv_x_weight,
    conv_x_bias,
    conv_bc_weight,
    conv_bc_bias,
    norm_gain,
    out_weight,
    final_gain,
    lm_weight,
    targets,
    doc_lengths,
):
    if fused_fits(residual, x_in, lm_weight):
        return fused(
            residual,
            x_in,
            bc_in,
            z_in,
            dt_raw,
            dt_bias,
            decay_rate,
            d_skip,
            conv_x_weight,
            conv_x_bias,
            conv_bc_weight,
            conv_bc_bias,
            norm_gain,
            out_weight,
            final_gain,
            lm_weight,
            targets,
            doc_lengths,
        )
    length = x_in.shape[0]
    inner_here = x_in.shape[1]
    heads_here = dt_raw.shape[0]
    seq_rank = lax.axis_index("seq")
    head_rank = lax.axis_index("head")
    offset_here = seq_rank * length
    positions = offset_here + jnp.arange(length, dtype=jnp.int32)
    doc_ids = document_of(positions, doc_lengths)
    columns_here = lm_weight.shape[1]
    devices = lax.axis_size("seq")
    width = -(-columns_here // (devices * 128)) * 128

    def window(rank):
        return jnp.minimum(rank * width, columns_here - width)

    depth = lm_weight.shape[0]
    vocab_weight = jnp.zeros((depth * devices, width), lm_weight.dtype)
    group = lax.axis_index("groups")
    groups = lax.axis_size("groups")
    band = depth // groups
    pieces = [
        lax.dynamic_slice(
            lm_weight, (group * band, window((seq_rank + by) % devices)), (band, width)
        )
        for by in range(1, devices)
    ]
    aims = [targets]
    for by in range(1, devices):
        aims.append(rotated(targets, "seq", by))
    margin = KERNEL - 1
    rims = shifted(
        jnp.concatenate([x_in[length - margin :], bc_in[length - margin :]], axis=1), "seq", 1
    )
    x_rim, bc_rim = rims[:, :inner_here], rims[:, inner_here:]
    keys_queries = causal_conv(
        bc_in, bc_rim, conv_bc_weight, conv_bc_bias, positions, doc_ids, doc_lengths
    )
    bmat, cmat = keys_queries[:, :STATE], keys_queries[:, STATE:]
    steps = jax.nn.softplus(dt_raw + dt_bias[:, None])
    climb = jnp.cumsum(steps * decay_rate[:, None], axis=1)
    before = document_of(jnp.reshape(offset_here - 1, (1,)), doc_lengths)[0]
    carried = (doc_ids == before).astype(jnp.float32)
    through = jnp.exp(-climb[:, length - 1]) * carried[length - 1]
    same = jnp.stack(
        [
            (document_of(positions - lag, doc_lengths) == doc_ids).astype(jnp.float32)
            for lag in range(KERNEL)
        ],
        axis=1,
    )
    last = (doc_ids == doc_ids[length - 1]).astype(jnp.float32)
    tail = jnp.exp(climb - climb[:, length - 1 :]) * last[None, :] * steps
    couples = heads_here // 2
    rows = jnp.concatenate(
        [climb.reshape(couples, 2, length), steps.reshape(couples, 2, length)], axis=1
    )
    cols = jnp.concatenate(
        [climb.reshape(couples, 2, length), tail.reshape(couples, 2, length)], axis=1
    ).transpose(0, 2, 1)
    rim = jnp.concatenate([jnp.zeros((8 - margin, inner_here), x_rim.dtype), x_rim], axis=0)
    values, own_end = conv_state(
        x_in,
        rim,
        conv_x_weight.astype(jnp.float32),
        conv_x_bias.astype(jnp.float32)[None, :],
        same,
        cols,
        bmat,
    )
    of_head = jnp.arange(inner_here, dtype=jnp.int32)[None, :] // HEAD_SIZE
    spread = (of_head == jnp.arange(heads_here, dtype=jnp.int32)[:, None]).astype(jnp.float32)
    incoming = entering(
        through, own_end.reshape(heads_here, HEAD_SIZE, STATE), "seq"
    ).reshape(inner_here, STATE)
    held_back = lax.optimization_barrier(tuple(pieces[1:]) + (incoming,))
    pieces, incoming = pieces[:1] + list(held_back[:-1]), held_back[-1]
    arrivals = []
    for by in range(1, devices):
        arrivals.append(rotated(pieces[by - 1], "seq", by))
    bands = []
    for by in range(1, devices):
        bands.append(
            [arrivals[by - 1]]
            + [rotated(arrivals[by - 1], "groups", hop) for hop in range(1, groups)]
        )
    order = jnp.arange(length, dtype=jnp.int32)
    inside = (doc_ids[:, None] == doc_ids[None, :]) & (order[:, None] >= order[None, :])
    scores = jnp.where(
        inside,
        lax.dot_general(
            cmat, bmat, (((1,), (1,)), ((), ())), preferred_element_type=jnp.float32
        ),
        0.0,
    )
    skip = jnp.dot(d_skip[None, :], spread, precision=HIGH)
    output = within(values, scores, cols, rows, skip)
    entry = jnp.dot((jnp.exp(-climb) * carried[None, :]).T, spread, precision=HIGH)
    arriving = lax.dot_general(
        cmat.astype(jnp.float32), incoming, (((1,), (1,)), ((), ())), precision=HALF
    )
    gated = (output + arriving * entry) * jax.nn.silu(z_in.astype(jnp.float32))
    square_sum = lax.psum(jnp.sum(gated * gated, axis=1), "head")
    scale = lax.rsqrt(square_sum / INNER + EPSILON)
    normed = (gated * scale[:, None] * norm_gain.astype(jnp.float32)[None, :]).astype(jnp.bfloat16)
    share = residual.shape[1]
    projected = scattered_product(normed, out_weight, "head")
    block_out = (residual.astype(jnp.float32) + projected).astype(jnp.bfloat16)
    widened = block_out.astype(jnp.float32)
    square_total = lax.psum(jnp.sum(widened * widened, axis=1), "head")
    gain_part = lax.dynamic_slice_in_dim(final_gain, head_rank * share, share, 0)
    final_scale = lax.rsqrt(square_total / D + EPSILON)
    hidden_part = (widened * final_scale[:, None] * gain_part.astype(jnp.float32)[None, :]).astype(
        jnp.bfloat16
    )
    own = lax.dynamic_slice_in_dim(lm_weight, window(seq_rank), width, 1)
    vocab_weight = lax.dynamic_update_slice_in_dim(vocab_weight, own, seq_rank * depth, 0)
    for by in range(1, devices):
        source = (seq_rank + devices - by) % devices
        for hop in range(groups):
            start = source * depth + (group + groups - hop) % groups * band
            vocab_weight = lax.dynamic_update_slice_in_dim(
                vocab_weight, bands[by - 1][hop], start, 0
            )
    column = jnp.arange(width, dtype=jnp.int32)
    first = head_rank * columns_here + window(seq_rank)
    live = column + window(seq_rank) >= seq_rank * width
    marks = jnp.zeros((3, length * devices), jnp.float32)
    for by in range(devices):
        source = (seq_rank + devices - by) % devices
        if by and by % 4 == 0:
            hidden_part, marks = lax.optimization_barrier((hidden_part, marks))
        rows = rotated(hidden_part, "seq", by) if by else hidden_part
        hidden = gathered_features(rows, "head")
        logits = jnp.dot(hidden, vocab_weight, preferred_element_type=jnp.float32)
        logits = jnp.where(live[None, :], logits, LOW)
        peak = jnp.max(logits, axis=1)
        wanted = aims[by] - first
        total = jnp.sum(jnp.exp(logits - peak[:, None]), axis=1)
        picked = jnp.sum(
            jnp.where((column[None, :] == wanted[:, None]) & live[None, :], logits, 0.0), axis=1
        )
        marks = lax.dynamic_update_slice_in_dim(
            marks, jnp.stack([peak, total, picked]), source * length, 1
        )
    for axis in ("head", "seq"):
        every_mark = lax.all_gather(marks, axis)
        peak = jnp.max(every_mark[:, 0], axis=0)
        total = jnp.sum(every_mark[:, 1] * jnp.exp(every_mark[:, 0] - peak[None]), axis=0)
        marks = jnp.stack([peak, total, jnp.sum(every_mark[:, 2], axis=0)])
    losses = marks[0] + jnp.log(marks[1]) - marks[2]
    every = document_of(jnp.arange(length * devices, dtype=jnp.int32), doc_lengths)
    documents = jnp.arange(doc_lengths.shape[0], dtype=jnp.int32)
    member = every[None, :] == documents[:, None]
    sums = jnp.sum(jnp.where(member, losses[None, :], 0.0), axis=1)
    return (block_out, sums / doc_lengths.astype(jnp.float32))


def solution(mesh):
    in_specs = (
        P(("groups", "seq"), "head"),
        P(("groups", "seq"), "head"),
        P(("groups", "seq"), None),
        P(("groups", "seq"), "head"),
        P("head", ("groups", "seq")),
        P("head"),
        P("head"),
        P("head"),
        P(None, "head"),
        P("head"),
        P(),
        P(),
        P("head"),
        P("head", None),
        P(),
        P("seq", "head"),
        P(("groups", "seq")),
        P("groups"),
    )
    out_specs = (P(("groups", "seq"), "head"), P("groups"))


    return jax.shard_map(local, mesh=mesh, in_specs=in_specs, out_specs=out_specs, check_vma=False)
```

```python
import functools

import jax
import jax.numpy as jnp
from jax import lax
from jax.experimental import pallas as pl
from jax.experimental.pallas import tpu as pltpu
from jax.sharding import PartitionSpec as P

D = 2560
HEAD_SIZE = 64
STATE = 128
KERNEL = 4
SPAN = 256
INNER = 5120


EPSILON = 1e-05
HIGH = lax.Precision.HIGHEST
HALF = lax.Precision.HIGH
LOW = -1e30
MESH = pl.DeviceIdType.MESH


def shifted(array, axis, by):
    length = lax.axis_size(axis)
    pairs = [(i, i + by) for i in range(length) if 0 <= i + by < length]
    return lax.ppermute(array, axis, pairs)


def rotated(array, axis, by):
    length = lax.axis_size(axis)
    return lax.ppermute(array, axis, [(i, (i + by) % length) for i in range(length)])


def sibling(array, axis):
    length = lax.axis_size(axis)
    return lax.ppermute(array, axis, [(i, i ^ 1) for i in range(length)])


def scattered_product(normed, weight, axis):
    length = lax.axis_size(axis)
    rank = lax.axis_index(axis)
    chips = length // 2
    share = weight.shape[1] // length

    def columns(core):
        return jnp.concatenate(
            [
                lax.dynamic_slice_in_dim(
                    weight, ((rank // 2 + by) % chips * 2 + core) * share, share, 1
                )
                for by in range(chips)
            ],
            axis=1,
        )

    theirs = columns(1 - rank % 2)
    ours = columns(rank % 2)
    other = jnp.dot(normed, theirs, preferred_element_type=jnp.float32)
    arrived = sibling(other, axis)
    pair = jnp.dot(normed, ours, preferred_element_type=jnp.float32) + arrived
    total = pair[:, :share]
    for by in range(1, chips):
        total = total + rotated(pair[:, by * share : (by + 1) * share], axis, 2 * by)
    return total


def gathered_features(part, axis):
    length = lax.axis_size(axis)
    rank = lax.axis_index(axis)
    chips = length // 2
    rows, share = part.shape
    column = [part] + [rotated(part, axis, 2 * by) for by in range(1, chips)]
    joined = jnp.concatenate(column, axis=1)
    twin = sibling(joined, axis)
    full = jnp.zeros((rows, share * length), part.dtype)
    for by in range(chips):
        source = (rank + 2 * (chips - by)) % length
        piece = slice(by * share, (by + 1) * share)
        full = lax.dynamic_update_slice_in_dim(full, joined[:, piece], source * share, 1)
        full = lax.dynamic_update_slice_in_dim(full, twin[:, piece], (source ^ 1) * share, 1)
    return full


def entering(through, state, axis):
    length = lax.axis_size(axis)
    tag = jnp.broadcast_to(through[:, None, None], (through.shape[0], 8, state.shape[2]))
    packed = shifted(jnp.concatenate([state, tag], axis=1), axis, 1)
    extent = state.shape[1]
    reach = 1
    while reach < length:
        earlier = shifted(packed, axis, reach)
        decay = packed[:, extent : extent + 1, :]
        packed = jnp.concatenate(
            [packed[:, :extent] + decay * earlier[:, :extent], decay * earlier[:, extent:]], axis=1
        )
        reach *= 2
    return packed[:, :extent]


def document_of(positions, doc_lengths):
    starts = jnp.cumsum(doc_lengths) - doc_lengths
    return jnp.sum((positions[:, None] >= starts[None, :]).astype(jnp.int32), axis=1) - 1


def causal_conv(signal, rim_rows, weight, bias, positions, doc_ids, doc_lengths):
    length = signal.shape[0]
    taps = weight.shape[0]
    joined = jnp.concatenate([rim_rows, signal], axis=0).astype(jnp.float32)
    total = jnp.zeros(signal.shape, jnp.float32) + bias.astype(jnp.float32)[None, :]
    for offset in range(taps):
        lag = taps - 1 - offset
        source = document_of(positions - lag, doc_lengths)
        same = (source == doc_ids).astype(jnp.float32)
        total = (
            total
            + weight[offset].astype(jnp.float32)[None, :]
            * joined[offset : offset + length]
            * same[:, None]
        )
    return jax.nn.silu(total).astype(jnp.bfloat16)


def conv_state_kernel(x_ref, rim_ref, taps_ref, bias_ref, same_ref, cols_ref, bmat_ref, values_ref, state_ref, held):
    length, lanes = x_ref.shape
    taps = taps_ref.shape[0]
    held[0:8, :] = rim_ref[...].astype(jnp.float32)
    held[8:, :] = x_ref[...].astype(jnp.float32)
    total = jnp.zeros((length, lanes), jnp.float32) + bias_ref[...]
    for offset in range(taps):
        lag = taps - 1 - offset
        rows = held[8 - lag : 8 - lag + length, :]
        total = total + taps_ref[offset : offset + 1, :] * rows * same_ref[:, lag : lag + 1]
    values = jax.nn.silu(total).astype(jnp.bfloat16)
    values_ref[...] = values
    first = lax.broadcasted_iota(jnp.int32, (length, lanes), 1) < HEAD_SIZE
    tail = jnp.where(first, cols_ref[0, :, 2:3], cols_ref[0, :, 3:4])
    scaled = values.astype(jnp.float32) * tail
    high = scaled.astype(jnp.bfloat16)
    low = (scaled - high.astype(jnp.float32)).astype(jnp.bfloat16)
    bmat = bmat_ref[...]
    dims = (((0,), (0,)), ((), ()))
    state_ref[...] = lax.dot_general(
        high, bmat, dims, preferred_element_type=jnp.float32
    ) + lax.dot_general(low, bmat, dims, preferred_element_type=jnp.float32)


def within_kernel(values_ref, scores_ref, cols_ref, rows_ref, skip_ref, out_ref):
    length, lanes = values_ref.shape
    for cut in range(0, length, SPAN):
        upto = cut + SPAN
        values = values_ref[0:upto, :]
        scores = scores_ref[cut:upto, 0:upto]
        parts = []
        for which in range(2):
            gap = rows_ref[0, which : which + 1, 0:upto] - cols_ref[0, cut:upto, which : which + 1]
            weights = (
                jnp.exp(jnp.minimum(gap, 0.0)) * scores * rows_ref[0, 2 + which : 3 + which, 0:upto]
            )
            high = weights.astype(jnp.bfloat16)
            low = (weights - high.astype(jnp.float32)).astype(jnp.bfloat16)
            parts.append(
                jnp.dot(high, values, preferred_element_type=jnp.float32)
                + jnp.dot(low, values, preferred_element_type=jnp.float32)
            )
        first = lax.broadcasted_iota(jnp.int32, (SPAN, lanes), 1) < HEAD_SIZE
        own = values_ref[cut:upto, :].astype(jnp.float32)
        out_ref[cut:upto, :] = jnp.where(first, parts[0], parts[1]) + skip_ref[...] * own


def conv_state(x_in, rim, taps, bias, same, cols, bmat):
    length, inner_here = x_in.shape
    lanes = 2 * HEAD_SIZE
    return pl.pallas_call(
        conv_state_kernel,
        grid=(inner_here // lanes,),
        in_specs=[
            pl.BlockSpec((length, lanes), lambda i: (0, i)),
            pl.BlockSpec((8, lanes), lambda i: (0, i)),
            pl.BlockSpec((taps.shape[0], lanes), lambda i: (0, i)),
            pl.BlockSpec((1, lanes), lambda i: (0, i)),
            pl.BlockSpec(same.shape, lambda i: (0, 0)),
            pl.BlockSpec((1, length, 4), lambda i: (i, 0, 0)),
            pl.BlockSpec(bmat.shape, lambda i: (0, 0)),
        ],
        out_specs=[
            pl.BlockSpec((length, lanes), lambda i: (0, i)),
            pl.BlockSpec((lanes, STATE), lambda i: (i, 0)),
        ],
        out_shape=[
            jax.ShapeDtypeStruct((length, inner_here), jnp.bfloat16),
            jax.ShapeDtypeStruct((inner_here, STATE), jnp.float32),
        ],
        scratch_shapes=[pltpu.VMEM((length + 8, lanes), jnp.float32)],
        cost_estimate=pl.CostEstimate(flops=10**9, bytes_accessed=6 * 10**6, transcendentals=10**6),
    )(x_in, rim, taps, bias, same, cols, bmat)


def within(values, scores, cols, rows, skip):
    length, inner_here = values.shape
    lanes = 2 * HEAD_SIZE
    return pl.pallas_call(
        within_kernel,
        grid=(inner_here // lanes,),
        in_specs=[
            pl.BlockSpec((length, lanes), lambda i: (0, i)),
            pl.BlockSpec(scores.shape, lambda i: (0, 0)),
            pl.BlockSpec((1, length, 4), lambda i: (i, 0, 0)),
            pl.BlockSpec((1, 4, length), lambda i: (i, 0, 0)),
            pl.BlockSpec((1, lanes), lambda i: (0, i)),
        ],
        out_specs=pl.BlockSpec((length, lanes), lambda i: (0, i)),
        out_shape=jax.ShapeDtypeStruct((length, inner_here), jnp.float32),
        cost_estimate=pl.CostEstimate(flops=8 * 10**9, bytes_accessed=20 * 10**6, transcendentals=10**7),
    )(values, scores, cols, rows, skip)


TILE = 128
LOSS_ROWS = 256
HALO = 16
PARTS = 4


def block_kernel(
    n, heads, groups, inner, features, widths,
    x_ref, z_ref, bc_ref, taps_ref, bias_ref, bc_taps_ref, bc_bias_ref, cols_ref, rows_ref,
    same_ref, doc_ref, skip_ref, gain_ref, res_ref, final_ref, tgt_ref, member_ref, ow_ref, lm_ref,
    block_ref, out_ref,
    ow_buf, w_buf, full, tgts, marks, parts, sums, halo_x, halo_bc, held, masks, values, keys,
    scores, state_out, state_in, gated, squares, tiles, normed, share_out, share_in, hid,
    load_sem, halo_send, halo_recv, w_send, w_recv, y_send, y_recv, state_send, state_recv,
    tile_send, tile_recv, share_send, share_recv,
    along_send, side_send, arrive, tgt_send, tgt_recv, mark_send, mark_recv, sum_send, sum_recv,
):
    g = lax.axis_index("groups")
    z = lax.axis_index("seq")
    h = lax.axis_index("head")
    length, inner_here = x_ref.shape
    share = res_ref.shape[1]
    depth, columns = lm_ref.shape
    starts = [sum(widths[:rank]) for rank in range(n)]
    band = depth // groups
    sub = band // PARTS
    total_peers = n * heads
    me = z * heads + h
    twin = h + 1 - 2 * lax.rem(h, 2)
    side = lax.rem(h + 2, heads)
    chunks = inner_here // TILE

    def remote(src, dst, send, recv, target):
        return pltpu.make_async_remote_copy(
            src_ref=src, dst_ref=dst, send_sem=send, recv_sem=recv,
            device_id=target, device_id_type=MESH,
        )

    def peer(k):
        flat = lax.rem(me + k, total_peers)
        return flat // heads, lax.rem(flat, heads)

    load_out = pltpu.make_async_copy(ow_ref, ow_buf, load_sem.at[0])
    load_out.start()

    def load_own(rank):
        return pltpu.make_async_copy(
            lm_ref.at[:, pl.ds(starts[rank], widths[rank])],
            w_buf.at[pl.ds(rank * depth, depth), pl.ds(0, widths[rank])],
            load_sem.at[1],
        )

    for rank in range(n):
        @pl.when(z == rank)
        def _():
            load_own(rank).start()

    barrier = pltpu.get_barrier_semaphore()

    @pl.loop(1, total_peers)
    def _(k):
        there, where_head = peer(k)
        pl.semaphore_signal(
            barrier, inc=1, device_id={"seq": there, "head": where_head}, device_id_type=MESH
        )

    for hop in range(1, groups):
        pl.semaphore_signal(
            barrier, inc=1, device_id={"groups": lax.rem(g + hop, groups)}, device_id_type=MESH
        )
    pl.semaphore_wait(barrier, total_peers - 1 + groups - 1)

    def halo_copies():
        tail_rows = pl.ds(length - HALO, HALO)
        return [
            remote(x_ref.at[tail_rows, :], halo_x, halo_send.at[0], halo_recv.at[0], {"seq": z + 1}),
            remote(bc_ref.at[tail_rows, :], halo_bc, halo_send.at[1], halo_recv.at[1], {"seq": z + 1}),
        ]

    @pl.when(z < n - 1)
    def _():
        for copy in halo_copies():
            copy.start()

    def w_rows(source, group, part):
        return pl.ds(pl.multiple_of(source * depth + group * band + part * sub, 16), sub)

    def w_copy(rank, part):
        columns_there = pl.ds(starts[rank], widths[rank])
        return remote(
            lm_ref.at[pl.ds(pl.multiple_of(g * band + part * sub, 16), sub), columns_there],
            w_buf.at[w_rows(z, g, part), pl.ds(0, widths[rank])],
            w_send.at[rank, part],
            w_recv.at[z, part],
            {"seq": rank},
        )

    def w_place(rank, source, group, part):
        return w_buf.at[w_rows(source, group, part), pl.ds(0, widths[rank])]

    def w_forward(rank, source, part, hop):
        place = w_place(rank, source, g, part)
        return remote(
            place, place, y_send.at[source, part, hop], y_recv.at[g, source, part],
            {"groups": lax.rem(g + hop, groups)},
        )

    def w_pass_on(rank, source, part):
        place = w_place(rank, source, g, part)
        remote(
            place, place, w_send.at[source, part], w_recv.at[source, part], {"seq": source}
        ).wait_recv()
        for hop in range(1, groups):
            w_forward(rank, source, part, hop).start()

    def legs(rank):
        far_first = list(range(n - 1, rank, -1)) + list(range(rank))
        every = [(source, part) for source in far_first for part in range(PARTS)]

        def early(source, part):
            if source < rank:
                return source == rank - 1 and (part == 0 or rank in (1, n - 1))
            if rank == 0:
                return source != 2
            return source > rank + 1 or (rank == n - 2 and part < PARTS // 2)

        return [leg for leg in every if early(*leg)], [leg for leg in every if not early(*leg)]

    for rank in range(n):
        @pl.when(z > rank)
        def _():
            for part in range(PARTS):
                w_copy(rank, part).start()

        @pl.when(z + 1 == rank)
        def _():
            w_copy(rank, 0).start()

    def tell(k, source):
        return remote(
            tgt_ref, tgts.at[source], tgt_send.at[k], tgt_recv.at[source],
            {"seq": lax.rem(z + k, n)},
        )

    for k in range(1, n):
        tell(k, z).start()
    tgts[z] = tgt_ref[...]

    for lag in range(1, KERNEL):
        masks[lag - 1] = jnp.broadcast_to(same_ref[:, lag : lag + 1], (length, TILE))

    @pl.when(z == 0)
    def _():
        halo_x[...] = jnp.zeros_like(halo_x)
        halo_bc[...] = jnp.zeros_like(halo_bc)
        state_in[...] = jnp.zeros_like(state_in)

    @pl.when(z > 0)
    def _():
        for copy in halo_copies():
            copy.wait_recv()

    def convolved(signal, halo, weight, bias, lanes):
        held[0:HALO, :] = halo[:, lanes].astype(jnp.float32)
        held[HALO:, :] = signal[:, lanes].astype(jnp.float32)
        total = jnp.zeros((length, TILE), jnp.float32) + bias[:, lanes]
        for offset in range(KERNEL):
            lag = KERNEL - 1 - offset
            term = weight[offset : offset + 1, lanes] * held[HALO - lag : HALO - lag + length, :]
            total = total + (term * masks[lag - 1] if lag else term)
        return jax.nn.silu(total).astype(jnp.bfloat16)

    for half in range(2):
        lanes = pl.ds(half * STATE, STATE)
        keys[:, lanes] = convolved(bc_ref, halo_bc, bc_taps_ref, bc_bias_ref, lanes)
    nt = (((1,), (1,)), ((), ()))
    for cut in range(0, length, SPAN):
        near = pl.ds(cut, SPAN)
        inside = (same_ref[near, 5:6] == doc_ref[0:1, :]) & (
            lax.broadcasted_iota(jnp.int32, (SPAN, length), 0) + cut
            >= lax.broadcasted_iota(jnp.int32, (SPAN, length), 1)
        )
        product = lax.dot_general(
            keys[near, STATE:], keys[:, :STATE], nt, preferred_element_type=jnp.float32
        )
        scores[near, :] = jnp.where(inside, product, 0.0)

    def state_copy(c):
        return remote(
            state_out.at[c], state_in.at[c], state_send.at[c], state_recv.at[c], {"seq": z + 1}
        )

    first = lax.broadcasted_iota(jnp.int32, (SPAN, TILE), 1) < HEAD_SIZE

    @pl.loop(0, chunks)
    def _(c):
        lanes = pl.ds(pl.multiple_of(c * TILE, TILE), TILE)
        own = convolved(x_ref, halo_x, taps_ref, bias_ref, lanes)
        values[:, lanes] = own
        early = lax.broadcasted_iota(jnp.int32, (length, TILE), 1) < HEAD_SIZE
        decay = jnp.where(early, cols_ref[c, :, 2:3], cols_ref[c, :, 3:4])
        scaled = own.astype(jnp.float32) * decay
        high = scaled.astype(jnp.bfloat16)
        low = (scaled - high.astype(jnp.float32)).astype(jnp.bfloat16)
        bmat = keys[:, :STATE]
        tn = (((0,), (0,)), ((), ()))
        state_out[c] = lax.dot_general(
            high, bmat, tn, preferred_element_type=jnp.float32
        ) + lax.dot_general(low, bmat, tn, preferred_element_type=jnp.float32)

        @pl.when(z == 0)
        def _():
            state_copy(c).start()

    squares[...] = jnp.zeros_like(squares)

    @pl.loop(0, chunks)
    def _(c):
        lanes = pl.ds(pl.multiple_of(c * TILE, TILE), TILE)

        @pl.when(z > 0)
        def _():
            state_copy(c).wait_recv()

        @pl.when((z > 0) & (z < n - 1))
        def _():
            top = lax.broadcasted_iota(jnp.int32, (TILE, STATE), 0) < HEAD_SIZE
            final = cols_ref[c, length - 1 : length, 0:2]
            through = jnp.where(top, jnp.exp(-final[:, 0:1]), jnp.exp(-final[:, 1:2]))
            through = through * same_ref[length - 1 : length, 4:5]
            state_out[c] = through * state_in[c] + state_out[c]
            state_copy(c).start()

        incoming = state_in[c]
        in_high = incoming.astype(jnp.bfloat16)
        in_low = (incoming - in_high.astype(jnp.float32)).astype(jnp.bfloat16)
        for cut in range(0, length, SPAN):
            upto = cut + SPAN
            near = pl.ds(cut, SPAN)
            signal = values[0:upto, lanes]
            sums_of = []
            entries = []
            for which in range(2):
                climb = cols_ref[c, near, which : which + 1]
                gap = rows_ref[c, which : which + 1, 0:upto] - climb
                weights = (
                    jnp.exp(jnp.minimum(gap, 0.0))
                    * scores[near, 0:upto]
                    * rows_ref[c, 2 + which : 3 + which, 0:upto]
                )
                high = weights.astype(jnp.bfloat16)
                low = (weights - high.astype(jnp.float32)).astype(jnp.bfloat16)
                sums_of.append(
                    jnp.dot(high, signal, preferred_element_type=jnp.float32)
                    + jnp.dot(low, signal, preferred_element_type=jnp.float32)
                )
                entries.append(jnp.exp(-climb) * same_ref[near, 4:5])
            cmat = keys[near, STATE:]
            arriving = lax.dot_general(
                cmat, in_high, nt, preferred_element_type=jnp.float32
            ) + lax.dot_general(cmat, in_low, nt, preferred_element_type=jnp.float32)
            mixed = (
                jnp.where(first, sums_of[0], sums_of[1])
                + skip_ref[:, lanes] * values[near, lanes].astype(jnp.float32)
                + arriving * jnp.where(first, entries[0], entries[1])
            )
            result = mixed * jax.nn.silu(z_ref[near, lanes].astype(jnp.float32))
            gated[near, lanes] = result
            squares[near, :] += result * result

    for rank in range(1, n):
        @pl.when(z + 1 == rank)
        def _():
            for part in range(1, PARTS):
                w_copy(rank, part).start()

        @pl.when(z + 1 < rank)
        def _():
            for part in range(PARTS):
                w_copy(rank, part).start()

    def tile_copy(which, k, slot_of):
        return remote(
            tiles.at[which, slot_of], tiles.at[which, slot_of], tile_send.at[which, k],
            tile_recv.at[which, slot_of], {"head": lax.rem(h + k, heads)},
        )

    def scale_of(which, partial, count):
        column = jnp.broadcast_to(jnp.sum(partial, axis=1, keepdims=True), (length, TILE))
        tiles[which, h] = jnp.transpose(column)[0:8, :]
        for k in range(1, heads):
            tile_copy(which, k, h).start()
        for k in range(1, heads):
            tile_copy(which, k, lax.rem(h + k, heads)).wait()
        total = tiles[which, 0]
        for head in range(1, heads):
            total = total + tiles[which, head]
        scale = lax.rsqrt(total / count + EPSILON)
        return jnp.transpose(jnp.broadcast_to(scale[0:1, :], (TILE, length)))

    squares[...] = scale_of(0, squares[...], inner)

    @pl.loop(0, chunks)
    def _(c):
        lanes = pl.ds(pl.multiple_of(c * TILE, TILE), TILE)
        normed[:, lanes] = (gated[:, lanes] * squares[...] * gain_ref[:, lanes]).astype(jnp.bfloat16)

    load_out.wait()

    def project(head, slot_of):
        @pl.loop(0, length // LOSS_ROWS)
        def _(step):
            near = pl.ds(pl.multiple_of(step * LOSS_ROWS, LOSS_ROWS), LOSS_ROWS)
            share_out[slot_of, near, :] = jnp.dot(
                normed[near, :],
                ow_buf[:, pl.ds(pl.multiple_of(head * share, TILE), share)],
                preferred_element_type=jnp.float32,
            )

    def share_copy(slot_of, target):
        return remote(
            share_out.at[slot_of], share_in.at[slot_of], share_send.at[slot_of],
            share_recv.at[slot_of], {"head": target},
        )

    project(lax.rem(twin + 2, heads), 0)
    share_copy(0, twin).start()
    project(side, 1)
    share_copy(0, twin).wait_recv()
    share_out[1] = share_out[1] + share_in[0]
    share_copy(1, side).start()
    project(twin, 2)
    share_copy(2, twin).start()
    project(h, 3)

    for rank in range(n):
        @pl.when(z == rank)
        def _():
            for source, part in legs(rank)[0]:
                w_pass_on(rank, source, part)

    share_copy(2, twin).wait_recv()
    share_copy(1, side).wait_recv()

    @pl.loop(0, length // LOSS_ROWS)
    def _(step):
        near = pl.ds(pl.multiple_of(step * LOSS_ROWS, LOSS_ROWS), LOSS_ROWS)
        total = share_out[3, near, :] + share_in[2, near, :] + share_in[1, near, :]
        block_ref[near, :] = (res_ref[near, :].astype(jnp.float32) + total).astype(jnp.bfloat16)

    square = jnp.zeros((length, TILE), jnp.float32)
    for cut in range(0, share, TILE):
        piece = block_ref[:, cut : cut + TILE].astype(jnp.float32)
        square = square + piece * piece
    squares[...] = scale_of(1, square, features)
    for cut in range(0, share, TILE):
        piece = block_ref[:, cut : cut + TILE].astype(jnp.float32)
        hid[:, cut : cut + TILE] = (
            piece * squares[...] * final_ref[:, cut : cut + TILE]
        ).astype(jnp.bfloat16)

    full[z, :, pl.ds(pl.multiple_of(h * share, TILE), share)] = hid[...]

    half_rows = length // 2

    def slot(block, head, half):
        near = pl.ds(half * half_rows, half_rows)
        return full.at[block, near, pl.ds(pl.multiple_of(head * share, TILE), share)]

    def ship(sems, block, head, half, target, first=False):
        place = slot(block, head, half)
        return remote(
            hid.at[pl.ds(half * half_rows, half_rows), :] if first else place, place,
            sems.at[block, half], arrive.at[block, head, half], target,
        )

    def right(block, half, first=False):
        return ship(along_send.at[0], block, h, half, {"seq": z + 1}, first)

    def left(block, half, first=False):
        return ship(along_send.at[1], block, h, half, {"seq": z - 1}, first)

    def across(block, half, first=False):
        return ship(side_send, block, h, half, {"head": side}, first)

    def twinned(kind, block, head, half, first=False):
        return ship(along_send.at[2 + kind], block, head, half, {"head": twin}, first)

    def arrived(block, head, half):
        twinned(0, block, head, half).wait_recv()

    for half in range(2):
        @pl.when(z < n - 1)
        def _():
            right(z, half, True).start()

        @pl.when(z > 0)
        def _():
            left(z, half, True).start()

        across(z, half, True).start()
        twinned(0, z, h, half, True).start()

    def mark_copy(block, head):
        return remote(
            marks.at[block, :, pl.ds(pl.multiple_of(head * TILE, TILE), TILE)], parts.at[me],
            mark_send.at[block, head], mark_recv.at[me], {"seq": block, "head": head},
        )

    live, start_column = widths[0], 0
    for rank in range(1, n):
        live = jnp.where(z == rank, widths[rank], live)
        start_column = jnp.where(z == rank, starts[rank], start_column)
    start_column = h * columns + start_column
    width = w_buf.shape[1]

    def compute(block, half):
        @pl.loop(0, half_rows // LOSS_ROWS)
        def _(step):
            at = pl.multiple_of(half * half_rows + step * LOSS_ROWS, LOSS_ROWS)
            logits = jnp.dot(
                full[block, pl.ds(at, LOSS_ROWS), :], w_buf[...], preferred_element_type=jnp.float32
            )
            wanted = tgts[block, 0:1, pl.ds(at, LOSS_ROWS)]
            wanted = jnp.transpose(jnp.broadcast_to(wanted, (TILE, LOSS_ROWS))) - start_column
            lane = lax.broadcasted_iota(jnp.int32, (LOSS_ROWS, TILE), 1)
            pieces = []
            for cut in range(0, width, TILE):
                piece = logits[:, cut : cut + TILE]
                if cut + TILE > min(widths):
                    piece = jnp.where(lane + cut < live, piece, LOW)
                pieces.append(piece)
            peak = pieces[0]
            for piece in pieces[1:]:
                peak = jnp.maximum(peak, piece)
            peak = jnp.max(peak, axis=1, keepdims=True)
            total = jnp.zeros((LOSS_ROWS, TILE), jnp.float32)
            picked = jnp.zeros((LOSS_ROWS, TILE), jnp.float32)
            for index, piece in enumerate(pieces):
                total = total + jnp.exp(piece - peak)
                here = lane + index * TILE == wanted
                if (index + 1) * TILE > min(widths):
                    here = here & (lane + index * TILE < live)
                picked = picked + jnp.where(here, piece, 0.0)
            total = jnp.sum(total, axis=1, keepdims=True)
            picked = jnp.sum(picked, axis=1, keepdims=True)
            tile = jnp.where(lane == 0, peak, jnp.where(lane == 1, total, picked))
            marks[block, :, pl.ds(at, LOSS_ROWS)] = jnp.transpose(tile)[0:8, :]

        @pl.loop(half * heads // 2, (half + 1) * heads // 2)
        def _(head):
            @pl.when((block != z) | (head != h))
            def _():
                mark_copy(block, head).start()

    def relay(block, half):
        arrived(block, side, half)
        twinned(1, block, side, half).start()

    def finish(block, half):
        arrived(block, twin, half)
        arrived(block, lax.rem(twin + 2, heads), half)
        compute(block, half)

    for rank in range(n):
        @pl.when(z == rank)
        def _():
            for source, part in legs(rank)[1]:
                w_pass_on(rank, source, part)

    def embedding_here():
        for k in range(1, n):
            tell(k, lax.rem(z + n - k, n)).wait()
        for rank in range(n):
            @pl.when(z == rank)
            def _():
                load_own(rank).wait()
                for source in range(n):
                    if source == rank:
                        continue
                    for hop in range(1, groups):
                        other = lax.rem(g + groups - hop, groups)
                        for part in range(PARTS):
                            place = w_place(rank, source, other, part)
                            remote(
                                place, place, y_send.at[source, part, hop],
                                y_recv.at[other, source, part], {"groups": other},
                            ).wait_recv()

    def over_step(step, act):
        if step == 0:
            act(z)
            return

        @pl.when(z >= step)
        def _():
            act(z - step)

        @pl.when(z + step < n)
        def _():
            act(z + step)

    def relay_step(step):
        over_step(step, lambda block: [relay(block, half) for half in range(2)])

    def finish_step(step):
        over_step(step, lambda block: [finish(block, half) for half in range(2)])

    def last_step(step):
        def act(block):
            for half in range(2):
                relay(block, half)
                finish(block, half)

        over_step(step, act)

    for step in range(1, n):
        for half in range(2):
            @pl.when(z >= step)
            def _():
                block = z - step
                arrived(block, h, half)

                @pl.when(z < n - 1)
                def _():
                    right(block, half).start()

                across(block, half).start()
                twinned(0, block, h, half).start()

            @pl.when(z + step < n)
            def _():
                block = z + step
                arrived(block, h, half)

                @pl.when(z > 0)
                def _():
                    left(block, half).start()

                across(block, half).start()
                twinned(0, block, h, half).start()

        if step == 1:
            relay_step(0)
        at_end = (z == 0) | (z == n - 1)
        if step == 1:
            @pl.when(at_end)
            def _():
                embedding_here()
                finish_step(0)

        if step == min(2, n - 1):
            @pl.when(jnp.logical_not(at_end))
            def _():
                embedding_here()
                finish_step(0)

        if step > 1:
            relay_step(step - 1)
            finish_step(step - 1)
    last_step(n - 1)

    @pl.when(z < n - 1)
    def _():
        for copy in halo_copies():
            copy.wait_send()

        @pl.loop(0, chunks)
        def _(c):
            state_copy(c).wait_send()

    for slot_of, target in ((0, twin), (1, side), (2, twin)):
        share_copy(slot_of, target).wait_send()
    for rank in range(n):
        @pl.when(z != rank)
        def _():
            for part in range(PARTS):
                w_copy(rank, part).wait_send()

        @pl.when(z == rank)
        def _():
            for source in range(n):
                for part in range(PARTS):
                    for hop in range(1, groups if source != rank else 1):
                        w_forward(rank, source, part, hop).wait_send()

    for block in range(n):
        for half in range(2):
            @pl.when((z < n - 1) & (z >= block))
            def _():
                right(block, half).wait_send()

            @pl.when((z > 0) & (z <= block))
            def _():
                left(block, half).wait_send()

            across(block, half).wait_send()
            twinned(0, block, h, half).wait_send()
            twinned(1, block, side, half).wait_send()

    parts[me] = marks[z, :, pl.ds(pl.multiple_of(h * TILE, TILE), TILE)]

    @pl.loop(1, total_peers)
    def _(k):
        there, where_head = peer(k)
        flat = there * heads + where_head
        remote(
            parts.at[flat], parts.at[flat], mark_send.at[there, where_head], mark_recv.at[flat],
            {"seq": there, "head": where_head},
        ).wait()

    peak = parts[0, 0:1, :]
    for flat in range(1, total_peers):
        peak = jnp.maximum(peak, parts[flat, 0:1, :])
    total = jnp.zeros((1, TILE), jnp.float32)
    picked = jnp.zeros((1, TILE), jnp.float32)
    for flat in range(total_peers):
        total = total + parts[flat, 1:2, :] * jnp.exp(parts[flat, 0:1, :] - peak)
        picked = picked + parts[flat, 2:3, :]
    losses = peak + jnp.log(total) - picked
    mine = jnp.sum(member_ref[...] * losses, axis=1, keepdims=True)
    sums[me] = jnp.broadcast_to(mine, sums.shape[1:])

    def sum_copy(k, slot_of):
        there, where_head = peer(k)
        return remote(
            sums.at[slot_of], sums.at[slot_of], sum_send.at[k], sum_recv.at[slot_of],
            {"seq": there, "head": where_head},
        )

    @pl.loop(1, total_peers)
    def _(k):
        sum_copy(k, me).start()

    @pl.loop(1, total_peers)
    def _(k):
        sum_copy(k, lax.rem(me + k, total_peers)).wait()

    grand = sums[0]
    for flat in range(1, total_peers):
        grand = grand + sums[flat]
    out_ref[...] = grand


def widths_of(columns, n):
    tiles = columns // TILE
    counts = [tiles // n + (rank < tiles % n) for rank in range(n)]
    if n > 2:
        counts[1] += 1
        counts[n - 1] -= 1
    return tuple(count * TILE for count in counts)


def fits(length, inner_here, share, depth, columns, n, heads, groups):
    widths = widths_of(columns, n)
    features = n * depth
    room = 2 * features * (n * length + max(widths) + inner_here)
    room += 4 * (length * inner_here * 4 + 6 * length * share + length * length)
    even = [inner_here % TILE, share % TILE, columns % TILE, depth % (groups * PARTS * 16)]
    even += [length % SPAN, length % (2 * LOSS_ROWS), length - heads * TILE, heads - 4]
    even += [share * heads - features]
    return not any(even) and n > 1 and min(widths) > 0 and room < 56 * 2**20


def block_stage(operands, whole, member, n, heads, groups):
    x_in, res = operands[0], operands[13]
    out_weight, lm_weight = whole
    length, inner_here = x_in.shape
    share = res.shape[1]
    features = out_weight.shape[1]
    widths = widths_of(lm_weight.shape[1], n)
    width = max(widths)
    peers = n * heads
    chunks = inner_here // TILE
    dma = pltpu.SemaphoreType.DMA
    vmem = pltpu.VMEM
    f32, bf16 = jnp.float32, jnp.bfloat16
    return pl.pallas_call(
        functools.partial(block_kernel, n, heads, groups, inner_here * heads, features, widths),
        out_shape=[
            jax.ShapeDtypeStruct((length, share), bf16),
            jax.ShapeDtypeStruct(member.shape, f32),
        ],
        in_specs=[pl.BlockSpec(memory_space=pltpu.VMEM)] * (len(operands) + 1)
        + [pl.BlockSpec(memory_space=pl.ANY)] * 2,
        out_specs=[pl.BlockSpec(memory_space=pltpu.VMEM)] * 2,
        scratch_shapes=[
            vmem((inner_here, features), bf16),
            vmem((features, width), bf16),
            vmem((n, length, features), bf16),
            vmem((n, 8, length), jnp.int32),
            vmem((n, 8, length), f32),
            vmem((peers, 8, TILE), f32),
            vmem((peers,) + member.shape, f32),
            vmem((HALO, inner_here), bf16),
            vmem((HALO, 2 * STATE), bf16),
            vmem((length + HALO, TILE), f32),
            vmem((KERNEL - 1, length, TILE), f32),
            vmem((length, inner_here), bf16),
            vmem((length, 2 * STATE), bf16),
            vmem((length, length), f32),
            vmem((chunks, TILE, STATE), f32),
            vmem((chunks, TILE, STATE), f32),
            vmem((length, inner_here), f32),
            vmem((length, TILE), f32),
            vmem((2, heads, 8, length), f32),
            vmem((length, inner_here), bf16),
            vmem((4, length, share), f32),
            vmem((3, length, share), f32),
            vmem((length, share), bf16),
            dma((2,)),
            dma((2,)),
            dma((2,)),
            dma((n, PARTS)),
            dma((n, PARTS)),
            dma((n, PARTS, groups)),
            dma((groups, n, PARTS)),
            dma((chunks,)),
            dma((chunks,)),
            dma((2, heads)),
            dma((2, heads)),
            dma((3,)),
            dma((3,)),
            dma((4, n, 2)),
            dma((n, 2)),
            dma((n, heads, 2)),
            dma((n,)),
            dma((n,)),
            dma((n, heads)),
            dma((peers,)),
            dma((peers,)),
            dma((peers,)),
        ],
        compiler_params=pltpu.CompilerParams(
            collective_id=0, has_side_effects=True, vmem_limit_bytes=63 * 2**20
        ),
        cost_estimate=pl.CostEstimate(
            flops=2 * n * length * features * width, bytes_accessed=4 * 10**7, transcendentals=10**7
        ),
    )(*operands, member, *whole)


def fused_fits(residual, x_in, lm_weight):
    length, inner_here = x_in.shape
    depth, columns = lm_weight.shape
    sizes = [lax.axis_size(axis) for axis in ("seq", "head", "groups")]
    return fits(
        length, inner_here, residual.shape[1], depth, columns, *sizes
    )


def fused(
    residual,
    x_in,
    bc_in,
    z_in,
    dt_raw,
    dt_bias,
    decay_rate,
    d_skip,
    conv_x_weight,
    conv_x_bias,
    conv_bc_weight,
    conv_bc_bias,
    norm_gain,
    out_weight,
    final_gain,
    lm_weight,
    targets,
    doc_lengths,
):
    length, _ = x_in.shape
    heads_here = dt_raw.shape[0]
    share = residual.shape[1]
    head_rank = lax.axis_index("head")
    offset_here = lax.axis_index("seq") * length
    positions = offset_here + jnp.arange(length, dtype=jnp.int32)
    doc_ids = document_of(positions, doc_lengths)
    before = document_of(jnp.reshape(offset_here - 1, (1,)), doc_lengths)[0]
    steps = jax.nn.softplus(dt_raw + dt_bias[:, None])
    climb = jnp.cumsum(steps * decay_rate[:, None], axis=1)
    last = (doc_ids == doc_ids[length - 1]).astype(jnp.float32)
    tail = jnp.exp(climb - climb[:, length - 1 :]) * last[None, :] * steps
    couples = heads_here // 2
    rows = jnp.concatenate(
        [climb.reshape(couples, 2, length), steps.reshape(couples, 2, length)], axis=1
    )
    cols = jnp.concatenate(
        [climb.reshape(couples, 2, length), tail.reshape(couples, 2, length)], axis=1
    ).transpose(0, 2, 1)
    flags = [document_of(positions - lag, doc_lengths) == doc_ids for lag in range(KERNEL)]
    flags += [doc_ids == before, doc_ids, doc_ids, doc_ids]
    same = jnp.stack([flag.astype(jnp.float32) for flag in flags], axis=1)
    doc_row = jnp.broadcast_to(doc_ids.astype(jnp.float32)[None, :], (8, length))
    documents = -(-doc_lengths.shape[0] // 8) * 8
    own_ids = lax.dynamic_slice_in_dim(doc_ids, head_rank * TILE, TILE, 0)
    member = (own_ids[None, :] == jnp.arange(documents, dtype=jnp.int32)[:, None]).astype(
        jnp.float32
    )
    final = lax.dynamic_slice_in_dim(final_gain, head_rank * share, share, 0)
    operands = [
        x_in,
        z_in,
        bc_in,
        conv_x_weight.astype(jnp.float32),
        conv_x_bias.astype(jnp.float32)[None, :],
        conv_bc_weight.astype(jnp.float32),
        conv_bc_bias.astype(jnp.float32)[None, :],
        cols,
        rows,
        same,
        doc_row,
        jnp.repeat(d_skip, HEAD_SIZE)[None, :],
        norm_gain.astype(jnp.float32)[None, :],
        residual,
        final.astype(jnp.float32)[None, :],
        jnp.broadcast_to(targets[None, :], (8, length)),
    ]
    sizes = [lax.axis_size(axis) for axis in ("seq", "head", "groups")]
    block_out, sums = block_stage(
        operands, (out_weight, lm_weight), member, *sizes
    )
    sums = sums[: doc_lengths.shape[0], 0]
    return (block_out, sums / doc_lengths.astype(jnp.float32))


def local(
    residual,
    x_in,
    bc_in,
    z_in,
    dt_raw,
    dt_bias,
    decay_rate,
    d_skip,
    conv_x_weight,
    conv_x_bias,
    conv_bc_weight,
    conv_bc_bias,
    norm_gain,
    out_weight,
    final_gain,
    lm_weight,
    targets,
    doc_lengths,
):
    if fused_fits(residual, x_in, lm_weight):
        return fused(
            residual,
            x_in,
            bc_in,
            z_in,
            dt_raw,
            dt_bias,
            decay_rate,
            d_skip,
            conv_x_weight,
            conv_x_bias,
            conv_bc_weight,
            conv_bc_bias,
            norm_gain,
            out_weight,
            final_gain,
            lm_weight,
            targets,
            doc_lengths,
        )
    length = x_in.shape[0]
    inner_here = x_in.shape[1]
    heads_here = dt_raw.shape[0]
    seq_rank = lax.axis_index("seq")
    head_rank = lax.axis_index("head")
    offset_here = seq_rank * length
    positions = offset_here + jnp.arange(length, dtype=jnp.int32)
    doc_ids = document_of(positions, doc_lengths)
    columns_here = lm_weight.shape[1]
    devices = lax.axis_size("seq")
    width = -(-columns_here // (devices * 128)) * 128

    def window(rank):
        return jnp.minimum(rank * width, columns_here - width)

    depth = lm_weight.shape[0]
    vocab_weight = jnp.zeros((depth * devices, width), lm_weight.dtype)
    group = lax.axis_index("groups")
    groups = lax.axis_size("groups")
    band = depth // groups
    pieces = [
        lax.dynamic_slice(
            lm_weight, (group * band, window((seq_rank + by) % devices)), (band, width)
        )
        for by in range(1, devices)
    ]
    aims = [targets]
    for by in range(1, devices):
        aims.append(rotated(targets, "seq", by))
    margin = KERNEL - 1
    rims = shifted(
        jnp.concatenate([x_in[length - margin :], bc_in[length - margin :]], axis=1), "seq", 1
    )
    x_rim, bc_rim = rims[:, :inner_here], rims[:, inner_here:]
    keys_queries = causal_conv(
        bc_in, bc_rim, conv_bc_weight, conv_bc_bias, positions, doc_ids, doc_lengths
    )
    bmat, cmat = keys_queries[:, :STATE], keys_queries[:, STATE:]
    steps = jax.nn.softplus(dt_raw + dt_bias[:, None])
    climb = jnp.cumsum(steps * decay_rate[:, None], axis=1)
    before = document_of(jnp.reshape(offset_here - 1, (1,)), doc_lengths)[0]
    carried = (doc_ids == before).astype(jnp.float32)
    through = jnp.exp(-climb[:, length - 1]) * carried[length - 1]
    same = jnp.stack(
        [
            (document_of(positions - lag, doc_lengths) == doc_ids).astype(jnp.float32)
            for lag in range(KERNEL)
        ],
        axis=1,
    )
    last = (doc_ids == doc_ids[length - 1]).astype(jnp.float32)
    tail = jnp.exp(climb - climb[:, length - 1 :]) * last[None, :] * steps
    couples = heads_here // 2
    rows = jnp.concatenate(
        [climb.reshape(couples, 2, length), steps.reshape(couples, 2, length)], axis=1
    )
    cols = jnp.concatenate(
        [climb.reshape(couples, 2, length), tail.reshape(couples, 2, length)], axis=1
    ).transpose(0, 2, 1)
    rim = jnp.concatenate([jnp.zeros((8 - margin, inner_here), x_rim.dtype), x_rim], axis=0)
    values, own_end = conv_state(
        x_in,
        rim,
        conv_x_weight.astype(jnp.float32),
        conv_x_bias.astype(jnp.float32)[None, :],
        same,
        cols,
        bmat,
    )
    of_head = jnp.arange(inner_here, dtype=jnp.int32)[None, :] // HEAD_SIZE
    spread = (of_head == jnp.arange(heads_here, dtype=jnp.int32)[:, None]).astype(jnp.float32)
    incoming = entering(
        through, own_end.reshape(heads_here, HEAD_SIZE, STATE), "seq"
    ).reshape(inner_here, STATE)
    held_back = lax.optimization_barrier(tuple(pieces[1:]) + (incoming,))
    pieces, incoming = pieces[:1] + list(held_back[:-1]), held_back[-1]
    arrivals = []
    for by in range(1, devices):
        arrivals.append(rotated(pieces[by - 1], "seq", by))
    bands = []
    for by in range(1, devices):
        bands.append(
            [arrivals[by - 1]]
            + [rotated(arrivals[by - 1], "groups", hop) for hop in range(1, groups)]
        )
    order = jnp.arange(length, dtype=jnp.int32)
    inside = (doc_ids[:, None] == doc_ids[None, :]) & (order[:, None] >= order[None, :])
    scores = jnp.where(
        inside,
        lax.dot_general(
            cmat, bmat, (((1,), (1,)), ((), ())), preferred_element_type=jnp.float32
        ),
        0.0,
    )
    skip = jnp.dot(d_skip[None, :], spread, precision=HIGH)
    output = within(values, scores, cols, rows, skip)
    entry = jnp.dot((jnp.exp(-climb) * carried[None, :]).T, spread, precision=HIGH)
    arriving = lax.dot_general(
        cmat.astype(jnp.float32), incoming, (((1,), (1,)), ((), ())), precision=HALF
    )
    gated = (output + arriving * entry) * jax.nn.silu(z_in.astype(jnp.float32))
    square_sum = lax.psum(jnp.sum(gated * gated, axis=1), "head")
    scale = lax.rsqrt(square_sum / INNER + EPSILON)
    normed = (gated * scale[:, None] * norm_gain.astype(jnp.float32)[None, :]).astype(jnp.bfloat16)
    share = residual.shape[1]
    projected = scattered_product(normed, out_weight, "head")
    block_out = (residual.astype(jnp.float32) + projected).astype(jnp.bfloat16)
    widened = block_out.astype(jnp.float32)
    square_total = lax.psum(jnp.sum(widened * widened, axis=1), "head")
    gain_part = lax.dynamic_slice_in_dim(final_gain, head_rank * share, share, 0)
    final_scale = lax.rsqrt(square_total / D + EPSILON)
    hidden_part = (widened * final_scale[:, None] * gain_part.astype(jnp.float32)[None, :]).astype(
        jnp.bfloat16
    )
    own = lax.dynamic_slice_in_dim(lm_weight, window(seq_rank), width, 1)
    vocab_weight = lax.dynamic_update_slice_in_dim(vocab_weight, own, seq_rank * depth, 0)
    for by in range(1, devices):
        source = (seq_rank + devices - by) % devices
        for hop in range(groups):
            start = source * depth + (group + groups - hop) % groups * band
            vocab_weight = lax.dynamic_update_slice_in_dim(
                vocab_weight, bands[by - 1][hop], start, 0
            )
    column = jnp.arange(width, dtype=jnp.int32)
    first = head_rank * columns_here + window(seq_rank)
    live = column + window(seq_rank) >= seq_rank * width
    marks = jnp.zeros((3, length * devices), jnp.float32)
    for by in range(devices):
        source = (seq_rank + devices - by) % devices
        if by and by % 4 == 0:
            hidden_part, marks = lax.optimization_barrier((hidden_part, marks))
        rows = rotated(hidden_part, "seq", by) if by else hidden_part
        hidden = gathered_features(rows, "head")
        logits = jnp.dot(hidden, vocab_weight, preferred_element_type=jnp.float32)
        logits = jnp.where(live[None, :], logits, LOW)
        peak = jnp.max(logits, axis=1)
        wanted = aims[by] - first
        total = jnp.sum(jnp.exp(logits - peak[:, None]), axis=1)
        picked = jnp.sum(
            jnp.where((column[None, :] == wanted[:, None]) & live[None, :], logits, 0.0), axis=1
        )
        marks = lax.dynamic_update_slice_in_dim(
            marks, jnp.stack([peak, total, picked]), source * length, 1
        )
    for axis in ("head", "seq"):
        every_mark = lax.all_gather(marks, axis)
        peak = jnp.max(every_mark[:, 0], axis=0)
        total = jnp.sum(every_mark[:, 1] * jnp.exp(every_mark[:, 0] - peak[None]), axis=0)
        marks = jnp.stack([peak, total, jnp.sum(every_mark[:, 2], axis=0)])
    losses = marks[0] + jnp.log(marks[1]) - marks[2]
    every = document_of(jnp.arange(length * devices, dtype=jnp.int32), doc_lengths)
    documents = jnp.arange(doc_lengths.shape[0], dtype=jnp.int32)
    member = every[None, :] == documents[:, None]
    sums = jnp.sum(jnp.where(member, losses[None, :], 0.0), axis=1)
    return (block_out, sums / doc_lengths.astype(jnp.float32))


def solution(mesh):
    in_specs = (
        P(("groups", "seq"), "head"),
        P(("groups", "seq"), "head"),
        P(("groups", "seq"), None),
        P(("groups", "seq"), "head"),
        P("head", ("groups", "seq")),
        P("head"),
        P("head"),
        P("head"),
        P(None, "head"),
        P("head"),
        P(),
        P(),
        P("head"),
        P("head", None),
        P(),
        P("seq", "head"),
        P(("groups", "seq")),
        P("groups"),
    )
    out_specs = (P(("groups", "seq"), "head"), P("groups"))


    return jax.shard_map(local, mesh=mesh, in_specs=in_specs, out_specs=out_specs, check_vma=False)
```

```python
import functools

import jax
import jax.numpy as jnp
from jax import lax
from jax.experimental import pallas as pl
from jax.experimental.pallas import tpu as pltpu
from jax.sharding import PartitionSpec as P

D = 2560
HEAD_SIZE = 64
STATE = 128
KERNEL = 4
SPAN = 256
INNER = 5120


EPSILON = 1e-05
HIGH = lax.Precision.HIGHEST
HALF = lax.Precision.HIGH
LOW = -1e30
MESH = pl.DeviceIdType.MESH


def shifted(array, axis, by):
    length = lax.axis_size(axis)
    pairs = [(i, i + by) for i in range(length) if 0 <= i + by < length]
    return lax.ppermute(array, axis, pairs)


def rotated(array, axis, by):
    length = lax.axis_size(axis)
    return lax.ppermute(array, axis, [(i, (i + by) % length) for i in range(length)])


def sibling(array, axis):
    length = lax.axis_size(axis)
    return lax.ppermute(array, axis, [(i, i ^ 1) for i in range(length)])


def scattered_product(normed, weight, axis):
    length = lax.axis_size(axis)
    rank = lax.axis_index(axis)
    chips = length // 2
    share = weight.shape[1] // length

    def columns(core):
        return jnp.concatenate(
            [
                lax.dynamic_slice_in_dim(
                    weight, ((rank // 2 + by) % chips * 2 + core) * share, share, 1
                )
                for by in range(chips)
            ],
            axis=1,
        )

    theirs = columns(1 - rank % 2)
    ours = columns(rank % 2)
    other = jnp.dot(normed, theirs, preferred_element_type=jnp.float32)
    arrived = sibling(other, axis)
    pair = jnp.dot(normed, ours, preferred_element_type=jnp.float32) + arrived
    total = pair[:, :share]
    for by in range(1, chips):
        total = total + rotated(pair[:, by * share : (by + 1) * share], axis, 2 * by)
    return total


def gathered_features(part, axis):
    length = lax.axis_size(axis)
    rank = lax.axis_index(axis)
    chips = length // 2
    rows, share = part.shape
    column = [part] + [rotated(part, axis, 2 * by) for by in range(1, chips)]
    joined = jnp.concatenate(column, axis=1)
    twin = sibling(joined, axis)
    full = jnp.zeros((rows, share * length), part.dtype)
    for by in range(chips):
        source = (rank + 2 * (chips - by)) % length
        piece = slice(by * share, (by + 1) * share)
        full = lax.dynamic_update_slice_in_dim(full, joined[:, piece], source * share, 1)
        full = lax.dynamic_update_slice_in_dim(full, twin[:, piece], (source ^ 1) * share, 1)
    return full


def entering(through, state, axis):
    length = lax.axis_size(axis)
    tag = jnp.broadcast_to(through[:, None, None], (through.shape[0], 8, state.shape[2]))
    packed = shifted(jnp.concatenate([state, tag], axis=1), axis, 1)
    extent = state.shape[1]
    reach = 1
    while reach < length:
        earlier = shifted(packed, axis, reach)
        decay = packed[:, extent : extent + 1, :]
        packed = jnp.concatenate(
            [packed[:, :extent] + decay * earlier[:, :extent], decay * earlier[:, extent:]], axis=1
        )
        reach *= 2
    return packed[:, :extent]


def document_of(positions, doc_lengths):
    starts = jnp.cumsum(doc_lengths) - doc_lengths
    return jnp.sum((positions[:, None] >= starts[None, :]).astype(jnp.int32), axis=1) - 1


def causal_conv(signal, rim_rows, weight, bias, positions, doc_ids, doc_lengths):
    length = signal.shape[0]
    taps = weight.shape[0]
    joined = jnp.concatenate([rim_rows, signal], axis=0).astype(jnp.float32)
    total = jnp.zeros(signal.shape, jnp.float32) + bias.astype(jnp.float32)[None, :]
    for offset in range(taps):
        lag = taps - 1 - offset
        source = document_of(positions - lag, doc_lengths)
        same = (source == doc_ids).astype(jnp.float32)
        total = (
            total
            + weight[offset].astype(jnp.float32)[None, :]
            * joined[offset : offset + length]
            * same[:, None]
        )
    return jax.nn.silu(total).astype(jnp.bfloat16)


def conv_state_kernel(x_ref, rim_ref, taps_ref, bias_ref, same_ref, cols_ref, bmat_ref, values_ref, state_ref, held):
    length, lanes = x_ref.shape
    taps = taps_ref.shape[0]
    held[0:8, :] = rim_ref[...].astype(jnp.float32)
    held[8:, :] = x_ref[...].astype(jnp.float32)
    total = jnp.zeros((length, lanes), jnp.float32) + bias_ref[...]
    for offset in range(taps):
        lag = taps - 1 - offset
        rows = held[8 - lag : 8 - lag + length, :]
        total = total + taps_ref[offset : offset + 1, :] * rows * same_ref[:, lag : lag + 1]
    values = jax.nn.silu(total).astype(jnp.bfloat16)
    values_ref[...] = values
    first = lax.broadcasted_iota(jnp.int32, (length, lanes), 1) < HEAD_SIZE
    tail = jnp.where(first, cols_ref[0, :, 2:3], cols_ref[0, :, 3:4])
    scaled = values.astype(jnp.float32) * tail
    high = scaled.astype(jnp.bfloat16)
    low = (scaled - high.astype(jnp.float32)).astype(jnp.bfloat16)
    bmat = bmat_ref[...]
    dims = (((0,), (0,)), ((), ()))
    state_ref[...] = lax.dot_general(
        high, bmat, dims, preferred_element_type=jnp.float32
    ) + lax.dot_general(low, bmat, dims, preferred_element_type=jnp.float32)


def within_kernel(values_ref, scores_ref, cols_ref, rows_ref, skip_ref, out_ref):
    length, lanes = values_ref.shape
    for cut in range(0, length, SPAN):
        upto = cut + SPAN
        values = values_ref[0:upto, :]
        scores = scores_ref[cut:upto, 0:upto]
        parts = []
        for which in range(2):
            gap = rows_ref[0, which : which + 1, 0:upto] - cols_ref[0, cut:upto, which : which + 1]
            weights = (
                jnp.exp(jnp.minimum(gap, 0.0)) * scores * rows_ref[0, 2 + which : 3 + which, 0:upto]
            )
            high = weights.astype(jnp.bfloat16)
            low = (weights - high.astype(jnp.float32)).astype(jnp.bfloat16)
            parts.append(
                jnp.dot(high, values, preferred_element_type=jnp.float32)
                + jnp.dot(low, values, preferred_element_type=jnp.float32)
            )
        first = lax.broadcasted_iota(jnp.int32, (SPAN, lanes), 1) < HEAD_SIZE
        own = values_ref[cut:upto, :].astype(jnp.float32)
        out_ref[cut:upto, :] = jnp.where(first, parts[0], parts[1]) + skip_ref[...] * own


def conv_state(x_in, rim, taps, bias, same, cols, bmat):
    length, inner_here = x_in.shape
    lanes = 2 * HEAD_SIZE
    return pl.pallas_call(
        conv_state_kernel,
        grid=(inner_here // lanes,),
        in_specs=[
            pl.BlockSpec((length, lanes), lambda i: (0, i)),
            pl.BlockSpec((8, lanes), lambda i: (0, i)),
            pl.BlockSpec((taps.shape[0], lanes), lambda i: (0, i)),
            pl.BlockSpec((1, lanes), lambda i: (0, i)),
            pl.BlockSpec(same.shape, lambda i: (0, 0)),
            pl.BlockSpec((1, length, 4), lambda i: (i, 0, 0)),
            pl.BlockSpec(bmat.shape, lambda i: (0, 0)),
        ],
        out_specs=[
            pl.BlockSpec((length, lanes), lambda i: (0, i)),
            pl.BlockSpec((lanes, STATE), lambda i: (i, 0)),
        ],
        out_shape=[
            jax.ShapeDtypeStruct((length, inner_here), jnp.bfloat16),
            jax.ShapeDtypeStruct((inner_here, STATE), jnp.float32),
        ],
        scratch_shapes=[pltpu.VMEM((length + 8, lanes), jnp.float32)],
        cost_estimate=pl.CostEstimate(flops=10**9, bytes_accessed=6 * 10**6, transcendentals=10**6),
    )(x_in, rim, taps, bias, same, cols, bmat)


def within(values, scores, cols, rows, skip):
    length, inner_here = values.shape
    lanes = 2 * HEAD_SIZE
    return pl.pallas_call(
        within_kernel,
        grid=(inner_here // lanes,),
        in_specs=[
            pl.BlockSpec((length, lanes), lambda i: (0, i)),
            pl.BlockSpec(scores.shape, lambda i: (0, 0)),
            pl.BlockSpec((1, length, 4), lambda i: (i, 0, 0)),
            pl.BlockSpec((1, 4, length), lambda i: (i, 0, 0)),
            pl.BlockSpec((1, lanes), lambda i: (0, i)),
        ],
        out_specs=pl.BlockSpec((length, lanes), lambda i: (0, i)),
        out_shape=jax.ShapeDtypeStruct((length, inner_here), jnp.float32),
        cost_estimate=pl.CostEstimate(flops=8 * 10**9, bytes_accessed=20 * 10**6, transcendentals=10**7),
    )(values, scores, cols, rows, skip)


TILE = 128
LOSS_ROWS = 256
HALO = 16
PARTS = 4


def block_kernel(
    n, heads, groups, inner, features, widths,
    x_ref, z_ref, bc_ref, taps_ref, bc_taps_ref, res_ref, tgt_ref, dt_ref, table_ref,
    lens_ref, dt_bias_ref, rate_ref, skip_ref, ow_ref, lm_ref,
    block_ref, out_ref,
    ow_buf, w_buf, full, tgts, marks, parts, sums, halo_x, halo_bc, held, masks, carried, rows, cols, values, keys,
    scores, state_out, state_in, gated, squares, tiles, normed, share_out, share_in, hid,
    load_sem, halo_send, halo_recv, w_send, w_recv, y_send, y_recv, state_send, state_recv,
    tile_send, tile_recv, share_send, share_recv,
    along_send, side_send, arrive, tgt_send, tgt_recv, mark_send, mark_recv, sum_send, sum_recv,
):
    g = lax.axis_index("groups")
    z = lax.axis_index("seq")
    h = lax.axis_index("head")
    length, inner_here = x_ref.shape
    share = res_ref.shape[1]
    depth, columns = lm_ref.shape
    starts = [sum(widths[:rank]) for rank in range(n)]
    band = depth // groups
    sub = band // PARTS
    total_peers = n * heads
    me = z * heads + h
    twin = h + 1 - 2 * lax.rem(h, 2)
    side = lax.rem(h + 2, heads)
    chunks = inner_here // TILE

    def remote(src, dst, send, recv, target):
        return pltpu.make_async_remote_copy(
            src_ref=src, dst_ref=dst, send_sem=send, recv_sem=recv,
            device_id=target, device_id_type=MESH,
        )

    def peer(k):
        flat = lax.rem(me + k, total_peers)
        return flat // heads, lax.rem(flat, heads)

    load_out = pltpu.make_async_copy(ow_ref, ow_buf, load_sem.at[0])
    load_out.start()

    def load_own(rank):
        return pltpu.make_async_copy(
            lm_ref.at[:, pl.ds(starts[rank], widths[rank])],
            w_buf.at[pl.ds(rank * depth, depth), pl.ds(0, widths[rank])],
            load_sem.at[1],
        )

    for rank in range(n):
        @pl.when(z == rank)
        def _():
            load_own(rank).start()

    barrier = pltpu.get_barrier_semaphore()

    @pl.loop(1, total_peers)
    def _(k):
        there, where_head = peer(k)
        pl.semaphore_signal(
            barrier, inc=1, device_id={"seq": there, "head": where_head}, device_id_type=MESH
        )

    for hop in range(1, groups):
        pl.semaphore_signal(
            barrier, inc=1, device_id={"groups": lax.rem(g + hop, groups)}, device_id_type=MESH
        )
    pl.semaphore_wait(barrier, total_peers - 1 + groups - 1)

    def halo_copies():
        tail_rows = pl.ds(length - HALO, HALO)
        return [
            remote(x_ref.at[tail_rows, :], halo_x, halo_send.at[0], halo_recv.at[0], {"seq": z + 1}),
            remote(bc_ref.at[tail_rows, :], halo_bc, halo_send.at[1], halo_recv.at[1], {"seq": z + 1}),
        ]

    @pl.when(z < n - 1)
    def _():
        for copy in halo_copies():
            copy.start()

    def w_rows(source, group, part):
        return pl.ds(pl.multiple_of(source * depth + group * band + part * sub, 16), sub)

    def w_copy(rank, part):
        columns_there = pl.ds(starts[rank], widths[rank])
        return remote(
            lm_ref.at[pl.ds(pl.multiple_of(g * band + part * sub, 16), sub), columns_there],
            w_buf.at[w_rows(z, g, part), pl.ds(0, widths[rank])],
            w_send.at[rank, part],
            w_recv.at[z, part],
            {"seq": rank},
        )

    def w_place(rank, source, group, part):
        return w_buf.at[w_rows(source, group, part), pl.ds(0, widths[rank])]

    def w_forward(rank, source, part, hop):
        place = w_place(rank, source, g, part)
        return remote(
            place, place, y_send.at[source, part, hop], y_recv.at[g, source, part],
            {"groups": lax.rem(g + hop, groups)},
        )

    def w_pass_on(rank, source, part):
        place = w_place(rank, source, g, part)
        remote(
            place, place, w_send.at[source, part], w_recv.at[source, part], {"seq": source}
        ).wait_recv()
        for hop in range(1, groups):
            w_forward(rank, source, part, hop).start()

    def legs(rank):
        far_first = list(range(n - 1, rank, -1)) + list(range(rank))
        every = [(source, part) for source in far_first for part in range(PARTS)]

        def early(source, part):
            if source < rank:
                return source == rank - 1 and (part == 0 or rank in (1, n - 1))
            if rank == 0:
                return source != 2
            return source > rank + 1 or (rank == n - 2 and part < PARTS // 2)

        return [leg for leg in every if early(*leg)], [leg for leg in every if not early(*leg)]

    for rank in range(n):
        @pl.when(z > rank)
        def _():
            for part in range(PARTS):
                w_copy(rank, part).start()

        @pl.when(z + 1 == rank)
        def _():
            w_copy(rank, 0).start()

    def tell(k, source):
        return remote(
            tgt_ref, tgts.at[source], tgt_send.at[k], tgt_recv.at[source],
            {"seq": lax.rem(z + k, n)},
        )

    for k in range(1, n):
        tell(k, z).start()
    tgts[z] = tgt_ref[...]

    starts_of = [jnp.int32(0)]
    for document in range(lens_ref.shape[0] - 1):
        starts_of.append(starts_of[-1] + lens_ref[document])

    def document(positions):
        total = (positions >= starts_of[0]).astype(jnp.int32)
        for start in starts_of[1:]:
            total = total + (positions >= start).astype(jnp.int32)
        return total

    offset_here = z * length

    def along(shape, axis):
        return lax.broadcasted_iota(jnp.int32, shape, axis) + offset_here

    here_heads = dt_ref.shape[0]
    head_row = lax.broadcasted_iota(jnp.int32, (here_heads, length), 0)
    lane_row = lax.broadcasted_iota(jnp.int32, (here_heads, length), 1)
    shift = jnp.zeros((here_heads, length), jnp.float32)
    rate = jnp.zeros((here_heads, length), jnp.float32)
    for head in range(here_heads):
        shift = jnp.where(head_row == head, dt_bias_ref[head], shift)
        rate = jnp.where(head_row == head, rate_ref[head], rate)
    raw = dt_ref[...] + shift
    steps = jnp.maximum(raw, 0.0) + jnp.log1p(jnp.exp(-jnp.abs(raw)))
    climb = steps * rate
    by = 1
    while by < length:
        climb = climb + jnp.where(lane_row >= by, pltpu.roll(climb, by, 1), 0.0)
        by *= 2
    is_last = document(along((here_heads, length), 1)) == document(offset_here + length - 1)
    leave = jnp.where(is_last, jnp.exp(climb - climb[:, length - 1 :]) * steps, 0.0)
    for c in range(chunks):
        pair = slice(2 * c, 2 * c + 2)
        rows[c, 0:2, :] = climb[pair]
        rows[c, 2:4, :] = steps[pair]
        rows[c, 4:6, :] = leave[pair]
        rows[c, 6:8, :] = leave[pair]

    token = along((length, TILE), 0)
    at_token = document(token)
    for lag in range(1, KERNEL):
        masks[lag - 1] = (document(token - lag) == at_token).astype(jnp.float32)
    carried[...] = (at_token == document(offset_here - 1)).astype(jnp.float32)

    @pl.when(z == 0)
    def _():
        halo_x[...] = jnp.zeros_like(halo_x)
        halo_bc[...] = jnp.zeros_like(halo_bc)
        state_in[...] = jnp.zeros_like(state_in)

    @pl.when(z > 0)
    def _():
        for copy in halo_copies():
            copy.wait_recv()

    def convolved(signal, halo, weight, bias, lanes):
        weight = weight[:, lanes].astype(jnp.float32)
        held[0:HALO, :] = halo[:, lanes].astype(jnp.float32)
        held[HALO:, :] = signal[:, lanes].astype(jnp.float32)
        total = jnp.zeros((length, TILE), jnp.float32) + bias
        for offset in range(KERNEL):
            lag = KERNEL - 1 - offset
            term = weight[offset : offset + 1, :] * held[HALO - lag : HALO - lag + length, :]
            total = total + (term * masks[lag - 1] if lag else term)
        return jax.nn.silu(total).astype(jnp.bfloat16)

    def line(at):
        return table_ref[pl.ds(at, 1), :]

    for half in range(2):
        lanes = pl.ds(half * STATE, STATE)
        keys[:, lanes] = convolved(bc_ref, halo_bc, bc_taps_ref, line(2 * chunks + half), lanes)
    nt = (((1,), (1,)), ((), ()))
    for cut in range(0, length, SPAN):
        near = pl.ds(cut, SPAN)
        target, source = along((SPAN, length), 0) + cut, along((SPAN, length), 1)
        inside = (document(target) == document(source)) & (target >= source)
        product = lax.dot_general(
            keys[near, STATE:], keys[:, :STATE], nt, preferred_element_type=jnp.float32
        )
        scores[near, :] = jnp.where(inside, product, 0.0)

    def state_copy(c):
        return remote(
            state_out.at[c], state_in.at[c], state_send.at[c], state_recv.at[c], {"seq": z + 1}
        )

    first = lax.broadcasted_iota(jnp.int32, (SPAN, TILE), 1) < HEAD_SIZE

    @pl.loop(0, chunks)
    def _(c):
        lanes = pl.ds(pl.multiple_of(c * TILE, TILE), TILE)
        own = convolved(x_ref, halo_x, taps_ref, line(c), lanes)
        values[:, lanes] = own
        early = lax.broadcasted_iota(jnp.int32, (length, TILE), 1) < HEAD_SIZE
        cols[c] = jnp.transpose(rows[c])
        decay = jnp.where(early, cols[c, :, 4:5], cols[c, :, 5:6])
        scaled = own.astype(jnp.float32) * decay
        high = scaled.astype(jnp.bfloat16)
        low = (scaled - high.astype(jnp.float32)).astype(jnp.bfloat16)
        bmat = keys[:, :STATE]
        tn = (((0,), (0,)), ((), ()))
        state_out[c] = lax.dot_general(
            high, bmat, tn, preferred_element_type=jnp.float32
        ) + lax.dot_general(low, bmat, tn, preferred_element_type=jnp.float32)

        @pl.when(z == 0)
        def _():
            state_copy(c).start()

    squares[...] = jnp.zeros_like(squares)

    @pl.loop(0, chunks)
    def _(c):
        lanes = pl.ds(pl.multiple_of(c * TILE, TILE), TILE)

        @pl.when(z > 0)
        def _():
            state_copy(c).wait_recv()

        @pl.when((z > 0) & (z < n - 1))
        def _():
            top = lax.broadcasted_iota(jnp.int32, (TILE, STATE), 0) < HEAD_SIZE
            final = cols[c, length - 1 : length, 0:2]
            through = jnp.where(top, jnp.exp(-final[:, 0:1]), jnp.exp(-final[:, 1:2]))
            through = through * carried[length - 1 : length, 0:1]
            state_out[c] = through * state_in[c] + state_out[c]
            state_copy(c).start()

        skip = jnp.where(first, skip_ref[2 * c], skip_ref[2 * c + 1])
        incoming = state_in[c]
        in_high = incoming.astype(jnp.bfloat16)
        in_low = (incoming - in_high.astype(jnp.float32)).astype(jnp.bfloat16)
        for cut in range(0, length, SPAN):
            upto = cut + SPAN
            near = pl.ds(cut, SPAN)
            signal = values[0:upto, lanes]
            sums_of = []
            entries = []
            for which in range(2):
                climb = cols[c, near, which : which + 1]
                gap = rows[c, which : which + 1, 0:upto] - climb
                weights = (
                    jnp.exp(jnp.minimum(gap, 0.0))
                    * scores[near, 0:upto]
                    * rows[c, 2 + which : 3 + which, 0:upto]
                )
                high = weights.astype(jnp.bfloat16)
                low = (weights - high.astype(jnp.float32)).astype(jnp.bfloat16)
                sums_of.append(
                    jnp.dot(high, signal, preferred_element_type=jnp.float32)
                    + jnp.dot(low, signal, preferred_element_type=jnp.float32)
                )
                entries.append(jnp.exp(-climb))
            cmat = keys[near, STATE:]
            arriving = lax.dot_general(
                cmat, in_high, nt, preferred_element_type=jnp.float32
            ) + lax.dot_general(cmat, in_low, nt, preferred_element_type=jnp.float32)
            mixed = (
                jnp.where(first, sums_of[0], sums_of[1])
                + skip * values[near, lanes].astype(jnp.float32)
                + arriving * (jnp.where(first, entries[0], entries[1]) * carried[near, :])
            )
            result = mixed * jax.nn.silu(z_ref[near, lanes].astype(jnp.float32))
            gated[near, lanes] = result
            squares[near, :] += result * result

    for rank in range(1, n):
        @pl.when(z + 1 == rank)
        def _():
            for part in range(1, PARTS):
                w_copy(rank, part).start()

        @pl.when(z + 1 < rank)
        def _():
            for part in range(PARTS):
                w_copy(rank, part).start()

    def tile_copy(which, k, slot_of):
        return remote(
            tiles.at[which, slot_of], tiles.at[which, slot_of], tile_send.at[which, k],
            tile_recv.at[which, slot_of], {"head": lax.rem(h + k, heads)},
        )

    def scale_of(which, partial, count):
        column = jnp.broadcast_to(jnp.sum(partial, axis=1, keepdims=True), (length, TILE))
        tiles[which, h] = jnp.transpose(column)[0:8, :]
        for k in range(1, heads):
            tile_copy(which, k, h).start()
        for k in range(1, heads):
            tile_copy(which, k, lax.rem(h + k, heads)).wait()
        total = tiles[which, 0]
        for head in range(1, heads):
            total = total + tiles[which, head]
        scale = lax.rsqrt(total / count + EPSILON)
        return jnp.transpose(jnp.broadcast_to(scale[0:1, :], (TILE, length)))

    squares[...] = scale_of(0, squares[...], inner)

    @pl.loop(0, chunks)
    def _(c):
        lanes = pl.ds(pl.multiple_of(c * TILE, TILE), TILE)
        normed[:, lanes] = (gated[:, lanes] * squares[...] * line(chunks + c)).astype(jnp.bfloat16)

    load_out.wait()

    def project(head, slot_of):
        @pl.loop(0, length // LOSS_ROWS)
        def _(step):
            near = pl.ds(pl.multiple_of(step * LOSS_ROWS, LOSS_ROWS), LOSS_ROWS)
            share_out[slot_of, near, :] = jnp.dot(
                normed[near, :],
                ow_buf[:, pl.ds(pl.multiple_of(head * share, TILE), share)],
                preferred_element_type=jnp.float32,
            )

    def share_copy(slot_of, target):
        return remote(
            share_out.at[slot_of], share_in.at[slot_of], share_send.at[slot_of],
            share_recv.at[slot_of], {"head": target},
        )

    project(lax.rem(twin + 2, heads), 0)
    share_copy(0, twin).start()
    project(side, 1)
    share_copy(0, twin).wait_recv()
    share_out[1] = share_out[1] + share_in[0]
    share_copy(1, side).start()
    project(twin, 2)
    share_copy(2, twin).start()
    project(h, 3)

    for rank in range(n):
        @pl.when(z == rank)
        def _():
            for source, part in legs(rank)[0]:
                w_pass_on(rank, source, part)

    share_copy(2, twin).wait_recv()
    share_copy(1, side).wait_recv()

    @pl.loop(0, length // LOSS_ROWS)
    def _(step):
        near = pl.ds(pl.multiple_of(step * LOSS_ROWS, LOSS_ROWS), LOSS_ROWS)
        total = share_out[3, near, :] + share_in[2, near, :] + share_in[1, near, :]
        block_ref[near, :] = (res_ref[near, :].astype(jnp.float32) + total).astype(jnp.bfloat16)

    square = jnp.zeros((length, TILE), jnp.float32)
    for cut in range(0, share, TILE):
        piece = block_ref[:, cut : cut + TILE].astype(jnp.float32)
        square = square + piece * piece
    squares[...] = scale_of(1, square, features)
    for cut in range(0, share, TILE):
        piece = block_ref[:, cut : cut + TILE].astype(jnp.float32)
        hid[:, cut : cut + TILE] = (
            piece * squares[...] * line(2 * chunks + 2 + h * (share // TILE) + cut // TILE)
        ).astype(jnp.bfloat16)

    full[z, :, pl.ds(pl.multiple_of(h * share, TILE), share)] = hid[...]

    half_rows = length // 2

    def near_of(half):
        start = half * half_rows
        return pl.ds(start if isinstance(start, int) else pl.multiple_of(start, 16), half_rows)

    def slot(block, head, half):
        near = near_of(half)
        return full.at[block, near, pl.ds(pl.multiple_of(head * share, TILE), share)]

    def ship(sems, block, head, half, target, first=False):
        place = slot(block, head, half)
        return remote(
            hid.at[near_of(half), :] if first else place, place,
            sems.at[block, half], arrive.at[block, head, half], target,
        )

    def right(block, half, first=False):
        return ship(along_send.at[0], block, h, half, {"seq": z + 1}, first)

    def left(block, half, first=False):
        return ship(along_send.at[1], block, h, half, {"seq": z - 1}, first)

    def across(block, half, first=False):
        return ship(side_send, block, h, half, {"head": side}, first)

    def twinned(kind, block, head, half, first=False):
        return ship(along_send.at[2 + kind], block, head, half, {"head": twin}, first)

    def arrived(block, head, half):
        twinned(0, block, head, half).wait_recv()

    for half in range(2):
        @pl.when(z < n - 1)
        def _():
            right(z, half, True).start()

        @pl.when(z > 0)
        def _():
            left(z, half, True).start()

        across(z, half, True).start()
        twinned(0, z, h, half, True).start()

    def mark_copy(block, head):
        return remote(
            marks.at[block, :, pl.ds(pl.multiple_of(head * TILE, TILE), TILE)], parts.at[me],
            mark_send.at[block, head], mark_recv.at[me], {"seq": block, "head": head},
        )

    live, start_column = widths[0], 0
    for rank in range(1, n):
        live = jnp.where(z == rank, widths[rank], live)
        start_column = jnp.where(z == rank, starts[rank], start_column)
    start_column = h * columns + start_column
    width = w_buf.shape[1]

    def compute(block, half):
        @pl.loop(0, half_rows // LOSS_ROWS)
        def _(step):
            at = pl.multiple_of(half * half_rows + step * LOSS_ROWS, LOSS_ROWS)
            logits = jnp.dot(
                full[block, pl.ds(at, LOSS_ROWS), :], w_buf[...], preferred_element_type=jnp.float32
            )
            wanted = []
            for cut in range(LOSS_ROWS // TILE):
                row = tgts[block, pl.ds(lax.div(at, TILE) + cut, 1), :]
                wanted.append(jnp.transpose(jnp.broadcast_to(row, (TILE, TILE))))
            wanted = jnp.concatenate(wanted, axis=0) - start_column
            lane = lax.broadcasted_iota(jnp.int32, (LOSS_ROWS, TILE), 1)
            pieces = []
            for cut in range(0, width, TILE):
                piece = logits[:, cut : cut + TILE]
                if cut + TILE > min(widths):
                    piece = jnp.where(lane + cut < live, piece, LOW)
                pieces.append(piece)
            peak = pieces[0]
            for piece in pieces[1:]:
                peak = jnp.maximum(peak, piece)
            peak = jnp.max(peak, axis=1, keepdims=True)
            total = jnp.zeros((LOSS_ROWS, TILE), jnp.float32)
            picked = jnp.zeros((LOSS_ROWS, TILE), jnp.float32)
            for index, piece in enumerate(pieces):
                total = total + jnp.exp(piece - peak)
                here = lane + index * TILE == wanted
                if (index + 1) * TILE > min(widths):
                    here = here & (lane + index * TILE < live)
                picked = picked + jnp.where(here, piece, 0.0)
            total = jnp.sum(total, axis=1, keepdims=True)
            picked = jnp.sum(picked, axis=1, keepdims=True)
            tile = jnp.where(lane == 0, peak, jnp.where(lane == 1, total, picked))
            marks[block, :, pl.ds(at, LOSS_ROWS)] = jnp.transpose(tile)[0:8, :]

        @pl.loop(half * (heads // 2), (half + 1) * (heads // 2))
        def _(head):
            @pl.when((block != z) | (head != h))
            def _():
                mark_copy(block, head).start()

    def relay(block, half):
        arrived(block, side, half)
        twinned(1, block, side, half).start()

    def finish(block, half):
        arrived(block, twin, half)
        arrived(block, lax.rem(twin + 2, heads), half)
        compute(block, half)

    for rank in range(n):
        @pl.when(z == rank)
        def _():
            for source, part in legs(rank)[1]:
                w_pass_on(rank, source, part)

    def embedding_here():
        for k in range(1, n):
            tell(k, lax.rem(z + n - k, n)).wait()
        for rank in range(n):
            @pl.when(z == rank)
            def _():
                load_own(rank).wait()
                for source in range(n):
                    if source == rank:
                        continue
                    for hop in range(1, groups):
                        other = lax.rem(g + groups - hop, groups)
                        for part in range(PARTS):
                            place = w_place(rank, source, other, part)
                            remote(
                                place, place, y_send.at[source, part, hop],
                                y_recv.at[other, source, part], {"groups": other},
                            ).wait_recv()

    def over_step(step, act):
        @pl.loop(0, 4 if step else 2)
        def _(turn):
            half = lax.rem(turn, 2)
            block = z - step + 2 * step * lax.div(turn, 2)

            @pl.when((block >= 0) & (block < n))
            def _():
                act(block, half)

    def last_step(block, half):
        relay(block, half)
        finish(block, half)

    for step in range(1, n):
        for half in range(2):
            @pl.when(z >= step)
            def _():
                block = z - step
                arrived(block, h, half)

                @pl.when(z < n - 1)
                def _():
                    right(block, half).start()

                across(block, half).start()
                twinned(0, block, h, half).start()

            @pl.when(z + step < n)
            def _():
                block = z + step
                arrived(block, h, half)

                @pl.when(z > 0)
                def _():
                    left(block, half).start()

                across(block, half).start()
                twinned(0, block, h, half).start()

        if step == 1:
            over_step(0, relay)
        at_end = (z == 0) | (z == n - 1)
        if step == 1:
            @pl.when(at_end)
            def _():
                embedding_here()
                over_step(0, finish)

        if step == min(2, n - 1):
            @pl.when(jnp.logical_not(at_end))
            def _():
                embedding_here()
                over_step(0, finish)

        if step > 1:
            over_step(step - 1, relay)
            over_step(step - 1, finish)
    over_step(n - 1, last_step)

    @pl.when(z < n - 1)
    def _():
        for copy in halo_copies():
            copy.wait_send()

        @pl.loop(0, chunks)
        def _(c):
            state_copy(c).wait_send()

    for slot_of, target in ((0, twin), (1, side), (2, twin)):
        share_copy(slot_of, target).wait_send()
    for rank in range(n):
        @pl.when(z != rank)
        def _():
            for part in range(PARTS):
                w_copy(rank, part).wait_send()

        @pl.when(z == rank)
        def _():
            for source in range(n):
                for part in range(PARTS):
                    for hop in range(1, groups if source != rank else 1):
                        w_forward(rank, source, part, hop).wait_send()

    for block in range(n):
        for half in range(2):
            @pl.when((z < n - 1) & (z >= block))
            def _():
                right(block, half).wait_send()

            @pl.when((z > 0) & (z <= block))
            def _():
                left(block, half).wait_send()

            across(block, half).wait_send()
            twinned(0, block, h, half).wait_send()
            twinned(1, block, side, half).wait_send()

    parts[me] = marks[z, :, pl.ds(pl.multiple_of(h * TILE, TILE), TILE)]

    @pl.loop(1, total_peers)
    def _(k):
        there, where_head = peer(k)
        flat = there * heads + where_head
        remote(
            parts.at[flat], parts.at[flat], mark_send.at[there, where_head], mark_recv.at[flat],
            {"seq": there, "head": where_head},
        ).wait()

    peak = parts[0, 0:1, :]
    for flat in range(1, total_peers):
        peak = jnp.maximum(peak, parts[flat, 0:1, :])
    total = jnp.zeros((1, TILE), jnp.float32)
    picked = jnp.zeros((1, TILE), jnp.float32)
    for flat in range(total_peers):
        total = total + parts[flat, 1:2, :] * jnp.exp(parts[flat, 0:1, :] - peak)
        picked = picked + parts[flat, 2:3, :]
    losses = peak + jnp.log(total) - picked
    member_shape = sums.shape[1:]
    position = along(member_shape, 1) + h * TILE
    member = document(position) == lax.broadcasted_iota(jnp.int32, member_shape, 0) + 1
    mine = jnp.sum(jnp.where(member, losses, 0.0), axis=1, keepdims=True)
    sums[me] = jnp.broadcast_to(mine, sums.shape[1:])

    def sum_copy(k, slot_of):
        there, where_head = peer(k)
        return remote(
            sums.at[slot_of], sums.at[slot_of], sum_send.at[k], sum_recv.at[slot_of],
            {"seq": there, "head": where_head},
        )

    @pl.loop(1, total_peers)
    def _(k):
        sum_copy(k, me).start()

    @pl.loop(1, total_peers)
    def _(k):
        sum_copy(k, lax.rem(me + k, total_peers)).wait()

    grand = sums[0]
    for flat in range(1, total_peers):
        grand = grand + sums[flat]
    out_ref[...] = grand


def widths_of(columns, n):
    tiles = columns // TILE
    counts = [tiles // n + (rank < tiles % n) for rank in range(n)]
    if n > 2:
        counts[1] += 1
        counts[n - 1] -= 1
    return tuple(count * TILE for count in counts)


def fits(length, inner_here, share, depth, columns, n, heads, groups):
    widths = widths_of(columns, n)
    features = n * depth
    room = 2 * features * (n * length + max(widths) + inner_here)
    room += 4 * (length * inner_here * 4 + 6 * length * share + length * length)
    even = [inner_here % TILE, share % TILE, columns % TILE, depth % (groups * PARTS * 16)]
    even += [length % SPAN, length % (2 * LOSS_ROWS), length - heads * TILE, heads - 4]
    even += [share * heads - features]
    return not any(even) and n > 1 and min(widths) > 0 and room < 56 * 2**20


def block_stage(operands, scalars, whole, n, heads, groups):
    x_in, res = operands[0], operands[5]
    out_weight, lm_weight = whole
    length, inner_here = x_in.shape
    share = res.shape[1]
    features = out_weight.shape[1]
    widths = widths_of(lm_weight.shape[1], n)
    width = max(widths)
    peers = n * heads
    chunks = inner_here // TILE
    result = (-(-scalars[0].shape[0] // 8) * 8, TILE)
    dma = pltpu.SemaphoreType.DMA
    vmem = pltpu.VMEM
    f32, bf16 = jnp.float32, jnp.bfloat16
    return pl.pallas_call(
        functools.partial(block_kernel, n, heads, groups, inner_here * heads, features, widths),
        out_shape=[
            jax.ShapeDtypeStruct((length, share), bf16),
            jax.ShapeDtypeStruct(result, f32),
        ],
        in_specs=[pl.BlockSpec(memory_space=pltpu.VMEM)] * len(operands)
        + [pl.BlockSpec(memory_space=pltpu.SMEM)] * len(scalars)
        + [pl.BlockSpec(memory_space=pl.ANY)] * 2,
        out_specs=[pl.BlockSpec(memory_space=pltpu.VMEM)] * 2,
        scratch_shapes=[
            vmem((inner_here, features), bf16),
            vmem((features, width), bf16),
            vmem((n, length, features), bf16),
            vmem((n, heads, TILE), jnp.int32),
            vmem((n, 8, length), f32),
            vmem((peers, 8, TILE), f32),
            vmem((peers,) + result, f32),
            vmem((HALO, inner_here), bf16),
            vmem((HALO, 2 * STATE), bf16),
            vmem((length + HALO, TILE), f32),
            vmem((KERNEL - 1, length, TILE), f32),
            vmem((length, TILE), f32),
            vmem((chunks, 8, length), f32),
            vmem((chunks, length, 8), f32),
            vmem((length, inner_here), bf16),
            vmem((length, 2 * STATE), bf16),
            vmem((length, length), f32),
            vmem((chunks, TILE, STATE), f32),
            vmem((chunks, TILE, STATE), f32),
            vmem((length, inner_here), f32),
            vmem((length, TILE), f32),
            vmem((2, heads, 8, length), f32),
            vmem((length, inner_here), bf16),
            vmem((4, length, share), f32),
            vmem((3, length, share), f32),
            vmem((length, share), bf16),
            dma((2,)),
            dma((2,)),
            dma((2,)),
            dma((n, PARTS)),
            dma((n, PARTS)),
            dma((n, PARTS, groups)),
            dma((groups, n, PARTS)),
            dma((chunks,)),
            dma((chunks,)),
            dma((2, heads)),
            dma((2, heads)),
            dma((3,)),
            dma((3,)),
            dma((4, n, 2)),
            dma((n, 2)),
            dma((n, heads, 2)),
            dma((n,)),
            dma((n,)),
            dma((n, heads)),
            dma((peers,)),
            dma((peers,)),
            dma((peers,)),
        ],
        compiler_params=pltpu.CompilerParams(
            collective_id=0, has_side_effects=True, vmem_limit_bytes=63 * 2**20
        ),
        cost_estimate=pl.CostEstimate(
            flops=2 * n * length * features * width, bytes_accessed=4 * 10**7, transcendentals=10**7
        ),
    )(*operands, *scalars, *whole)


def fused_fits(residual, x_in, lm_weight):
    length, inner_here = x_in.shape
    depth, columns = lm_weight.shape
    sizes = [lax.axis_size(axis) for axis in ("seq", "head", "groups")]
    return fits(
        length, inner_here, residual.shape[1], depth, columns, *sizes
    )


def fused(
    residual,
    x_in,
    bc_in,
    z_in,
    dt_raw,
    dt_bias,
    decay_rate,
    d_skip,
    conv_x_weight,
    conv_x_bias,
    conv_bc_weight,
    conv_bc_bias,
    norm_gain,
    out_weight,
    final_gain,
    lm_weight,
    targets,
    doc_lengths,
):
    table = jnp.concatenate([conv_x_bias, norm_gain, conv_bc_bias, final_gain])
    operands = [
        x_in,
        z_in,
        bc_in,
        conv_x_weight,
        conv_bc_weight,
        residual,
        targets.reshape(-1, TILE),
        dt_raw,
        table.astype(jnp.float32).reshape(-1, TILE),
    ]
    scalars = [doc_lengths, dt_bias, decay_rate, d_skip]
    sizes = [lax.axis_size(axis) for axis in ("seq", "head", "groups")]
    block_out, sums = block_stage(operands, scalars, (out_weight, lm_weight), *sizes)
    sums = sums[: doc_lengths.shape[0], 0]
    return (block_out, sums / doc_lengths.astype(jnp.float32))


def local(
    residual,
    x_in,
    bc_in,
    z_in,
    dt_raw,
    dt_bias,
    decay_rate,
    d_skip,
    conv_x_weight,
    conv_x_bias,
    conv_bc_weight,
    conv_bc_bias,
    norm_gain,
    out_weight,
    final_gain,
    lm_weight,
    targets,
    doc_lengths,
):
    if fused_fits(residual, x_in, lm_weight):
        return fused(
            residual,
            x_in,
            bc_in,
            z_in,
            dt_raw,
            dt_bias,
            decay_rate,
            d_skip,
            conv_x_weight,
            conv_x_bias,
            conv_bc_weight,
            conv_bc_bias,
            norm_gain,
            out_weight,
            final_gain,
            lm_weight,
            targets,
            doc_lengths,
        )
    length = x_in.shape[0]
    inner_here = x_in.shape[1]
    heads_here = dt_raw.shape[0]
    seq_rank = lax.axis_index("seq")
    head_rank = lax.axis_index("head")
    offset_here = seq_rank * length
    positions = offset_here + jnp.arange(length, dtype=jnp.int32)
    doc_ids = document_of(positions, doc_lengths)
    columns_here = lm_weight.shape[1]
    devices = lax.axis_size("seq")
    width = -(-columns_here // (devices * 128)) * 128

    def window(rank):
        return jnp.minimum(rank * width, columns_here - width)

    depth = lm_weight.shape[0]
    vocab_weight = jnp.zeros((depth * devices, width), lm_weight.dtype)
    group = lax.axis_index("groups")
    groups = lax.axis_size("groups")
    band = depth // groups
    pieces = [
        lax.dynamic_slice(
            lm_weight, (group * band, window((seq_rank + by) % devices)), (band, width)
        )
        for by in range(1, devices)
    ]
    aims = [targets]
    for by in range(1, devices):
        aims.append(rotated(targets, "seq", by))
    margin = KERNEL - 1
    rims = shifted(
        jnp.concatenate([x_in[length - margin :], bc_in[length - margin :]], axis=1), "seq", 1
    )
    x_rim, bc_rim = rims[:, :inner_here], rims[:, inner_here:]
    keys_queries = causal_conv(
        bc_in, bc_rim, conv_bc_weight, conv_bc_bias, positions, doc_ids, doc_lengths
    )
    bmat, cmat = keys_queries[:, :STATE], keys_queries[:, STATE:]
    steps = jax.nn.softplus(dt_raw + dt_bias[:, None])
    climb = jnp.cumsum(steps * decay_rate[:, None], axis=1)
    before = document_of(jnp.reshape(offset_here - 1, (1,)), doc_lengths)[0]
    carried = (doc_ids == before).astype(jnp.float32)
    through = jnp.exp(-climb[:, length - 1]) * carried[length - 1]
    same = jnp.stack(
        [
            (document_of(positions - lag, doc_lengths) == doc_ids).astype(jnp.float32)
            for lag in range(KERNEL)
        ],
        axis=1,
    )
    last = (doc_ids == doc_ids[length - 1]).astype(jnp.float32)
    tail = jnp.exp(climb - climb[:, length - 1 :]) * last[None, :] * steps
    couples = heads_here // 2
    rows = jnp.concatenate(
        [climb.reshape(couples, 2, length), steps.reshape(couples, 2, length)], axis=1
    )
    cols = jnp.concatenate(
        [climb.reshape(couples, 2, length), tail.reshape(couples, 2, length)], axis=1
    ).transpose(0, 2, 1)
    rim = jnp.concatenate([jnp.zeros((8 - margin, inner_here), x_rim.dtype), x_rim], axis=0)
    values, own_end = conv_state(
        x_in,
        rim,
        conv_x_weight.astype(jnp.float32),
        conv_x_bias.astype(jnp.float32)[None, :],
        same,
        cols,
        bmat,
    )
    of_head = jnp.arange(inner_here, dtype=jnp.int32)[None, :] // HEAD_SIZE
    spread = (of_head == jnp.arange(heads_here, dtype=jnp.int32)[:, None]).astype(jnp.float32)
    incoming = entering(
        through, own_end.reshape(heads_here, HEAD_SIZE, STATE), "seq"
    ).reshape(inner_here, STATE)
    held_back = lax.optimization_barrier(tuple(pieces[1:]) + (incoming,))
    pieces, incoming = pieces[:1] + list(held_back[:-1]), held_back[-1]
    arrivals = []
    for by in range(1, devices):
        arrivals.append(rotated(pieces[by - 1], "seq", by))
    bands = []
    for by in range(1, devices):
        bands.append(
            [arrivals[by - 1]]
            + [rotated(arrivals[by - 1], "groups", hop) for hop in range(1, groups)]
        )
    order = jnp.arange(length, dtype=jnp.int32)
    inside = (doc_ids[:, None] == doc_ids[None, :]) & (order[:, None] >= order[None, :])
    scores = jnp.where(
        inside,
        lax.dot_general(
            cmat, bmat, (((1,), (1,)), ((), ())), preferred_element_type=jnp.float32
        ),
        0.0,
    )
    skip = jnp.dot(d_skip[None, :], spread, precision=HIGH)
    output = within(values, scores, cols, rows, skip)
    entry = jnp.dot((jnp.exp(-climb) * carried[None, :]).T, spread, precision=HIGH)
    arriving = lax.dot_general(
        cmat.astype(jnp.float32), incoming, (((1,), (1,)), ((), ())), precision=HALF
    )
    gated = (output + arriving * entry) * jax.nn.silu(z_in.astype(jnp.float32))
    square_sum = lax.psum(jnp.sum(gated * gated, axis=1), "head")
    scale = lax.rsqrt(square_sum / INNER + EPSILON)
    normed = (gated * scale[:, None] * norm_gain.astype(jnp.float32)[None, :]).astype(jnp.bfloat16)
    share = residual.shape[1]
    projected = scattered_product(normed, out_weight, "head")
    block_out = (residual.astype(jnp.float32) + projected).astype(jnp.bfloat16)
    widened = block_out.astype(jnp.float32)
    square_total = lax.psum(jnp.sum(widened * widened, axis=1), "head")
    gain_part = lax.dynamic_slice_in_dim(final_gain, head_rank * share, share, 0)
    final_scale = lax.rsqrt(square_total / D + EPSILON)
    hidden_part = (widened * final_scale[:, None] * gain_part.astype(jnp.float32)[None, :]).astype(
        jnp.bfloat16
    )
    own = lax.dynamic_slice_in_dim(lm_weight, window(seq_rank), width, 1)
    vocab_weight = lax.dynamic_update_slice_in_dim(vocab_weight, own, seq_rank * depth, 0)
    for by in range(1, devices):
        source = (seq_rank + devices - by) % devices
        for hop in range(groups):
            start = source * depth + (group + groups - hop) % groups * band
            vocab_weight = lax.dynamic_update_slice_in_dim(
                vocab_weight, bands[by - 1][hop], start, 0
            )
    column = jnp.arange(width, dtype=jnp.int32)
    first = head_rank * columns_here + window(seq_rank)
    live = column + window(seq_rank) >= seq_rank * width
    marks = jnp.zeros((3, length * devices), jnp.float32)
    for by in range(devices):
        source = (seq_rank + devices - by) % devices
        if by and by % 4 == 0:
            hidden_part, marks = lax.optimization_barrier((hidden_part, marks))
        rows = rotated(hidden_part, "seq", by) if by else hidden_part
        hidden = gathered_features(rows, "head")
        logits = jnp.dot(hidden, vocab_weight, preferred_element_type=jnp.float32)
        logits = jnp.where(live[None, :], logits, LOW)
        peak = jnp.max(logits, axis=1)
        wanted = aims[by] - first
        total = jnp.sum(jnp.exp(logits - peak[:, None]), axis=1)
        picked = jnp.sum(
            jnp.where((column[None, :] == wanted[:, None]) & live[None, :], logits, 0.0), axis=1
        )
        marks = lax.dynamic_update_slice_in_dim(
            marks, jnp.stack([peak, total, picked]), source * length, 1
        )
    for axis in ("head", "seq"):
        every_mark = lax.all_gather(marks, axis)
        peak = jnp.max(every_mark[:, 0], axis=0)
        total = jnp.sum(every_mark[:, 1] * jnp.exp(every_mark[:, 0] - peak[None]), axis=0)
        marks = jnp.stack([peak, total, jnp.sum(every_mark[:, 2], axis=0)])
    losses = marks[0] + jnp.log(marks[1]) - marks[2]
    every = document_of(jnp.arange(length * devices, dtype=jnp.int32), doc_lengths)
    documents = jnp.arange(doc_lengths.shape[0], dtype=jnp.int32)
    member = every[None, :] == documents[:, None]
    sums = jnp.sum(jnp.where(member, losses[None, :], 0.0), axis=1)
    return (block_out, sums / doc_lengths.astype(jnp.float32))


def solution(mesh):
    in_specs = (
        P(("groups", "seq"), "head"),
        P(("groups", "seq"), "head"),
        P(("groups", "seq"), None),
        P(("groups", "seq"), "head"),
        P("head", ("groups", "seq")),
        P("head"),
        P("head"),
        P("head"),
        P(None, "head"),
        P("head"),
        P(),
        P(),
        P("head"),
        P("head", None),
        P(),
        P("seq", "head"),
        P(("groups", "seq")),
        P("groups"),
    )
    out_specs = (P(("groups", "seq"), "head"), P("groups"))


    return jax.shard_map(local, mesh=mesh, in_specs=in_specs, out_specs=out_specs, check_vma=False)
```

```python
import functools

import jax
import jax.numpy as jnp
from jax import lax
from jax.experimental import pallas as pl
from jax.experimental.pallas import tpu as pltpu
from jax.sharding import PartitionSpec as P

D = 2560
HEAD_SIZE = 64
STATE = 128
KERNEL = 4
SPAN = 256
INNER = 5120


EPSILON = 1e-05
HIGH = lax.Precision.HIGHEST
HALF = lax.Precision.HIGH
LOW = -1e30
MESH = pl.DeviceIdType.MESH


def shifted(array, axis, by):
    length = lax.axis_size(axis)
    pairs = [(i, i + by) for i in range(length) if 0 <= i + by < length]
    return lax.ppermute(array, axis, pairs)


def rotated(array, axis, by):
    length = lax.axis_size(axis)
    return lax.ppermute(array, axis, [(i, (i + by) % length) for i in range(length)])


def sibling(array, axis):
    length = lax.axis_size(axis)
    return lax.ppermute(array, axis, [(i, i ^ 1) for i in range(length)])


def scattered_product(normed, weight, axis):
    length = lax.axis_size(axis)
    rank = lax.axis_index(axis)
    chips = length // 2
    share = weight.shape[1] // length

    def columns(core):
        return jnp.concatenate(
            [
                lax.dynamic_slice_in_dim(
                    weight, ((rank // 2 + by) % chips * 2 + core) * share, share, 1
                )
                for by in range(chips)
            ],
            axis=1,
        )

    theirs = columns(1 - rank % 2)
    ours = columns(rank % 2)
    other = jnp.dot(normed, theirs, preferred_element_type=jnp.float32)
    arrived = sibling(other, axis)
    pair = jnp.dot(normed, ours, preferred_element_type=jnp.float32) + arrived
    total = pair[:, :share]
    for by in range(1, chips):
        total = total + rotated(pair[:, by * share : (by + 1) * share], axis, 2 * by)
    return total


def gathered_features(part, axis):
    length = lax.axis_size(axis)
    rank = lax.axis_index(axis)
    chips = length // 2
    rows, share = part.shape
    column = [part] + [rotated(part, axis, 2 * by) for by in range(1, chips)]
    joined = jnp.concatenate(column, axis=1)
    twin = sibling(joined, axis)
    full = jnp.zeros((rows, share * length), part.dtype)
    for by in range(chips):
        source = (rank + 2 * (chips - by)) % length
        piece = slice(by * share, (by + 1) * share)
        full = lax.dynamic_update_slice_in_dim(full, joined[:, piece], source * share, 1)
        full = lax.dynamic_update_slice_in_dim(full, twin[:, piece], (source ^ 1) * share, 1)
    return full


def entering(through, state, axis):
    length = lax.axis_size(axis)
    tag = jnp.broadcast_to(through[:, None, None], (through.shape[0], 8, state.shape[2]))
    packed = shifted(jnp.concatenate([state, tag], axis=1), axis, 1)
    extent = state.shape[1]
    reach = 1
    while reach < length:
        earlier = shifted(packed, axis, reach)
        decay = packed[:, extent : extent + 1, :]
        packed = jnp.concatenate(
            [packed[:, :extent] + decay * earlier[:, :extent], decay * earlier[:, extent:]], axis=1
        )
        reach *= 2
    return packed[:, :extent]


def document_of(positions, doc_lengths):
    starts = jnp.cumsum(doc_lengths) - doc_lengths
    return jnp.sum((positions[:, None] >= starts[None, :]).astype(jnp.int32), axis=1) - 1


def causal_conv(signal, rim_rows, weight, bias, positions, doc_ids, doc_lengths):
    length = signal.shape[0]
    taps = weight.shape[0]
    joined = jnp.concatenate([rim_rows, signal], axis=0).astype(jnp.float32)
    total = jnp.zeros(signal.shape, jnp.float32) + bias.astype(jnp.float32)[None, :]
    for offset in range(taps):
        lag = taps - 1 - offset
        source = document_of(positions - lag, doc_lengths)
        same = (source == doc_ids).astype(jnp.float32)
        total = (
            total
            + weight[offset].astype(jnp.float32)[None, :]
            * joined[offset : offset + length]
            * same[:, None]
        )
    return jax.nn.silu(total).astype(jnp.bfloat16)


def conv_state_kernel(x_ref, rim_ref, taps_ref, bias_ref, same_ref, cols_ref, bmat_ref, values_ref, state_ref, held):
    length, lanes = x_ref.shape
    taps = taps_ref.shape[0]
    held[0:8, :] = rim_ref[...].astype(jnp.float32)
    held[8:, :] = x_ref[...].astype(jnp.float32)
    total = jnp.zeros((length, lanes), jnp.float32) + bias_ref[...]
    for offset in range(taps):
        lag = taps - 1 - offset
        rows = held[8 - lag : 8 - lag + length, :]
        total = total + taps_ref[offset : offset + 1, :] * rows * same_ref[:, lag : lag + 1]
    values = jax.nn.silu(total).astype(jnp.bfloat16)
    values_ref[...] = values
    first = lax.broadcasted_iota(jnp.int32, (length, lanes), 1) < HEAD_SIZE
    tail = jnp.where(first, cols_ref[0, :, 2:3], cols_ref[0, :, 3:4])
    scaled = values.astype(jnp.float32) * tail
    high = scaled.astype(jnp.bfloat16)
    low = (scaled - high.astype(jnp.float32)).astype(jnp.bfloat16)
    bmat = bmat_ref[...]
    dims = (((0,), (0,)), ((), ()))
    state_ref[...] = lax.dot_general(
        high, bmat, dims, preferred_element_type=jnp.float32
    ) + lax.dot_general(low, bmat, dims, preferred_element_type=jnp.float32)


def within_kernel(values_ref, scores_ref, cols_ref, rows_ref, skip_ref, out_ref):
    length, lanes = values_ref.shape
    for cut in range(0, length, SPAN):
        upto = cut + SPAN
        values = values_ref[0:upto, :]
        scores = scores_ref[cut:upto, 0:upto]
        parts = []
        for which in range(2):
            gap = rows_ref[0, which : which + 1, 0:upto] - cols_ref[0, cut:upto, which : which + 1]
            weights = (
                jnp.exp(jnp.minimum(gap, 0.0)) * scores * rows_ref[0, 2 + which : 3 + which, 0:upto]
            )
            high = weights.astype(jnp.bfloat16)
            low = (weights - high.astype(jnp.float32)).astype(jnp.bfloat16)
            parts.append(
                jnp.dot(high, values, preferred_element_type=jnp.float32)
                + jnp.dot(low, values, preferred_element_type=jnp.float32)
            )
        first = lax.broadcasted_iota(jnp.int32, (SPAN, lanes), 1) < HEAD_SIZE
        own = values_ref[cut:upto, :].astype(jnp.float32)
        out_ref[cut:upto, :] = jnp.where(first, parts[0], parts[1]) + skip_ref[...] * own


def conv_state(x_in, rim, taps, bias, same, cols, bmat):
    length, inner_here = x_in.shape
    lanes = 2 * HEAD_SIZE
    return pl.pallas_call(
        conv_state_kernel,
        grid=(inner_here // lanes,),
        in_specs=[
            pl.BlockSpec((length, lanes), lambda i: (0, i)),
            pl.BlockSpec((8, lanes), lambda i: (0, i)),
            pl.BlockSpec((taps.shape[0], lanes), lambda i: (0, i)),
            pl.BlockSpec((1, lanes), lambda i: (0, i)),
            pl.BlockSpec(same.shape, lambda i: (0, 0)),
            pl.BlockSpec((1, length, 4), lambda i: (i, 0, 0)),
            pl.BlockSpec(bmat.shape, lambda i: (0, 0)),
        ],
        out_specs=[
            pl.BlockSpec((length, lanes), lambda i: (0, i)),
            pl.BlockSpec((lanes, STATE), lambda i: (i, 0)),
        ],
        out_shape=[
            jax.ShapeDtypeStruct((length, inner_here), jnp.bfloat16),
            jax.ShapeDtypeStruct((inner_here, STATE), jnp.float32),
        ],
        scratch_shapes=[pltpu.VMEM((length + 8, lanes), jnp.float32)],
        cost_estimate=pl.CostEstimate(flops=10**9, bytes_accessed=6 * 10**6, transcendentals=10**6),
    )(x_in, rim, taps, bias, same, cols, bmat)


def within(values, scores, cols, rows, skip):
    length, inner_here = values.shape
    lanes = 2 * HEAD_SIZE
    return pl.pallas_call(
        within_kernel,
        grid=(inner_here // lanes,),
        in_specs=[
            pl.BlockSpec((length, lanes), lambda i: (0, i)),
            pl.BlockSpec(scores.shape, lambda i: (0, 0)),
            pl.BlockSpec((1, length, 4), lambda i: (i, 0, 0)),
            pl.BlockSpec((1, 4, length), lambda i: (i, 0, 0)),
            pl.BlockSpec((1, lanes), lambda i: (0, i)),
        ],
        out_specs=pl.BlockSpec((length, lanes), lambda i: (0, i)),
        out_shape=jax.ShapeDtypeStruct((length, inner_here), jnp.float32),
        cost_estimate=pl.CostEstimate(flops=8 * 10**9, bytes_accessed=20 * 10**6, transcendentals=10**7),
    )(values, scores, cols, rows, skip)


TILE = 128
LOSS_ROWS = 256
HALO = 16
PARTS = 4
SPLIT = 2


def block_kernel(
    n, heads, groups, inner, features, widths,
    x_ref, z_ref, bc_ref, taps_ref, bc_taps_ref, res_ref, tgt_ref, dt_ref, table_ref,
    lens_ref, dt_bias_ref, rate_ref, skip_ref, ow_ref, lm_ref,
    block_ref, out_ref,
    ow_buf, w_buf, full, tgts, marks, parts, sums, halo_x, halo_bc, held, masks, carried, rows, cols, values, keys,
    scores, state_out, state_in, gated, squares, tiles, normed, share_out, share_in, hid,
    load_sem, halo_send, halo_recv, w_send, w_recv, y_send, y_recv, state_send, state_recv,
    tile_send, tile_recv, share_send, share_recv,
    along_send, side_send, arrive, tgt_send, tgt_recv, mark_send, mark_recv, sum_send, sum_recv,
):
    g = lax.axis_index("groups")
    z = lax.axis_index("seq")
    h = lax.axis_index("head")
    length, inner_here = x_ref.shape
    share = res_ref.shape[1]
    depth, columns = lm_ref.shape
    starts = [sum(widths[:rank]) for rank in range(n)]
    band = depth // groups
    sub = band // PARTS
    total_peers = n * heads
    me = z * heads + h
    twin = h + 1 - 2 * lax.rem(h, 2)
    side = lax.rem(h + 2, heads)
    chunks = inner_here // TILE

    def remote(src, dst, send, recv, target):
        return pltpu.make_async_remote_copy(
            src_ref=src, dst_ref=dst, send_sem=send, recv_sem=recv,
            device_id=target, device_id_type=MESH,
        )

    def peer(k):
        flat = lax.rem(me + k, total_peers)
        return flat // heads, lax.rem(flat, heads)

    load_out = pltpu.make_async_copy(ow_ref, ow_buf, load_sem.at[0])
    load_out.start()

    def load_own(rank):
        return pltpu.make_async_copy(
            lm_ref.at[:, pl.ds(starts[rank], widths[rank])],
            w_buf.at[pl.ds(rank * depth, depth), pl.ds(0, widths[rank])],
            load_sem.at[1],
        )

    for rank in range(n):
        @pl.when(z == rank)
        def _():
            load_own(rank).start()

    barrier = pltpu.get_barrier_semaphore()

    @pl.loop(1, total_peers)
    def _(k):
        there, where_head = peer(k)
        pl.semaphore_signal(
            barrier, inc=1, device_id={"seq": there, "head": where_head}, device_id_type=MESH
        )

    for hop in range(1, groups):
        pl.semaphore_signal(
            barrier, inc=1, device_id={"groups": lax.rem(g + hop, groups)}, device_id_type=MESH
        )
    pl.semaphore_wait(barrier, total_peers - 1 + groups - 1)

    def halo_copies():
        tail_rows = pl.ds(length - HALO, HALO)
        return [
            remote(x_ref.at[tail_rows, :], halo_x, halo_send.at[0], halo_recv.at[0], {"seq": z + 1}),
            remote(bc_ref.at[tail_rows, :], halo_bc, halo_send.at[1], halo_recv.at[1], {"seq": z + 1}),
        ]

    @pl.when(z < n - 1)
    def _():
        for copy in halo_copies():
            copy.start()

    def w_rows(source, group, part):
        return pl.ds(pl.multiple_of(source * depth + group * band + part * sub, 16), sub)

    def w_copy(rank, part):
        columns_there = pl.ds(starts[rank], widths[rank])
        return remote(
            lm_ref.at[pl.ds(pl.multiple_of(g * band + part * sub, 16), sub), columns_there],
            w_buf.at[w_rows(z, g, part), pl.ds(0, widths[rank])],
            w_send.at[rank, part],
            w_recv.at[z, part],
            {"seq": rank},
        )

    def w_place(rank, source, group, part):
        return w_buf.at[w_rows(source, group, part), pl.ds(0, widths[rank])]

    def w_forward(rank, source, part, hop):
        place = w_place(rank, source, g, part)
        return remote(
            place, place, y_send.at[source, part, hop], y_recv.at[g, source, part],
            {"groups": lax.rem(g + hop, groups)},
        )

    def w_pass_on(rank, source, part):
        place = w_place(rank, source, g, part)
        remote(
            place, place, w_send.at[source, part], w_recv.at[source, part], {"seq": source}
        ).wait_recv()
        for hop in range(1, groups):
            w_forward(rank, source, part, hop).start()

    def legs(rank):
        far_first = list(range(n - 1, rank, -1)) + list(range(rank))
        every = [(source, part) for source in far_first for part in range(PARTS)]

        def stage(leg):
            source, part = leg
            if rank == 0:
                return 0 if source == n - 1 and part < PARTS - 1 else 1 if source != 2 else 2
            if source == rank - 1:
                return 0 if part == 0 else 1 if rank in (1, n - 1) else 2
            if source < rank:
                return 1 if rank == n - 1 and part < PARTS - 1 and source == 0 else 2
            return 1 if source > rank + 1 or (rank == n - 2 and part < PARTS // 2) else 2

        staged = [[leg for leg in every if stage(leg) == which] for which in range(3)]
        if rank > 0:
            staged[1].sort(key=lambda leg: leg[1] if rank < n - 1 else -leg[0])
        if rank < n - 1:
            staged[2].sort(key=lambda leg: (-leg[0], leg[1]))
        return staged

    def pass_on_stage(which):
        for rank in range(n):
            @pl.when(z == rank)
            def _():
                for source, part in legs(rank)[which]:
                    w_pass_on(rank, source, part)

    for rank in range(n):
        @pl.when(z > rank)
        def _():
            for part in range(PARTS):
                w_copy(rank, part).start()

        @pl.when(z + 1 == rank)
        def _():
            w_copy(rank, 0).start()

    def tell(k, source):
        return remote(
            tgt_ref, tgts.at[source], tgt_send.at[k], tgt_recv.at[source],
            {"seq": lax.rem(z + k, n)},
        )

    for k in range(1, n):
        tell(k, z).start()
    tgts[z] = tgt_ref[...]

    starts_of = [jnp.int32(0)]
    for document in range(lens_ref.shape[0] - 1):
        starts_of.append(starts_of[-1] + lens_ref[document])

    def document(positions):
        total = (positions >= starts_of[0]).astype(jnp.int32)
        for start in starts_of[1:]:
            total = total + (positions >= start).astype(jnp.int32)
        return total

    offset_here = z * length

    def along(shape, axis):
        return lax.broadcasted_iota(jnp.int32, shape, axis) + offset_here

    here_heads = dt_ref.shape[0]
    head_row = lax.broadcasted_iota(jnp.int32, (here_heads, length), 0)
    lane_row = lax.broadcasted_iota(jnp.int32, (here_heads, length), 1)
    shift = jnp.zeros((here_heads, length), jnp.float32)
    rate = jnp.zeros((here_heads, length), jnp.float32)
    for head in range(here_heads):
        shift = jnp.where(head_row == head, dt_bias_ref[head], shift)
        rate = jnp.where(head_row == head, rate_ref[head], rate)
    raw = dt_ref[...] + shift
    steps = jnp.maximum(raw, 0.0) + jnp.log1p(jnp.exp(-jnp.abs(raw)))
    climb = steps * rate
    by = 1
    while by < length:
        climb = climb + jnp.where(lane_row >= by, pltpu.roll(climb, by, 1), 0.0)
        by *= 2
    is_last = document(along((here_heads, length), 1)) == document(offset_here + length - 1)
    leave = jnp.where(is_last, jnp.exp(climb - climb[:, length - 1 :]) * steps, 0.0)
    for c in range(chunks):
        pair = slice(2 * c, 2 * c + 2)
        rows[c, 0:2, :] = climb[pair]
        rows[c, 2:4, :] = steps[pair]
        rows[c, 4:6, :] = leave[pair]
        rows[c, 6:8, :] = leave[pair]

    token = along((length, TILE), 0)
    at_token = document(token)
    for lag in range(1, KERNEL):
        masks[lag - 1] = (document(token - lag) == at_token).astype(jnp.float32)
    carried[...] = (at_token == document(offset_here - 1)).astype(jnp.float32)

    @pl.when(z == 0)
    def _():
        halo_x[...] = jnp.zeros_like(halo_x)
        halo_bc[...] = jnp.zeros_like(halo_bc)
        state_in[...] = jnp.zeros_like(state_in)

    @pl.when(z > 0)
    def _():
        for copy in halo_copies():
            copy.wait_recv()

    def convolved(signal, halo, weight, bias, lanes):
        weight = weight[:, lanes].astype(jnp.float32)
        held[0:HALO, :] = halo[:, lanes].astype(jnp.float32)
        held[HALO:, :] = signal[:, lanes].astype(jnp.float32)
        total = jnp.zeros((length, TILE), jnp.float32) + bias
        for offset in range(KERNEL):
            lag = KERNEL - 1 - offset
            term = weight[offset : offset + 1, :] * held[HALO - lag : HALO - lag + length, :]
            total = total + (term * masks[lag - 1] if lag else term)
        return jax.nn.silu(total).astype(jnp.bfloat16)

    def line(at):
        return table_ref[pl.ds(at, 1), :]

    for half in range(2):
        lanes = pl.ds(half * STATE, STATE)
        keys[:, lanes] = convolved(bc_ref, halo_bc, bc_taps_ref, line(2 * chunks + half), lanes)
    nt = (((1,), (1,)), ((), ()))
    for cut in range(0, length, SPAN):
        near = pl.ds(cut, SPAN)
        target, source = along((SPAN, length), 0) + cut, along((SPAN, length), 1)
        inside = (document(target) == document(source)) & (target >= source)
        product = lax.dot_general(
            keys[near, STATE:], keys[:, :STATE], nt, preferred_element_type=jnp.float32
        )
        scores[near, :] = jnp.where(inside, product, 0.0)

    def state_copy(c):
        return remote(
            state_out.at[c], state_in.at[c], state_send.at[c], state_recv.at[c], {"seq": z + 1}
        )

    first = lax.broadcasted_iota(jnp.int32, (SPAN, TILE), 1) < HEAD_SIZE

    @pl.loop(0, chunks)
    def _(c):
        lanes = pl.ds(pl.multiple_of(c * TILE, TILE), TILE)
        own = convolved(x_ref, halo_x, taps_ref, line(c), lanes)
        values[:, lanes] = own
        early = lax.broadcasted_iota(jnp.int32, (length, TILE), 1) < HEAD_SIZE
        cols[c] = jnp.transpose(rows[c])
        decay = jnp.where(early, cols[c, :, 4:5], cols[c, :, 5:6])
        scaled = own.astype(jnp.float32) * decay
        high = scaled.astype(jnp.bfloat16)
        low = (scaled - high.astype(jnp.float32)).astype(jnp.bfloat16)
        bmat = keys[:, :STATE]
        tn = (((0,), (0,)), ((), ()))
        state_out[c] = lax.dot_general(
            high, bmat, tn, preferred_element_type=jnp.float32
        ) + lax.dot_general(low, bmat, tn, preferred_element_type=jnp.float32)

        @pl.when(z == 0)
        def _():
            state_copy(c).start()

    squares[...] = jnp.zeros_like(squares)

    @pl.loop(0, chunks)
    def _(c):
        lanes = pl.ds(pl.multiple_of(c * TILE, TILE), TILE)

        @pl.when(z > 0)
        def _():
            state_copy(c).wait_recv()

        @pl.when((z > 0) & (z < n - 1))
        def _():
            top = lax.broadcasted_iota(jnp.int32, (TILE, STATE), 0) < HEAD_SIZE
            final = cols[c, length - 1 : length, 0:2]
            through = jnp.where(top, jnp.exp(-final[:, 0:1]), jnp.exp(-final[:, 1:2]))
            through = through * carried[length - 1 : length, 0:1]
            state_out[c] = through * state_in[c] + state_out[c]
            state_copy(c).start()

        skip = jnp.where(first, skip_ref[2 * c], skip_ref[2 * c + 1])
        incoming = state_in[c]
        in_high = incoming.astype(jnp.bfloat16)
        in_low = (incoming - in_high.astype(jnp.float32)).astype(jnp.bfloat16)
        for cut in range(0, length, SPAN):
            upto = cut + SPAN
            near = pl.ds(cut, SPAN)
            signal = values[0:upto, lanes]
            sums_of = []
            entries = []
            for which in range(2):
                climb = cols[c, near, which : which + 1]
                gap = rows[c, which : which + 1, 0:upto] - climb
                weights = (
                    jnp.exp(jnp.minimum(gap, 0.0))
                    * scores[near, 0:upto]
                    * rows[c, 2 + which : 3 + which, 0:upto]
                )
                high = weights.astype(jnp.bfloat16)
                low = (weights - high.astype(jnp.float32)).astype(jnp.bfloat16)
                sums_of.append(
                    jnp.dot(high, signal, preferred_element_type=jnp.float32)
                    + jnp.dot(low, signal, preferred_element_type=jnp.float32)
                )
                entries.append(jnp.exp(-climb))
            cmat = keys[near, STATE:]
            arriving = lax.dot_general(
                cmat, in_high, nt, preferred_element_type=jnp.float32
            ) + lax.dot_general(cmat, in_low, nt, preferred_element_type=jnp.float32)
            mixed = (
                jnp.where(first, sums_of[0], sums_of[1])
                + skip * values[near, lanes].astype(jnp.float32)
                + arriving * (jnp.where(first, entries[0], entries[1]) * carried[near, :])
            )
            result = mixed * jax.nn.silu(z_ref[near, lanes].astype(jnp.float32))
            gated[near, lanes] = result
            squares[near, :] += result * result

    for rank in range(1, n):
        @pl.when(z + 1 == rank)
        def _():
            for part in range(1, PARTS):
                w_copy(rank, part).start()

    for rank in range(n - 1, 1, -1):
        @pl.when(z + 1 < rank)
        def _():
            for part in range(PARTS):
                w_copy(rank, part).start()

    pass_on_stage(0)

    def tile_copy(which, k, slot_of):
        return remote(
            tiles.at[which, slot_of], tiles.at[which, slot_of], tile_send.at[which, k],
            tile_recv.at[which, slot_of], {"head": lax.rem(h + k, heads)},
        )

    def scale_of(which, partial, count):
        column = jnp.broadcast_to(jnp.sum(partial, axis=1, keepdims=True), (length, TILE))
        tiles[which, h] = jnp.transpose(column)[0:8, :]
        for k in range(1, heads):
            tile_copy(which, k, h).start()
        for k in range(1, heads):
            tile_copy(which, k, lax.rem(h + k, heads)).wait()
        total = tiles[which, 0]
        for head in range(1, heads):
            total = total + tiles[which, head]
        scale = lax.rsqrt(total / count + EPSILON)
        return jnp.transpose(jnp.broadcast_to(scale[0:1, :], (TILE, length)))

    squares[...] = scale_of(0, squares[...], inner)

    @pl.loop(0, chunks)
    def _(c):
        lanes = pl.ds(pl.multiple_of(c * TILE, TILE), TILE)
        normed[:, lanes] = (gated[:, lanes] * squares[...] * line(chunks + c)).astype(jnp.bfloat16)

    load_out.wait()

    def project(head, slot_of):
        @pl.loop(0, length // LOSS_ROWS)
        def _(step):
            near = pl.ds(pl.multiple_of(step * LOSS_ROWS, LOSS_ROWS), LOSS_ROWS)
            share_out[slot_of, near, :] = jnp.dot(
                normed[near, :],
                ow_buf[:, pl.ds(pl.multiple_of(head * share, TILE), share)],
                preferred_element_type=jnp.float32,
            )

    def share_copy(slot_of, target):
        return remote(
            share_out.at[slot_of], share_in.at[slot_of], share_send.at[slot_of],
            share_recv.at[slot_of], {"head": target},
        )

    project(lax.rem(twin + 2, heads), 0)
    share_copy(0, twin).start()
    project(side, 1)
    share_copy(0, twin).wait_recv()
    share_out[1] = share_out[1] + share_in[0]
    share_copy(1, side).start()
    project(twin, 2)
    share_copy(2, twin).start()
    project(h, 3)

    pass_on_stage(1)

    share_copy(2, twin).wait_recv()
    share_copy(1, side).wait_recv()

    @pl.loop(0, length // LOSS_ROWS)
    def _(step):
        near = pl.ds(pl.multiple_of(step * LOSS_ROWS, LOSS_ROWS), LOSS_ROWS)
        total = share_out[3, near, :] + share_in[2, near, :] + share_in[1, near, :]
        block_ref[near, :] = (res_ref[near, :].astype(jnp.float32) + total).astype(jnp.bfloat16)

    square = jnp.zeros((length, TILE), jnp.float32)
    for cut in range(0, share, TILE):
        piece = block_ref[:, cut : cut + TILE].astype(jnp.float32)
        square = square + piece * piece
    squares[...] = scale_of(1, square, features)
    for cut in range(0, share, TILE):
        piece = block_ref[:, cut : cut + TILE].astype(jnp.float32)
        hid[:, cut : cut + TILE] = (
            piece * squares[...] * line(2 * chunks + 2 + h * (share // TILE) + cut // TILE)
        ).astype(jnp.bfloat16)

    full[z, :, pl.ds(pl.multiple_of(h * share, TILE), share)] = hid[...]

    half_rows = length // SPLIT
    logit_rows = min(LOSS_ROWS, half_rows)

    def near_of(half):
        start = half * half_rows
        return pl.ds(start if isinstance(start, int) else pl.multiple_of(start, 16), half_rows)

    def slot(block, head, half):
        near = near_of(half)
        return full.at[block, near, pl.ds(pl.multiple_of(head * share, TILE), share)]

    def ship(sems, block, head, half, target, first=False):
        place = slot(block, head, half)
        return remote(
            hid.at[near_of(half), :] if first else place, place,
            sems.at[block, half], arrive.at[block, head, half], target,
        )

    def right(block, half, first=False):
        return ship(along_send.at[0], block, h, half, {"seq": z + 1}, first)

    def left(block, half, first=False):
        return ship(along_send.at[1], block, h, half, {"seq": z - 1}, first)

    def across(block, half, first=False):
        return ship(side_send, block, h, half, {"head": side}, first)

    def twinned(kind, block, head, half, first=False):
        return ship(along_send.at[2 + kind], block, head, half, {"head": twin}, first)

    def arrived(block, head, half):
        twinned(0, block, head, half).wait_recv()

    for half in range(SPLIT):
        @pl.when(z < n - 1)
        def _():
            right(z, half, True).start()

        @pl.when(z > 0)
        def _():
            left(z, half, True).start()

        across(z, half, True).start()
        twinned(0, z, h, half, True).start()

    def mark_copy(block, head):
        return remote(
            marks.at[block, :, pl.ds(pl.multiple_of(head * TILE, TILE), TILE)], parts.at[me],
            mark_send.at[block, head], mark_recv.at[me], {"seq": block, "head": head},
        )

    live, start_column = widths[0], 0
    for rank in range(1, n):
        live = jnp.where(z == rank, widths[rank], live)
        start_column = jnp.where(z == rank, starts[rank], start_column)
    start_column = h * columns + start_column
    width = w_buf.shape[1]

    def compute(block, half):
        @pl.loop(0, half_rows // logit_rows)
        def _(step):
            at = pl.multiple_of(half * half_rows + step * logit_rows, logit_rows)
            logits = jnp.dot(
                full[block, pl.ds(at, logit_rows), :], w_buf[...], preferred_element_type=jnp.float32
            )
            wanted = []
            for cut in range(logit_rows // TILE):
                row = tgts[block, pl.ds(lax.div(at, TILE) + cut, 1), :]
                wanted.append(jnp.transpose(jnp.broadcast_to(row, (TILE, TILE))))
            wanted = jnp.concatenate(wanted, axis=0) - start_column
            lane = lax.broadcasted_iota(jnp.int32, (logit_rows, TILE), 1)
            pieces = []
            for cut in range(0, width, TILE):
                piece = logits[:, cut : cut + TILE]
                if cut + TILE > min(widths):
                    piece = jnp.where(lane + cut < live, piece, LOW)
                pieces.append(piece)
            peak = pieces[0]
            for piece in pieces[1:]:
                peak = jnp.maximum(peak, piece)
            peak = jnp.max(peak, axis=1, keepdims=True)
            total = jnp.zeros((logit_rows, TILE), jnp.float32)
            picked = jnp.zeros((logit_rows, TILE), jnp.float32)
            for index, piece in enumerate(pieces):
                total = total + jnp.exp(piece - peak)
                here = lane + index * TILE == wanted
                if (index + 1) * TILE > min(widths):
                    here = here & (lane + index * TILE < live)
                picked = picked + jnp.where(here, piece, 0.0)
            total = jnp.sum(total, axis=1, keepdims=True)
            picked = jnp.sum(picked, axis=1, keepdims=True)
            tile = jnp.where(lane == 0, peak, jnp.where(lane == 1, total, picked))
            marks[block, :, pl.ds(at, logit_rows)] = jnp.transpose(tile)[0:8, :]

        @pl.loop(half * (heads // SPLIT), (half + 1) * (heads // SPLIT))
        def _(head):
            @pl.when((block != z) | (head != h))
            def _():
                mark_copy(block, head).start()

    def relay(block, half):
        arrived(block, side, half)
        twinned(1, block, side, half).start()

    def finish(block, half):
        arrived(block, twin, half)
        arrived(block, lax.rem(twin + 2, heads), half)
        compute(block, half)

    pass_on_stage(2)

    def embedding_here():
        for k in range(1, n):
            tell(k, lax.rem(z + n - k, n)).wait()
        for rank in range(n):
            @pl.when(z == rank)
            def _():
                load_own(rank).wait()
                for source in range(n):
                    if source == rank:
                        continue
                    for hop in range(1, groups):
                        other = lax.rem(g + groups - hop, groups)
                        for part in range(PARTS):
                            place = w_place(rank, source, other, part)
                            remote(
                                place, place, y_send.at[source, part, hop],
                                y_recv.at[other, source, part], {"groups": other},
                            ).wait_recv()

    def over_step(step, act, low=0, high=SPLIT):
        span = high - low

        @pl.loop(0, 2 * span if step else span)
        def _(turn):
            half = low + lax.rem(turn, span)
            block = z - step + 2 * step * lax.div(turn, span)

            @pl.when((block >= 0) & (block < n))
            def _():
                act(block, half)

    def last_step(block, half):
        relay(block, half)
        finish(block, half)

    def from_left(step, half):
        @pl.when(z >= step)
        def _():
            block = z - step
            arrived(block, h, half)

            @pl.when(z < n - 1)
            def _():
                right(block, half).start()

            across(block, half).start()
            twinned(0, block, h, half).start()

    def from_right(step, half):
        @pl.when(z + step < n)
        def _():
            block = z + step
            arrived(block, h, half)

            @pl.when(z > 0)
            def _():
                left(block, half).start()

            across(block, half).start()
            twinned(0, block, h, half).start()

    @pl.when(z >= n // 2)
    def _():
        for half in range(SPLIT):
            from_right(1, half)

    at_end = (z == 0) | (z == n - 1)
    for step in range(1, n):
        for half in range(SPLIT):
            from_left(step, half)
            if step > 1:
                from_right(step, half)
                continue

            @pl.when(z < n // 2)
            def _():
                from_right(1, half)

            if half == 0:
                over_step(0, relay)

                @pl.when(at_end)
                def _():
                    embedding_here()

            @pl.when(at_end)
            def _():
                finish(z, half)

        if step == 1:
            @pl.when(jnp.logical_not(at_end))
            def _():
                embedding_here()
                over_step(0, finish)

        elif step < n - 1:
            over_step(step - 1, relay)
            over_step(step - 1, finish)
    if n > 2:
        over_step(n - 2, relay)
        over_step(n - 2, finish, 0, SPLIT - 1)
        over_step(n - 1, relay, 0, 1)
        over_step(n - 2, finish, SPLIT - 1, SPLIT)
        over_step(n - 1, relay, 1, SPLIT)
        over_step(n - 1, finish)
    else:
        over_step(n - 1, last_step)

    @pl.when(z < n - 1)
    def _():
        for copy in halo_copies():
            copy.wait_send()

        @pl.loop(0, chunks)
        def _(c):
            state_copy(c).wait_send()

    for slot_of, target in ((0, twin), (1, side), (2, twin)):
        share_copy(slot_of, target).wait_send()
    for rank in range(n):
        @pl.when(z != rank)
        def _():
            for part in range(PARTS):
                w_copy(rank, part).wait_send()

        @pl.when(z == rank)
        def _():
            for source in range(n):
                for part in range(PARTS):
                    for hop in range(1, groups if source != rank else 1):
                        w_forward(rank, source, part, hop).wait_send()

    for block in range(n):
        for half in range(SPLIT):
            @pl.when((z < n - 1) & (z >= block))
            def _():
                right(block, half).wait_send()

            @pl.when((z > 0) & (z <= block))
            def _():
                left(block, half).wait_send()

            across(block, half).wait_send()
            twinned(0, block, h, half).wait_send()
            twinned(1, block, side, half).wait_send()

    parts[me] = marks[z, :, pl.ds(pl.multiple_of(h * TILE, TILE), TILE)]

    @pl.loop(1, total_peers)
    def _(k):
        there, where_head = peer(k)
        flat = there * heads + where_head
        remote(
            parts.at[flat], parts.at[flat], mark_send.at[there, where_head], mark_recv.at[flat],
            {"seq": there, "head": where_head},
        ).wait()

    peak = parts[0, 0:1, :]
    for flat in range(1, total_peers):
        peak = jnp.maximum(peak, parts[flat, 0:1, :])
    total = jnp.zeros((1, TILE), jnp.float32)
    picked = jnp.zeros((1, TILE), jnp.float32)
    for flat in range(total_peers):
        total = total + parts[flat, 1:2, :] * jnp.exp(parts[flat, 0:1, :] - peak)
        picked = picked + parts[flat, 2:3, :]
    losses = peak + jnp.log(total) - picked
    member_shape = sums.shape[1:]
    position = along(member_shape, 1) + h * TILE
    member = document(position) == lax.broadcasted_iota(jnp.int32, member_shape, 0) + 1
    mine = jnp.sum(jnp.where(member, losses, 0.0), axis=1, keepdims=True)
    sums[me] = jnp.broadcast_to(mine, sums.shape[1:])

    def sum_copy(k, slot_of):
        there, where_head = peer(k)
        return remote(
            sums.at[slot_of], sums.at[slot_of], sum_send.at[k], sum_recv.at[slot_of],
            {"seq": there, "head": where_head},
        )

    @pl.loop(1, total_peers)
    def _(k):
        sum_copy(k, me).start()

    @pl.loop(1, total_peers)
    def _(k):
        sum_copy(k, lax.rem(me + k, total_peers)).wait()

    grand = sums[0]
    for flat in range(1, total_peers):
        grand = grand + sums[flat]
    out_ref[...] = grand


def widths_of(columns, n):
    tiles = columns // TILE
    counts = [tiles // n + (rank < tiles % n) for rank in range(n)]
    if n > 2:
        counts[1] += 1
        counts[n - 1] -= 1
    return tuple(count * TILE for count in counts)


def fits(length, inner_here, share, depth, columns, n, heads, groups):
    widths = widths_of(columns, n)
    features = n * depth
    room = 2 * features * (n * length + max(widths) + inner_here)
    room += 4 * (length * inner_here * 4 + 6 * length * share + length * length)
    even = [inner_here % TILE, share % TILE, columns % TILE, depth % (groups * PARTS * 16)]
    even += [length % SPAN, length % LOSS_ROWS, length % (SPLIT * TILE), heads % SPLIT, length - heads * TILE, heads - 4]
    even += [share * heads - features]
    return not any(even) and n > 1 and min(widths) > 0 and room < 56 * 2**20


def block_stage(operands, scalars, whole, n, heads, groups):
    x_in, res = operands[0], operands[5]
    out_weight, lm_weight = whole
    length, inner_here = x_in.shape
    share = res.shape[1]
    features = out_weight.shape[1]
    widths = widths_of(lm_weight.shape[1], n)
    width = max(widths)
    peers = n * heads
    chunks = inner_here // TILE
    result = (-(-scalars[0].shape[0] // 8) * 8, TILE)
    dma = pltpu.SemaphoreType.DMA
    vmem = pltpu.VMEM
    f32, bf16 = jnp.float32, jnp.bfloat16
    return pl.pallas_call(
        functools.partial(block_kernel, n, heads, groups, inner_here * heads, features, widths),
        out_shape=[
            jax.ShapeDtypeStruct((length, share), bf16),
            jax.ShapeDtypeStruct(result, f32),
        ],
        in_specs=[pl.BlockSpec(memory_space=pltpu.VMEM)] * len(operands)
        + [pl.BlockSpec(memory_space=pltpu.SMEM)] * len(scalars)
        + [pl.BlockSpec(memory_space=pl.ANY)] * 2,
        out_specs=[pl.BlockSpec(memory_space=pltpu.VMEM)] * 2,
        scratch_shapes=[
            vmem((inner_here, features), bf16),
            vmem((features, width), bf16),
            vmem((n, length, features), bf16),
            vmem((n, heads, TILE), jnp.int32),
            vmem((n, 8, length), f32),
            vmem((peers, 8, TILE), f32),
            vmem((peers,) + result, f32),
            vmem((HALO, inner_here), bf16),
            vmem((HALO, 2 * STATE), bf16),
            vmem((length + HALO, TILE), f32),
            vmem((KERNEL - 1, length, TILE), f32),
            vmem((length, TILE), f32),
            vmem((chunks, 8, length), f32),
            vmem((chunks, length, 8), f32),
            vmem((length, inner_here), bf16),
            vmem((length, 2 * STATE), bf16),
            vmem((length, length), f32),
            vmem((chunks, TILE, STATE), f32),
            vmem((chunks, TILE, STATE), f32),
            vmem((length, inner_here), f32),
            vmem((length, TILE), f32),
            vmem((2, heads, 8, length), f32),
            vmem((length, inner_here), bf16),
            vmem((4, length, share), f32),
            vmem((3, length, share), f32),
            vmem((length, share), bf16),
            dma((2,)),
            dma((2,)),
            dma((2,)),
            dma((n, PARTS)),
            dma((n, PARTS)),
            dma((n, PARTS, groups)),
            dma((groups, n, PARTS)),
            dma((chunks,)),
            dma((chunks,)),
            dma((2, heads)),
            dma((2, heads)),
            dma((3,)),
            dma((3,)),
            dma((4, n, SPLIT)),
            dma((n, SPLIT)),
            dma((n, heads, SPLIT)),
            dma((n,)),
            dma((n,)),
            dma((n, heads)),
            dma((peers,)),
            dma((peers,)),
            dma((peers,)),
        ],
        compiler_params=pltpu.CompilerParams(
            collective_id=0, has_side_effects=True, vmem_limit_bytes=63 * 2**20
        ),
        cost_estimate=pl.CostEstimate(
            flops=2 * n * length * features * width, bytes_accessed=4 * 10**7, transcendentals=10**7
        ),
    )(*operands, *scalars, *whole)


def fused_fits(residual, x_in, lm_weight):
    length, inner_here = x_in.shape
    depth, columns = lm_weight.shape
    sizes = [lax.axis_size(axis) for axis in ("seq", "head", "groups")]
    return fits(
        length, inner_here, residual.shape[1], depth, columns, *sizes
    )


def fused(
    residual,
    x_in,
    bc_in,
    z_in,
    dt_raw,
    dt_bias,
    decay_rate,
    d_skip,
    conv_x_weight,
    conv_x_bias,
    conv_bc_weight,
    conv_bc_bias,
    norm_gain,
    out_weight,
    final_gain,
    lm_weight,
    targets,
    doc_lengths,
):
    table = jnp.concatenate([conv_x_bias, norm_gain, conv_bc_bias, final_gain])
    operands = [
        x_in,
        z_in,
        bc_in,
        conv_x_weight,
        conv_bc_weight,
        residual,
        targets.reshape(-1, TILE),
        dt_raw,
        table.astype(jnp.float32).reshape(-1, TILE),
    ]
    scalars = [doc_lengths, dt_bias, decay_rate, d_skip]
    sizes = [lax.axis_size(axis) for axis in ("seq", "head", "groups")]
    block_out, sums = block_stage(operands, scalars, (out_weight, lm_weight), *sizes)
    sums = sums[: doc_lengths.shape[0], 0]
    return (block_out, sums / doc_lengths.astype(jnp.float32))


def local(
    residual,
    x_in,
    bc_in,
    z_in,
    dt_raw,
    dt_bias,
    decay_rate,
    d_skip,
    conv_x_weight,
    conv_x_bias,
    conv_bc_weight,
    conv_bc_bias,
    norm_gain,
    out_weight,
    final_gain,
    lm_weight,
    targets,
    doc_lengths,
):
    if fused_fits(residual, x_in, lm_weight):
        return fused(
            residual,
            x_in,
            bc_in,
            z_in,
            dt_raw,
            dt_bias,
            decay_rate,
            d_skip,
            conv_x_weight,
            conv_x_bias,
            conv_bc_weight,
            conv_bc_bias,
            norm_gain,
            out_weight,
            final_gain,
            lm_weight,
            targets,
            doc_lengths,
        )
    length = x_in.shape[0]
    inner_here = x_in.shape[1]
    heads_here = dt_raw.shape[0]
    seq_rank = lax.axis_index("seq")
    head_rank = lax.axis_index("head")
    offset_here = seq_rank * length
    positions = offset_here + jnp.arange(length, dtype=jnp.int32)
    doc_ids = document_of(positions, doc_lengths)
    columns_here = lm_weight.shape[1]
    devices = lax.axis_size("seq")
    width = -(-columns_here // (devices * 128)) * 128

    def window(rank):
        return jnp.minimum(rank * width, columns_here - width)

    depth = lm_weight.shape[0]
    vocab_weight = jnp.zeros((depth * devices, width), lm_weight.dtype)
    group = lax.axis_index("groups")
    groups = lax.axis_size("groups")
    band = depth // groups
    pieces = [
        lax.dynamic_slice(
            lm_weight, (group * band, window((seq_rank + by) % devices)), (band, width)
        )
        for by in range(1, devices)
    ]
    aims = [targets]
    for by in range(1, devices):
        aims.append(rotated(targets, "seq", by))
    margin = KERNEL - 1
    rims = shifted(
        jnp.concatenate([x_in[length - margin :], bc_in[length - margin :]], axis=1), "seq", 1
    )
    x_rim, bc_rim = rims[:, :inner_here], rims[:, inner_here:]
    keys_queries = causal_conv(
        bc_in, bc_rim, conv_bc_weight, conv_bc_bias, positions, doc_ids, doc_lengths
    )
    bmat, cmat = keys_queries[:, :STATE], keys_queries[:, STATE:]
    steps = jax.nn.softplus(dt_raw + dt_bias[:, None])
    climb = jnp.cumsum(steps * decay_rate[:, None], axis=1)
    before = document_of(jnp.reshape(offset_here - 1, (1,)), doc_lengths)[0]
    carried = (doc_ids == before).astype(jnp.float32)
    through = jnp.exp(-climb[:, length - 1]) * carried[length - 1]
    same = jnp.stack(
        [
            (document_of(positions - lag, doc_lengths) == doc_ids).astype(jnp.float32)
            for lag in range(KERNEL)
        ],
        axis=1,
    )
    last = (doc_ids == doc_ids[length - 1]).astype(jnp.float32)
    tail = jnp.exp(climb - climb[:, length - 1 :]) * last[None, :] * steps
    couples = heads_here // 2
    rows = jnp.concatenate(
        [climb.reshape(couples, 2, length), steps.reshape(couples, 2, length)], axis=1
    )
    cols = jnp.concatenate(
        [climb.reshape(couples, 2, length), tail.reshape(couples, 2, length)], axis=1
    ).transpose(0, 2, 1)
    rim = jnp.concatenate([jnp.zeros((8 - margin, inner_here), x_rim.dtype), x_rim], axis=0)
    values, own_end = conv_state(
        x_in,
        rim,
        conv_x_weight.astype(jnp.float32),
        conv_x_bias.astype(jnp.float32)[None, :],
        same,
        cols,
        bmat,
    )
    of_head = jnp.arange(inner_here, dtype=jnp.int32)[None, :] // HEAD_SIZE
    spread = (of_head == jnp.arange(heads_here, dtype=jnp.int32)[:, None]).astype(jnp.float32)
    incoming = entering(
        through, own_end.reshape(heads_here, HEAD_SIZE, STATE), "seq"
    ).reshape(inner_here, STATE)
    held_back = lax.optimization_barrier(tuple(pieces[1:]) + (incoming,))
    pieces, incoming = pieces[:1] + list(held_back[:-1]), held_back[-1]
    arrivals = []
    for by in range(1, devices):
        arrivals.append(rotated(pieces[by - 1], "seq", by))
    bands = []
    for by in range(1, devices):
        bands.append(
            [arrivals[by - 1]]
            + [rotated(arrivals[by - 1], "groups", hop) for hop in range(1, groups)]
        )
    order = jnp.arange(length, dtype=jnp.int32)
    inside = (doc_ids[:, None] == doc_ids[None, :]) & (order[:, None] >= order[None, :])
    scores = jnp.where(
        inside,
        lax.dot_general(
            cmat, bmat, (((1,), (1,)), ((), ())), preferred_element_type=jnp.float32
        ),
        0.0,
    )
    skip = jnp.dot(d_skip[None, :], spread, precision=HIGH)
    output = within(values, scores, cols, rows, skip)
    entry = jnp.dot((jnp.exp(-climb) * carried[None, :]).T, spread, precision=HIGH)
    arriving = lax.dot_general(
        cmat.astype(jnp.float32), incoming, (((1,), (1,)), ((), ())), precision=HALF
    )
    gated = (output + arriving * entry) * jax.nn.silu(z_in.astype(jnp.float32))
    square_sum = lax.psum(jnp.sum(gated * gated, axis=1), "head")
    scale = lax.rsqrt(square_sum / INNER + EPSILON)
    normed = (gated * scale[:, None] * norm_gain.astype(jnp.float32)[None, :]).astype(jnp.bfloat16)
    share = residual.shape[1]
    projected = scattered_product(normed, out_weight, "head")
    block_out = (residual.astype(jnp.float32) + projected).astype(jnp.bfloat16)
    widened = block_out.astype(jnp.float32)
    square_total = lax.psum(jnp.sum(widened * widened, axis=1), "head")
    gain_part = lax.dynamic_slice_in_dim(final_gain, head_rank * share, share, 0)
    final_scale = lax.rsqrt(square_total / D + EPSILON)
    hidden_part = (widened * final_scale[:, None] * gain_part.astype(jnp.float32)[None, :]).astype(
        jnp.bfloat16
    )
    own = lax.dynamic_slice_in_dim(lm_weight, window(seq_rank), width, 1)
    vocab_weight = lax.dynamic_update_slice_in_dim(vocab_weight, own, seq_rank * depth, 0)
    for by in range(1, devices):
        source = (seq_rank + devices - by) % devices
        for hop in range(groups):
            start = source * depth + (group + groups - hop) % groups * band
            vocab_weight = lax.dynamic_update_slice_in_dim(
                vocab_weight, bands[by - 1][hop], start, 0
            )
    column = jnp.arange(width, dtype=jnp.int32)
    first = head_rank * columns_here + window(seq_rank)
    live = column + window(seq_rank) >= seq_rank * width
    marks = jnp.zeros((3, length * devices), jnp.float32)
    for by in range(devices):
        source = (seq_rank + devices - by) % devices
        if by and by % 4 == 0:
            hidden_part, marks = lax.optimization_barrier((hidden_part, marks))
        rows = rotated(hidden_part, "seq", by) if by else hidden_part
        hidden = gathered_features(rows, "head")
        logits = jnp.dot(hidden, vocab_weight, preferred_element_type=jnp.float32)
        logits = jnp.where(live[None, :], logits, LOW)
        peak = jnp.max(logits, axis=1)
        wanted = aims[by] - first
        total = jnp.sum(jnp.exp(logits - peak[:, None]), axis=1)
        picked = jnp.sum(
            jnp.where((column[None, :] == wanted[:, None]) & live[None, :], logits, 0.0), axis=1
        )
        marks = lax.dynamic_update_slice_in_dim(
            marks, jnp.stack([peak, total, picked]), source * length, 1
        )
    for axis in ("head", "seq"):
        every_mark = lax.all_gather(marks, axis)
        peak = jnp.max(every_mark[:, 0], axis=0)
        total = jnp.sum(every_mark[:, 1] * jnp.exp(every_mark[:, 0] - peak[None]), axis=0)
        marks = jnp.stack([peak, total, jnp.sum(every_mark[:, 2], axis=0)])
    losses = marks[0] + jnp.log(marks[1]) - marks[2]
    every = document_of(jnp.arange(length * devices, dtype=jnp.int32), doc_lengths)
    documents = jnp.arange(doc_lengths.shape[0], dtype=jnp.int32)
    member = every[None, :] == documents[:, None]
    sums = jnp.sum(jnp.where(member, losses[None, :], 0.0), axis=1)
    return (block_out, sums / doc_lengths.astype(jnp.float32))


def solution(mesh):
    in_specs = (
        P(("groups", "seq"), "head"),
        P(("groups", "seq"), "head"),
        P(("groups", "seq"), None),
        P(("groups", "seq"), "head"),
        P("head", ("groups", "seq")),
        P("head"),
        P("head"),
        P("head"),
        P(None, "head"),
        P("head"),
        P(),
        P(),
        P("head"),
        P("head", None),
        P(),
        P("seq", "head"),
        P(("groups", "seq")),
        P("groups"),
    )
    out_specs = (P(("groups", "seq"), "head"), P("groups"))


    return jax.shard_map(local, mesh=mesh, in_specs=in_specs, out_specs=out_specs, check_vma=False)
```
